32 devices in a mesh: dp: 4 (over x, core), mp: 8 (over z, y).
Axes of the slice: x: 2, y: 2, z: 4, core: 2. Of those that a mesh axis runs over, the one named last changes fastest.
Arguments:
- tokens: bfloat16 [25088, 512], P(('dp', 'mp')), may hold values from -6 to 6
- cotangent: bfloat16 [25088, 512], P(('dp', 'mp')), may hold values from -6 to 6
- image_counts: int32 [4], replicated, may hold values from 1 to 32, 96 in all
- params: float32 [8, 394324], P('mp', 'dp'), may hold values from -4 to 4, as said below
- moment_one: float32 [8, 394324], P('mp', 'dp'), may hold values from -96 to 96
- moment_two: float32 [8, 394324], P('mp', 'dp'), may hold values from 0 to 40, as said below
Outputs:
- output: bfloat16 [25088, 512], P(('dp', 'mp'))
- input_grad: bfloat16 [25088, 512], P(('dp', 'mp'))
- param_grad: float32 [8, 394324], P('mp', 'dp')
- new_params: float32 [8, 394324], P('mp', 'dp')
- revised_first_mean: float32 [8, 394324], P('mp', 'dp')
- new_moment_two: float32 [8, 394324], P('mp', 'dp')
The draws below stay inside these ranges and needn't reach their ends.
Inputs may be any that keep to these rules, and one draw needn't show every extreme that they name: `image_counts`: the live images of a group are its first slots; the counts add up to three quarters of all slots, rounded down, and one group is full. `params`: laid out as its meaning says. `moment_two`: Positive, laid out as params.
All inputs are finite; a program needn't handle non-finite values.
Results may differ from the reference program's by a relative error of at most 0.022.
Values may be sent and summed in bfloat16 or wider, within the bound.
A program may use at most 192 MiB of HBM per device.

```python
import math
import jax
import jax.numpy as jnp
import numpy as np
from jax import lax

C = 512
FF = 2048
HD = 32
WIN = 7
MAP = 14
SHIFT = 3
IMG_DEV = 32
PIX = 196
TOKENS = 25088
PAR_RANK = 394324
WEIGHTS_RANK = 393216
N_DP = 4
N_MP = 8


def segment_layout():
    width_rank = C // N_MP
    hidden_rank = FF // N_MP
    heads = width_rank // HD
    span = 2 * WIN - 1
    lengths = [3 * C * width_rank, width_rank * C, C * hidden_rank, hidden_rank * C, width_rank, width_rank, width_rank, width_rank, width_rank, width_rank, width_rank, hidden_rank, width_rank, span * span * heads]
    position = jnp.arange(PAR_RANK, dtype=jnp.int32)[None, :]
    segment = jnp.zeros((1, PAR_RANK), jnp.int32)
    running = 0
    for length in lengths:
        running = running + length
        segment = segment + (position >= running).astype(jnp.int32)
    return segment


def draw_params(key, part):
    keys = jax.random.split(key, 2)
    base = jnp.clip(jax.random.normal(keys[0], (N_MP, PAR_RANK), jnp.float32), -4.0, 4.0)
    spread = jax.random.uniform(keys[1], (N_MP, PAR_RANK), jnp.float32, 0.5, 1.5)
    segment = segment_layout()
    factors = [C ** (-0.5), 4.0 * C ** (-0.5), C ** (-0.5), 1.5 * FF ** (-0.5), 0.0, 0.3, 0.3, 0.3, 0.3, 0.0, 0.3, 0.3, 0.3, 1.0, 0.3]
    scale = jnp.zeros((N_MP, PAR_RANK), jnp.float32)
    for index, factor in enumerate(factors):
        scale = jnp.where(segment == index, factor, scale)
    value = base * scale
    gain_mask = (segment == 4) | (segment == 9)
    return jnp.where(gain_mask, spread, value)


def draw_moment_two(key, part):
    segment = segment_layout()
    grad_scale = [0.3, 1.0, 0.4, 0.5, 1.0, 1.0, 0.3, 0.3, 1.0, 1.0, 1.0, 0.4, 1.0, 0.1, 1.0]
    size = jnp.zeros((N_MP, PAR_RANK), jnp.float32)
    for index, factor in enumerate(grad_scale):
        size = jnp.where(segment == index, factor * factor, size)
    factor_draw = jnp.exp(jax.random.uniform(key, (N_MP, PAR_RANK), jnp.float32, math.log(0.5), math.log(2.0)))
    return 0.001 * 0.75 * TOKENS * size * factor_draw


def block_levels(rng, dims, pieces, smallest, high):
    gain, own = 1.0, jax.random.fold_in(rng, 6)
    for dim, blocks in pieces:
        draws = jnp.exp(jax.random.uniform(jax.random.fold_in(own, dim), (blocks,), jnp.float32, smallest / len(pieces), high / len(pieces)))
        gain = gain * jnp.repeat(draws, dims[dim] // blocks).reshape([-1 if axis == dim else 1 for axis in range(len(dims))])
    return gain


def profile(count, total, most, lean):
    loads = [(1 << 20) // math.isqrt(grade ** lean) + 1 for grade in range(2, count + 1)]
    rest, holding = total - most - (count - 1), [1] * (count - 1)
    while rest > 0:
        free = [i for i in range(count - 1) if holding[i] < most]
        whole, budget = sum([loads[i] for i in free]), rest
        for i in free:
            addition = min(most - holding[i], max(1, budget * loads[i] // whole), rest)
            holding[i] = holding[i] + addition
            rest = rest - addition
    return np.array([most] + holding)


def uneven_parts(key, number_of, total, bound, skew):
    if number_of == 2:
        one = jax.random.randint(key, (), max(1, total - bound), min(bound, total - 1) + 1)
        return jnp.stack([one, total - one])
    sizes = jnp.asarray(profile(number_of, total, bound, skew), jnp.int32)
    pairs = (number_of - 1) // 2
    giver, receiver = sizes[1:1 + 2 * pairs:2], sizes[2:2 + 2 * pairs:2]
    room = jnp.minimum(giver - 1, bound - receiver)
    shifted = jax.random.randint(jax.random.fold_in(key, 1), (pairs,), 0, 1 << 20) % (room + 1)
    sizes = sizes.at[1:1 + 2 * pairs:2].set(giver - shifted).at[2:2 + 2 * pairs:2].set(receiver + shifted)
    return sizes[jax.random.permutation(jax.random.fold_in(key, 2), number_of)]


def gaussian(own_key, shape, deviation, limit, cuts=(), kind=jnp.bfloat16):
    loudness = block_levels(own_key, shape, cuts, -0.22, 0.18) if cuts else 1.0
    drawn = jax.random.normal(own_key, shape, jnp.float32) * deviation * loudness
    return jnp.minimum(jnp.maximum(drawn, -limit), limit).astype(kind)


def setup_inputs(seed: int = 0) -> dict:
    key_list = jax.random.split(jax.random.key(seed), 7)
    tokens = gaussian(key_list[0], (TOKENS, C), 1.0, 6.0, ((0, 32),))
    cotangent = gaussian(key_list[1], (TOKENS, C), 1.0, 6.0, ((0, 32),))
    image_counts = uneven_parts(key_list[2], N_DP, N_DP * IMG_DEV * 3 // 4, IMG_DEV, 2).astype(jnp.int32)
    params = draw_params(jax.random.fold_in(key_list[6], 71), 0)
    moment_one = gaussian(key_list[4], (N_MP, PAR_RANK), (0.1 * TOKENS ** 0.5), 96.0, ((0, 8), (1, 4)), jnp.float32)
    moment_two = draw_moment_two(jax.random.fold_in(key_list[6], 71), 0)
    return {"tokens": tokens, "cotangent": cotangent, "image_counts": image_counts, "params": params, "moment_one": moment_one, "moment_two": moment_two}


norm_eps = 1e-05
mask_fill = -100.0
learn_rate = 0.05
beta_one = 0.9
second_decay_rate = 0.999
adam_eps = 1e-08
weight_decay = 0.05
adam_step = 2.0

def combine_rule(spec, left, right):
    return jnp.einsum(spec, left.astype(jnp.float32), right.astype(jnp.float32))

def segment_shapes(width_rank, hidden_rank):
    span = 2 * WIN - 1
    return [('qkv_weight', (C, 3 * width_rank)), ('proj_weight', (width_rank, C)), ('fc1_weight', (C, hidden_rank)), ('fc2_weight', (hidden_rank, C)), ('norm1_gain', (width_rank,)), ('norm1_bias', (width_rank,)), ('query_bias', (width_rank,)), ('value_bias', (width_rank,)), ('proj_bias', (width_rank,)), ('norm2_gain', (width_rank,)), ('norm2_bias', (width_rank,)), ('fc1_bias', (hidden_rank,)), ('fc2_bias', (width_rank,)), ('table', (span * span, width_rank // HD))]

def unpack(flat, width_rank, hidden_rank):
    groups = flat.shape[0]
    owner_pieces = {}
    offset = 0
    for label, shape in segment_shapes(width_rank, hidden_rank):
        amount = math.prod(shape)
        owner_pieces[label] = flat[:, offset:offset + amount].reshape((groups,) + shape)
        offset = offset + amount
    return owner_pieces

def pack(owner_pieces, width_rank, hidden_rank, length):
    groups = owner_pieces['qkv_weight'].shape[0]
    parts = [owner_pieces[label].reshape(groups, -1) for label, shape in segment_shapes(width_rank, hidden_rank)]
    used = sum((part.shape[1] for part in parts))
    parts.append(jnp.zeros((groups, length - used), jnp.float32))
    return jnp.concatenate(parts, axis=1)

def window_tables():
    side = MAP // WIN
    span = 2 * WIN - 1
    inner = jnp.arange(WIN * WIN, dtype=jnp.int32)
    row_in = inner // WIN
    col_in = inner % WIN
    offset_index = (row_in[:, None] - row_in[None, :] + WIN - 1) * span + (col_in[:, None] - col_in[None, :] + WIN - 1)
    one_hot = (offset_index.reshape(-1)[:, None] == jnp.arange(span * span, dtype=jnp.int32)[None, :]).astype(jnp.float32)
    window_ids = jnp.arange(side * side, dtype=jnp.int32)
    row_coord = (window_ids // side)[:, None] * WIN + row_in[None, :]
    col_coord = (window_ids % side)[:, None] * WIN + col_in[None, :]

    def region(coord):
        return (coord >= MAP - WIN).astype(jnp.int32) + (coord >= MAP - SHIFT).astype(jnp.int32)
    region_ids = region(row_coord) * 3 + region(col_coord)
    mask = jnp.where(region_ids[:, :, None] == region_ids[:, None, :], 0.0, mask_fill).astype(jnp.float32)
    return (one_hot, mask)

def to_windows(raster):
    width = raster.shape[-1]
    side = MAP // WIN
    grid = raster.reshape(-1, MAP, MAP, width)
    grid = jnp.roll(grid, (-SHIFT, -SHIFT), (1, 2))
    grid = grid.reshape(-1, side, WIN, side, WIN, width).transpose(0, 1, 3, 2, 4, 5)
    return grid.reshape(-1, side * side, WIN * WIN, width)

def from_windows(blocks):
    width = blocks.shape[-1]
    side = MAP // WIN
    grid = blocks.reshape(-1, side, side, WIN, WIN, width).transpose(0, 1, 3, 2, 4, 5)
    grid = grid.reshape(-1, MAP, MAP, width)
    grid = jnp.roll(grid, (SHIFT, SHIFT), (1, 2))
    return grid.reshape(-1, width)

def norm_stats(values):
    center = lax.optimization_barrier(jnp.mean(values, axis=1, keepdims=True))
    spread = lax.optimization_barrier(jnp.mean(jnp.square(values - center), axis=1, keepdims=True))
    return (center, lax.rsqrt(spread + norm_eps))

def norm_back(scaled, unit, scale):
    return scale * (scaled - lax.optimization_barrier(jnp.mean(scaled, axis=1, keepdims=True)) - unit * lax.optimization_barrier(jnp.mean(scaled * unit, axis=1, keepdims=True)))

def gelu(values):
    return values * (0.5 * (1.0 + lax.erf(values * (1.0 / math.sqrt(2.0)))))

def gelu_derivative(values):
    cdf = 0.5 * (1.0 + lax.erf(values * (1.0 / math.sqrt(2.0))))
    density = jnp.exp(-0.5 * values * values) * (1.0 / math.sqrt(2.0 * math.pi))
    return cdf + values * density

def qkv_finish(raw, query_bias, value_bias):
    shift = jnp.stack([query_bias, jnp.zeros_like(query_bias), value_bias], axis=1)
    factor = jnp.array([HD ** (-0.5), 1.0, 1.0], jnp.float32)[None, None, :, None]
    return ((raw + shift[None]) * factor).astype(jnp.bfloat16)

def window_scores(blocks, table, one_hot, mask):
    heads = table.shape[1]
    size = WIN * WIN
    bias = jnp.dot(one_hot, table, precision=lax.Precision.HIGHEST).reshape(size, size, heads).transpose(2, 0, 1)
    scores = combine_rule('nwphd,nwqhd->nwhpq', blocks[:, :, :, :, 0, :], blocks[:, :, :, :, 1, :])
    return scores + bias[None, None] + mask[None, :, None]

def attend_forward(projected, table, one_hot, mask):
    heads = table.shape[1]
    blocks = to_windows(projected)
    count, wins = (blocks.shape[0], blocks.shape[1])
    blocks = blocks.reshape(count, wins, WIN * WIN, heads, 3, HD)
    scores = window_scores(blocks, table, one_hot, mask)
    top = lax.optimization_barrier(jnp.max(scores, axis=-1, keepdims=True))
    log_total = top + jnp.log(lax.optimization_barrier(jnp.sum(jnp.exp(scores - top), axis=-1, keepdims=True)))
    soft = jnp.exp(scores - log_total).astype(jnp.bfloat16)
    mixed = combine_rule('nwhpq,nwqhd->nwphd', soft, blocks[:, :, :, :, 2, :]).astype(jnp.bfloat16)
    return (from_windows(mixed.reshape(count, wins, WIN * WIN, heads * HD)), log_total)

def attend_backward(projected, grad_mixed, table, log_total, one_hot, mask):
    heads = table.shape[1]
    size = WIN * WIN
    blocks = to_windows(projected)
    count, wins = (blocks.shape[0], blocks.shape[1])
    blocks = blocks.reshape(count, wins, size, heads, 3, HD)
    scores = window_scores(blocks, table, one_hot, mask)
    soft = jnp.exp(scores - log_total)
    incoming = to_windows(grad_mixed).reshape(count, wins, size, heads, HD)
    grad_value = combine_rule('nwhpq,nwphd->nwqhd', soft.astype(jnp.bfloat16), incoming)
    grad_soft = combine_rule('nwphd,nwqhd->nwhpq', incoming, blocks[:, :, :, :, 2, :])
    inner = lax.optimization_barrier(jnp.sum(soft * grad_soft, axis=-1, keepdims=True))
    grad_scores = soft * (grad_soft - inner)
    grad_bias = lax.optimization_barrier(jnp.sum(grad_scores, axis=(0, 1))).transpose(1, 2, 0).reshape(size * size, heads)
    grad_table = jnp.dot(one_hot.T, grad_bias, precision=lax.Precision.HIGHEST)
    rounded = grad_scores.astype(jnp.bfloat16)
    grad_query = combine_rule('nwhpq,nwqhd->nwphd', rounded, blocks[:, :, :, :, 1, :]) * HD ** (-0.5)
    grad_key = combine_rule('nwhpq,nwphd->nwqhd', rounded, blocks[:, :, :, :, 0, :])
    stacked = jnp.stack([grad_query, grad_key, grad_value], axis=4).reshape(count, wins, size, heads * 3 * HD)
    return (from_windows(stacked), grad_table)

def cluster_totals(spec, left, right):
    parts = combine_rule(spec, left, right).astype(jnp.bfloat16)
    parts = lax.optimization_barrier(parts)
    return lax.optimization_barrier(jnp.sum(parts.astype(jnp.float32), axis=0))

def local_block(tokens, cotangent, live, owner_pieces, one_hot, mask):
    groups = owner_pieces['qkv_weight'].shape[0]
    width_rank = owner_pieces['proj_weight'].shape[1]
    heads = groups * (width_rank // HD)
    rows = tokens.shape[0]

    def linear_entries_arg(label):
        return owner_pieces[label].astype(jnp.float32).reshape(-1)
    live_col = live[:, None]
    inputs = tokens.astype(jnp.float32)
    center1, scale1 = norm_stats(inputs)
    unit1 = (inputs - center1) * scale1
    gain1 = linear_entries_arg('norm1_gain')
    normed1 = (unit1 * gain1 + linear_entries_arg('norm1_bias')).astype(jnp.bfloat16)
    raw = combine_rule('tc,gck->tgk', normed1, owner_pieces['qkv_weight']).reshape(rows, heads, 3, HD)
    projected = qkv_finish(raw, linear_entries_arg('query_bias').reshape(heads, HD), linear_entries_arg('value_bias').reshape(heads, HD))
    projected = projected.reshape(rows, heads * 3 * HD)
    table = owner_pieces['table'].astype(jnp.float32).transpose(1, 0, 2).reshape(-1, heads)
    mixed, log_total = attend_forward(projected, table, one_hot, mask)
    mixed_groups = mixed.reshape(rows, groups, width_rank)
    attended = cluster_totals('tgk,gkc->gtc', mixed_groups, owner_pieces['proj_weight']) + linear_entries_arg('proj_bias')
    residual = inputs + attended
    center2, scale2 = norm_stats(residual)
    unit2 = (residual - center2) * scale2
    gain2 = linear_entries_arg('norm2_gain')
    normed2 = (unit2 * gain2 + linear_entries_arg('norm2_bias')).astype(jnp.bfloat16)
    hidden_before_gelu = combine_rule('tc,gcf->tgf', normed2, owner_pieces['fc1_weight']) + owner_pieces['fc1_bias'].astype(jnp.float32)[None]
    nonlinear_token_list = gelu(hidden_before_gelu).astype(jnp.bfloat16)
    perceptron_result = cluster_totals('ayg,ygj->yaj', nonlinear_token_list, owner_pieces['fc2_weight']) + linear_entries_arg('fc2_bias')
    output = (live_col * (residual + perceptron_result)).astype(jnp.bfloat16)
    grad_out = live_col * cotangent.astype(jnp.float32)
    gradient_low_precision = grad_out.astype(jnp.bfloat16)
    parameter_gradients = {}
    parameter_gradients['fc2_bias'] = lax.optimization_barrier(jnp.sum(grad_out, axis=0)).reshape(groups, width_rank)
    parameter_gradients['fc2_weight'] = combine_rule('abl,ai->bli', nonlinear_token_list, gradient_low_precision)
    gradient_before_gelu = combine_rule('bs,qns->bqn', gradient_low_precision, owner_pieces['fc2_weight']) * gelu_derivative(hidden_before_gelu)
    parameter_gradients['fc1_bias'] = lax.optimization_barrier(jnp.sum(gradient_before_gelu, axis=0))
    preact_rounded = gradient_before_gelu.astype(jnp.bfloat16)
    parameter_gradients['fc1_weight'] = combine_rule('tc,tgf->gcf', normed2, preact_rounded)
    grad_norm2 = cluster_totals('tgf,gcf->gtc', preact_rounded, owner_pieces['fc1_weight'])
    parameter_gradients['norm2_gain'] = lax.optimization_barrier(jnp.sum(grad_norm2 * unit2, axis=0)).reshape(groups, width_rank)
    parameter_gradients['norm2_bias'] = lax.optimization_barrier(jnp.sum(grad_norm2, axis=0)).reshape(groups, width_rank)
    grad_residual = grad_out + norm_back(grad_norm2 * gain2, unit2, scale2)
    parameter_gradients['proj_bias'] = lax.optimization_barrier(jnp.sum(grad_residual, axis=0)).reshape(groups, width_rank)
    residual_rounded = grad_residual.astype(jnp.bfloat16)
    parameter_gradients['proj_weight'] = combine_rule('tgk,tc->gkc', mixed_groups, residual_rounded)
    grad_mixed = combine_rule('tc,gkc->tgk', residual_rounded, owner_pieces['proj_weight']).astype(jnp.bfloat16).reshape(rows, heads * HD)
    grad_projected, grad_table = attend_backward(projected, grad_mixed, table, log_total, one_hot, mask)
    split = grad_projected.reshape(rows, heads, 3, HD)
    parameter_gradients['query_bias'] = lax.optimization_barrier(jnp.sum(split[:, :, 0, :], axis=0)).reshape(groups, width_rank)
    parameter_gradients['value_bias'] = lax.optimization_barrier(jnp.sum(split[:, :, 2, :], axis=0)).reshape(groups, width_rank)
    parameter_gradients['table'] = grad_table.reshape(-1, groups, heads // groups).transpose(1, 0, 2)
    projected_rounded = grad_projected.astype(jnp.bfloat16).reshape(rows, groups, 3 * width_rank)
    parameter_gradients['qkv_weight'] = combine_rule('tc,tgk->gck', normed1, projected_rounded)
    grad_norm1 = cluster_totals('tgk,gck->gtc', projected_rounded, owner_pieces['qkv_weight'])
    parameter_gradients['norm1_gain'] = lax.optimization_barrier(jnp.sum(grad_norm1 * unit1, axis=0)).reshape(groups, width_rank)
    parameter_gradients['norm1_bias'] = lax.optimization_barrier(jnp.sum(grad_norm1, axis=0)).reshape(groups, width_rank)
    grad_input = (grad_residual + norm_back(grad_norm1 * gain1, unit1, scale1)).astype(jnp.bfloat16)
    return (output, grad_input, parameter_gradients)

def reference(tokens, cotangent, image_counts, params, moment_one, moment_two):
    width_rank = C // N_MP
    hidden_rank = FF // N_MP
    owner_pieces = unpack(params.astype(jnp.bfloat16), width_rank, hidden_rank)
    one_hot, mask = window_tables()
    block_rows = N_MP * PIX
    blocks = TOKENS // block_rows
    images = jnp.arange(TOKENS // PIX, dtype=jnp.int32)
    limits = image_counts[images // IMG_DEV]
    live_images = (images % IMG_DEV < limits).astype(jnp.float32)
    live = jnp.repeat(live_images, PIX)
    zero_grads = {label: jnp.zeros((N_MP,) + shape, jnp.float32) for label, shape in segment_shapes(width_rank, hidden_rank)}

    def step(carry, slices):
        block_tokens, block_cot, block_live = slices
        block_out, block_grad, parameter_gradients = local_block(block_tokens, block_cot, block_live, owner_pieces, one_hot, mask)
        carry = jax.tree.map(lambda first, second: first + second, carry, parameter_gradients)
        return (carry, (block_out, block_grad))
    totals, (outs, grad_ins) = lax.scan(step, zero_grads, (tokens.reshape(blocks, block_rows, C), cotangent.reshape(blocks, block_rows, C), live.reshape(blocks, block_rows)))
    output = outs.reshape(TOKENS, C)
    input_grad = grad_ins.reshape(TOKENS, C)
    param_grad = pack(totals, width_rank, hidden_rank, PAR_RANK)
    decays = (jnp.arange(PAR_RANK, dtype=jnp.int32)[None, :] < WEIGHTS_RANK).astype(jnp.float32)
    new_one = beta_one * moment_one + (1.0 - beta_one) * param_grad
    new_two = second_decay_rate * moment_two + (1.0 - second_decay_rate) * param_grad * param_grad
    corrected_one = new_one / (1.0 - beta_one ** adam_step)
    corrected_two = new_two / (1.0 - second_decay_rate ** adam_step)
    new_params = params - learn_rate * (corrected_one / (jnp.sqrt(corrected_two) + adam_eps) + weight_decay * decays * params)
    return (output, input_grad, param_grad, new_params, new_one, new_two)
```

```python
import functools
import math

import jax
import jax.numpy as jnp
import numpy as np
from jax import lax
from jax.experimental import pallas as pl
from jax.experimental.pallas import tpu as pltpu
from jax.sharding import PartitionSpec as P

C = 512
FF = 2048
HD = 32
WIN = 7
MAP = 14
SHIFT = 3
PIX = MAP * MAP
HEADS = C // HD
SEG = 64
GH = 4
NG = HEADS // GH
SIDE = MAP // WIN
NW = SIDE * SIDE
SPAN = 2 * WIN - 1

norm_eps = 1e-05
mask_fill = -100.0
learn_rate = 0.05
beta_one = 0.9
second_decay_rate = 0.999
adam_eps = 1e-08
weight_decay = 0.05
adam_step = 2.0
f32 = jnp.float32
bf16 = jnp.bfloat16


def mm(a, b):
    return lax.dot_general(a, b, (((1,), (0,)), ((), ())), preferred_element_type=f32)


def mm_t(a, b):
    return lax.dot_general(a, b, (((1,), (1,)), ((), ())), preferred_element_type=f32)


def mm_r(a, b):
    return lax.dot_general(a, b, (((0,), (0,)), ((), ())), preferred_element_type=f32)


def norm_stats(values):
    center = jnp.mean(values, axis=1, keepdims=True)
    spread = jnp.mean(jnp.square(values - center), axis=1, keepdims=True)
    return center, lax.rsqrt(spread + norm_eps)


def norm_back(scaled, unit, scale):
    return scale * (
        scaled
        - jnp.mean(scaled, axis=1, keepdims=True)
        - unit * jnp.mean(scaled * unit, axis=1, keepdims=True)
    )


def phi_parts(v):
    z = jnp.abs(v) * (1.0 / math.sqrt(2.0))
    t = 1.0 / (1.0 + 0.3275911 * z)
    poly = t * (
        0.254829592
        + t * (-0.284496736 + t * (1.421413741 + t * (-1.453152027 + t * 1.061405429)))
    )
    e = jnp.exp(-0.5 * v * v)
    tail = 0.5 * poly * e
    return jnp.where(v >= 0, 1.0 - tail, tail), e


def window_sites():
    w = np.arange(NW)[:, None]
    p = np.arange(WIN * WIN)[None, :]
    row = (w // SIDE) * WIN + p // WIN
    col = (w % SIDE) * WIN + p % WIN
    token = ((row + SHIFT) % MAP) * MAP + (col + SHIFT) % MAP

    def region(c):
        return (c >= MAP - WIN).astype(np.int32) + (c >= MAP - SHIFT).astype(np.int32)

    ids = region(row) * 3 + region(col)
    return token, ids


def image_frames(images):
    starts = [PIX * i // 16 * 16 for i in range(images)]
    offsets = [PIX * i - s for i, s in enumerate(starts)]
    length = -(-(PIX + max(offsets)) // 16) * 16
    return starts, offsets, length


def placement(images):
    token, _ = window_sites()
    starts, offsets, length = image_frames(images)
    sel = np.zeros((images, NW * SEG, length), np.float32)
    for i in range(images):
        for w in range(NW):
            sel[i, w * SEG + np.arange(WIN * WIN), token[w] + offsets[i]] = 1.0
    return sel


def score_bias(table):
    size = WIN * WIN
    p = np.arange(size)
    a, b = p // WIN, p % WIN
    off = (a[None, :] - a[:, None] + WIN - 1) * SPAN + b[None, :] - b[:, None] + WIN - 1
    one_hot = np.zeros((size, size, SPAN * SPAN), np.float32)
    one_hot[np.arange(size)[:, None], np.arange(size)[None, :], off] = 1.0
    _, ids = window_sites()
    full_mask = np.full((NW, SEG, SEG), 0.0, np.float32)
    full_mask[:, size:, :] = -1e30
    full_mask[:, :size, :size] = np.where(ids[:, :, None] == ids[:, None, :], 0.0, mask_fill)
    onehot = jnp.asarray(one_hot.reshape(size * size, -1), bf16)
    bias = jnp.dot(table.T.astype(bf16), onehot.T, preferred_element_type=f32)
    bias = bias.reshape(NG, GH, size, size)
    bias = jnp.pad(bias, ((0, 0), (0, 0), (0, SEG - size), (0, SEG - size)))
    bias = bias.transpose(0, 2, 1, 3)
    out = bias[None] + jnp.asarray(full_mask)[:, None, :, None, :]
    return out.reshape(NW * NG, SEG, GH * SEG)


def table_back(acc):
    size = WIN * WIN
    p = np.arange(size)
    a, b = p // WIN, p % WIN
    off = (a[None, :] - a[:, None] + WIN - 1) * SPAN + b[None, :] - b[:, None] + WIN - 1
    one_hot = np.zeros((size * size, SPAN * SPAN), np.float32)
    one_hot[np.arange(size * size), off.reshape(-1)] = 1.0
    acc = acc.reshape(NG, SEG, GH, SEG)[:, :size, :, :size].transpose(0, 2, 1, 3).reshape(HEADS, size * size)
    hi = acc.astype(bf16)
    lo = (acc - hi.astype(f32)).astype(bf16)
    oh = jnp.asarray(one_hot, bf16)
    return (
        jnp.dot(hi, oh, preferred_element_type=f32) + jnp.dot(lo, oh, preferred_element_type=f32)
    ).T


def lane_head_mask():
    return lax.broadcasted_iota(jnp.int32, (SEG, GH * HD), 1) // HD


def block_diag(part, head_of_lane):
    zero = jnp.zeros_like(part)
    return jnp.concatenate([jnp.where(head_of_lane == h, part, zero) for h in range(GH)], axis=0)


def diag_pick(full, head_of_lane):
    out = full[:SEG]
    for h in range(1, GH):
        out = jnp.where(head_of_lane == h, full[h * SEG : (h + 1) * SEG], out)
    return out


def compute_kernel(
    images, rows, block, length,
    nlive, x, cot, wqkv, wproj, w1, w2, vecs, b1, bias, sel,
    out, gin, gqkv_w, gproj_w, g1_w, g2_w, gvec, gb1, acc,
    ln1, qkv, wq, probs, mixw, mixed, ln2, act, gpre, gresb, gres, gmix, gwin,
):
    blocks = rows // block
    frame = image_frames(images)[0]
    head_of_lane = lane_head_mask()

    def vec(i):
        return vecs[i : i + 1, :]

    gvec[...] = jnp.zeros_like(gvec)
    gb1[...] = jnp.zeros_like(gb1)
    acc[...] = jnp.zeros_like(acc)
    mixed[...] = jnp.zeros_like(mixed)

    def norm_rows(t, _):
        sl = pl.ds(pl.multiple_of(t * block, 16), block)
        xin = x[sl, :].astype(f32)
        center, scale = norm_stats(xin)
        normed = ((xin - center) * scale * vec(0) + vec(1)).astype(bf16)
        ln1[sl, :] = normed
        qkv[sl, 0:C] = ((mm_t(normed, wqkv[0:C, :]) + vec(2)) * HD ** (-0.5)).astype(bf16)
        qkv[sl, C : 2 * C] = mm_t(normed, wqkv[C : 2 * C, :]).astype(bf16)
        qkv[sl, 2 * C : 3 * C] = (mm_t(normed, wqkv[2 * C : 3 * C, :]) + vec(3)).astype(bf16)
        return 0

    lax.fori_loop(0, blocks, norm_rows, 0)

    for i in range(images):
        fr = pl.ds(frame[i], length)
        wq[i] = mm(sel[i], qkv[fr, :]).astype(bf16)

        def window(w, _):
            ws = pl.ds(pl.multiple_of(w * SEG, SEG), SEG)
            for g in range(NG):
                q = wq[i, ws, g * 128 : (g + 1) * 128]
                k = wq[i, ws, C + g * 128 : C + (g + 1) * 128]
                v = wq[i, ws, 2 * C + g * 128 : 2 * C + (g + 1) * 128]
                st = mm_t(k, block_diag(q, head_of_lane)) + bias[w * NG + g]
                e = jnp.exp(st - jnp.max(st, axis=0, keepdims=True))
                pt = (e * (1.0 / jnp.sum(e, axis=0, keepdims=True))).astype(bf16)
                probs[i, w * NG + g] = pt
                mixw[ws, g * 128 : (g + 1) * 128] = diag_pick(mm_r(pt, v), head_of_lane).astype(bf16)
            return 0

        lax.fori_loop(0, NW, window, 0)
        mixed[fr, :] = (mixed[fr, :].astype(f32) + mm_r(sel[i], mixw[...])).astype(bf16)

    def middle(t, _):
        sl = pl.ds(pl.multiple_of(t * block, 16), block)
        xin = x[sl, :].astype(f32)
        res = xin + (mm(mixed[sl, :], wproj[...]) + vec(4))
        center, scale = norm_stats(res)
        unit = (res - center) * scale
        normed = (unit * vec(5) + vec(6)).astype(bf16)
        ln2[sl, :] = normed
        live = (
            lax.broadcasted_iota(jnp.int32, (block, 1), 0) + t * block < nlive[0]
        ).astype(f32)
        gout = live * cot[sl, :].astype(f32)
        goutb = gout.astype(bf16)
        feed = jnp.zeros((block, C), f32)
        gln = jnp.zeros((block, C), f32)
        for j in range(4):
            js = slice(j * 512, (j + 1) * 512)
            pre = mm(normed, w1[:, js]) + b1[:, js]
            phi, e = phi_parts(pre)
            av = (pre * phi).astype(bf16)
            act[sl, js] = av
            feed = feed + mm(av, w2[js, :])
            gp = mm_t(goutb, w2[js, :]) * (phi + pre * (e * (1.0 / math.sqrt(2.0 * math.pi))))
            gb1[:, js] += jnp.sum(gp, axis=0, keepdims=True)
            gpb = gp.astype(bf16)
            gpre[sl, js] = gpb
            gln = gln + mm_t(gpb, w1[:, js])
        out[sl, :] = (live * (res + feed + vec(7))).astype(bf16)
        gr = gout + norm_back(gln * vec(5), unit, scale)
        gres[sl, :] = gr
        grb = gr.astype(bf16)
        gresb[sl, :] = grb
        gmix[sl, :] = mm_t(grb, wproj[...]).astype(bf16)
        gvec[4:5, :] += jnp.sum(gr, axis=0, keepdims=True)
        gvec[5:6, :] += jnp.sum(gln * unit, axis=0, keepdims=True)
        gvec[6:7, :] += jnp.sum(gln, axis=0, keepdims=True)
        gvec[7:8, :] += jnp.sum(gout, axis=0, keepdims=True)
        return 0

    lax.fori_loop(0, blocks, middle, 0)

    def masked_cot():
        live = (lax.broadcasted_iota(jnp.int32, (rows, 1), 0) < nlive[0]).astype(bf16)
        return cot[...] * live

    gout_all = masked_cot()

    def ff_grads(j, _):
        js = pl.ds(pl.multiple_of(j * 256, 256), 256)
        g2_w[:, js] = mm_r(gout_all, act[:, js]).astype(g2_w.dtype)
        g1_w[:, js] = mm_r(ln2[...], gpre[:, js]).astype(g1_w.dtype)
        return 0

    lax.fori_loop(0, FF // 256, ff_grads, 0)
    gproj_w[...] = mm_r(mixed[...], gresb[...]).astype(gproj_w.dtype)

    qkv[...] = jnp.zeros_like(qkv)
    for i in range(images):
        fr = pl.ds(frame[i], length)
        mixw[...] = mm(sel[i], gmix[fr, :]).astype(bf16)

        def window(w, _):
            ws = pl.ds(pl.multiple_of(w * SEG, SEG), SEG)
            for g in range(NG):
                q = wq[i, ws, g * 128 : (g + 1) * 128]
                k = wq[i, ws, C + g * 128 : C + (g + 1) * 128]
                v = wq[i, ws, 2 * C + g * 128 : 2 * C + (g + 1) * 128]
                pt = probs[i, w * NG + g]
                dod = block_diag(mixw[ws, g * 128 : (g + 1) * 128], head_of_lane)
                gv = mm(pt, dod)
                dpt = mm_t(v, dod)
                ptf = pt.astype(f32)
                prod = ptf * dpt
                dst = prod - ptf * jnp.sum(prod, axis=0, keepdims=True)
                acc[g] += dst
                dsb = dst.astype(bf16)
                gk = mm(dsb, block_diag(q, head_of_lane))
                gq = diag_pick(mm_r(dsb, k), head_of_lane) * HD ** (-0.5)
                gl = slice(g * 128, (g + 1) * 128)
                gvec[2:3, gl] += jnp.sum(gq, axis=0, keepdims=True)
                gvec[3:4, gl] += jnp.sum(gv, axis=0, keepdims=True)
                gwin[ws, g * 128 : (g + 1) * 128] = gq.astype(bf16)
                gwin[ws, C + g * 128 : C + (g + 1) * 128] = gk.astype(bf16)
                gwin[ws, 2 * C + g * 128 : 2 * C + (g + 1) * 128] = gv.astype(bf16)
            return 0

        lax.fori_loop(0, NW, window, 0)
        qkv[fr, :] = (qkv[fr, :].astype(f32) + mm_r(sel[i], gwin[...])).astype(bf16)

    def last(t, _):
        sl = pl.ds(pl.multiple_of(t * block, 16), block)
        gln = mm(qkv[sl, :], wqkv[...])
        xin = x[sl, :].astype(f32)
        center, scale = norm_stats(xin)
        unit = (xin - center) * scale
        gvec[0:1, :] += jnp.sum(gln * unit, axis=0, keepdims=True)
        gvec[1:2, :] += jnp.sum(gln, axis=0, keepdims=True)
        gin[sl, :] = (gres[sl, :] + norm_back(gln * vec(0), unit, scale)).astype(bf16)
        return 0

    lax.fori_loop(0, blocks, last, 0)

    def qkv_grads(j, _):
        js = pl.ds(pl.multiple_of(j * 256, 256), 256)
        gqkv_w[js, :] = mm_r(qkv[:, js], ln1[...]).astype(gqkv_w.dtype)
        return 0

    lax.fori_loop(0, 3 * C // 256, qkv_grads, 0)


def block_size(rows):
    for cand in (112, 80, 64, 48, 32, 16):
        if rows % cand == 0:
            return cand
    return rows


def block_compute(x, cot, nlive, wqkv, wproj, w1, w2, vecs, b1, bias, interpret=False):
    tokens = x.shape[0]
    images = tokens // PIX
    rows = -(-tokens // 16) * 16
    if rows != tokens:
        x = jnp.pad(x, ((0, rows - tokens), (0, 0)))
        cot = jnp.pad(cot, ((0, rows - tokens), (0, 0)))
    block = block_size(rows)
    starts, _, length = image_frames(images)
    assert starts[-1] + length <= rows
    sel = jnp.asarray(placement(images), bf16)
    vmem = pl.BlockSpec(memory_space=pltpu.VMEM)
    smem = pl.BlockSpec(memory_space=pltpu.SMEM)
    s = jax.ShapeDtypeStruct
    outs = pl.pallas_call(
        functools.partial(compute_kernel, images, rows, block, length),
        out_shape=(
            s((rows, C), bf16),
            s((rows, C), bf16),
            s((3 * C, C), bf16),
            s((C, C), bf16),
            s((C, FF), bf16),
            s((C, FF), bf16),
            s((8, C), f32),
            s((1, FF), f32),
            s((NG, SEG, GH * SEG), f32),
        ),
        in_specs=[smem] + [vmem] * 10,
        out_specs=(vmem,) * 9,
        scratch_shapes=[
            pltpu.VMEM((rows, C), bf16),
            pltpu.VMEM((rows, 3 * C), bf16),
            pltpu.VMEM((images, NW * SEG, 3 * C), bf16),
            pltpu.VMEM((images, NW * NG, SEG, GH * SEG), bf16),
            pltpu.VMEM((NW * SEG, C), bf16),
            pltpu.VMEM((rows, C), bf16),
            pltpu.VMEM((rows, C), bf16),
            pltpu.VMEM((rows, FF), bf16),
            pltpu.VMEM((rows, FF), bf16),
            pltpu.VMEM((rows, C), bf16),
            pltpu.VMEM((rows, C), f32),
            pltpu.VMEM((rows, C), bf16),
            pltpu.VMEM((NW * SEG, 3 * C), bf16),
        ],
        compiler_params=pltpu.CompilerParams(vmem_limit_bytes=60 * 1024 * 1024),
        interpret=interpret,
    )(nlive, x, cot, wqkv, wproj, w1, w2, vecs, b1, bias, sel)
    return (outs[0][:tokens], outs[1][:tokens]) + outs[2:]


VEC_LABELS = [
    "norm1_gain",
    "norm1_bias",
    "query_bias",
    "value_bias",
    "proj_bias",
    "norm2_gain",
    "norm2_bias",
    "fc2_bias",
]


def segment_shapes(width_rank, hidden_rank):
    return [
        ("qkv_weight", (C, 3 * width_rank)),
        ("proj_weight", (width_rank, C)),
        ("fc1_weight", (C, hidden_rank)),
        ("fc2_weight", (hidden_rank, C)),
        ("norm1_gain", (width_rank,)),
        ("norm1_bias", (width_rank,)),
        ("query_bias", (width_rank,)),
        ("value_bias", (width_rank,)),
        ("proj_bias", (width_rank,)),
        ("norm2_gain", (width_rank,)),
        ("norm2_bias", (width_rank,)),
        ("fc1_bias", (hidden_rank,)),
        ("fc2_bias", (width_rank,)),
        ("table", (SPAN * SPAN, width_rank // HD)),
    ]


def unpack(flat, width_rank, hidden_rank):
    pieces = {}
    offset = 0
    for label, shape in segment_shapes(width_rank, hidden_rank):
        amount = math.prod(shape)
        pieces[label] = flat[:, offset : offset + amount].reshape((flat.shape[0],) + shape)
        offset = offset + amount
    return pieces


def local(tokens, cotangent, image_counts, params, moment_one, moment_two):
    ranks = lax.axis_size("mp")
    rank = lax.axis_index("mp")
    group = lax.axis_index("dp")
    width = C // ranks
    hidden = FF // ranks
    heads = width // HD
    rows = tokens.shape[0]
    shard_length = params.shape[1]
    length = shard_length * lax.axis_size("dp")
    owned = lax.all_gather(params.astype(bf16), "mp", axis=0, tiled=True)
    owned = lax.all_gather(owned, "dp", axis=1, tiled=True)
    op = unpack(owned, width, hidden)
    wqkv = op["qkv_weight"].reshape(ranks, C, heads, 3, HD).transpose(3, 0, 2, 4, 1).reshape(3 * C, C)
    wproj = op["proj_weight"].reshape(C, C)
    w1 = op["fc1_weight"].transpose(1, 0, 2).reshape(C, FF)
    w2 = op["fc2_weight"].reshape(FF, C)
    vecs = jnp.stack([op[n].reshape(C) for n in VEC_LABELS]).astype(f32)
    b1 = op["fc1_bias"].reshape(1, FF).astype(f32)
    bias = score_bias(op["table"].transpose(1, 0, 2).reshape(-1, HEADS))
    limit = jnp.sum(
        jnp.where(jnp.arange(image_counts.shape[0], dtype=jnp.int32) == group, image_counts, 0)
    )
    nlive = jnp.clip(limit * PIX - rank * rows, 0, rows).reshape(1)
    output, grad_input, gqkv, gproj, g1, g2, gvec, gb1, acc = block_compute(
        tokens, cotangent, nlive, wqkv, wproj, w1, w2, vecs, b1, bias
    )
    gtable = table_back(acc)
    gvec = gvec.reshape(8, ranks, width)
    pieces = [
        gqkv.reshape(3, ranks, heads, HD, C).transpose(1, 4, 2, 0, 3).reshape(ranks, -1),
        gproj.reshape(ranks, -1),
        g1.reshape(C, ranks, hidden).transpose(1, 0, 2).reshape(ranks, -1),
        g2.T.reshape(ranks, -1),
    ]
    pieces += [gvec[i].astype(bf16) for i in range(7)]
    pieces += [gb1.reshape(ranks, hidden).astype(bf16), gvec[7].astype(bf16)]
    pieces += [gtable.reshape(-1, ranks, heads).transpose(1, 0, 2).reshape(ranks, -1).astype(bf16)]
    used = sum(p.shape[1] for p in pieces)
    pieces.append(jnp.zeros((ranks, length - used), bf16))
    flat = jnp.concatenate(pieces, axis=1)
    flat = lax.psum_scatter(flat, "mp", scatter_dimension=0, tiled=True)
    grad_shard = lax.psum_scatter(flat, "dp", scatter_dimension=1, tiled=True).astype(f32)
    weights_rank = (4 * C * C + 2 * C * FF) // ranks
    position = group * shard_length + jnp.arange(shard_length, dtype=jnp.int32)[None, :]
    decays = (position < weights_rank).astype(jnp.float32)
    new_one = beta_one * moment_one + (1.0 - beta_one) * grad_shard
    new_two = second_decay_rate * moment_two + (1.0 - second_decay_rate) * grad_shard * grad_shard
    corrected_one = new_one / (1.0 - beta_one**adam_step)
    corrected_two = new_two / (1.0 - second_decay_rate**adam_step)
    new_params = params - learn_rate * (
        corrected_one / (jnp.sqrt(corrected_two) + adam_eps) + weight_decay * decays * params
    )
    return (output, grad_input, grad_shard, new_params, new_one, new_two)


def solution(mesh):
    return jax.shard_map(
        local,
        mesh=mesh,
        in_specs=(
            P(("dp", "mp"), None),
            P(("dp", "mp"), None),
            P(),
            P("mp", "dp"),
            P("mp", "dp"),
            P("mp", "dp"),
        ),
        out_specs=(
            P(("dp", "mp"), None),
            P(("dp", "mp"), None),
            P("mp", "dp"),
            P("mp", "dp"),
            P("mp", "dp"),
            P("mp", "dp"),
        ),
        check_vma=False,
    )
```

```python
import functools
import math

import jax
import jax.numpy as jnp
import numpy as np
from jax import lax
from jax.experimental import pallas as pl
from jax.experimental.pallas import tpu as pltpu
from jax.sharding import PartitionSpec as P

C = 512
FF = 2048
HD = 32
WIN = 7
MAP = 14
SHIFT = 3
PIX = MAP * MAP
HEADS = C // HD
SEG = 64
GH = 4
NG = HEADS // GH
SIDE = MAP // WIN
NW = SIDE * SIDE
SPAN = 2 * WIN - 1

norm_eps = 1e-05
mask_fill = -100.0
learn_rate = 0.05
beta_one = 0.9
second_decay_rate = 0.999
adam_eps = 1e-08
weight_decay = 0.05
adam_step = 2.0
f32 = jnp.float32
bf16 = jnp.bfloat16


def mm(a, b):
    return lax.dot_general(a, b, (((1,), (0,)), ((), ())), preferred_element_type=f32)


def mm_t(a, b):
    return lax.dot_general(a, b, (((1,), (1,)), ((), ())), preferred_element_type=f32)


def mm_r(a, b):
    return lax.dot_general(a, b, (((0,), (0,)), ((), ())), preferred_element_type=f32)


def norm_stats(values):
    center = jnp.mean(values, axis=1, keepdims=True)
    spread = jnp.mean(jnp.square(values - center), axis=1, keepdims=True)
    return center, lax.rsqrt(spread + norm_eps)


def norm_back(scaled, unit, scale):
    return scale * (
        scaled
        - jnp.mean(scaled, axis=1, keepdims=True)
        - unit * jnp.mean(scaled * unit, axis=1, keepdims=True)
    )


def phi_parts(v):
    z = jnp.abs(v) * (1.0 / math.sqrt(2.0))
    t = 1.0 / (1.0 + 0.3275911 * z)
    poly = t * (
        0.254829592
        + t * (-0.284496736 + t * (1.421413741 + t * (-1.453152027 + t * 1.061405429)))
    )
    e = jnp.exp(-0.5 * v * v)
    tail = 0.5 * poly * e
    return jnp.where(v >= 0, 1.0 - tail, tail), e


def window_sites():
    w = np.arange(NW)[:, None]
    p = np.arange(WIN * WIN)[None, :]
    row = (w // SIDE) * WIN + p // WIN
    col = (w % SIDE) * WIN + p % WIN
    token = ((row + SHIFT) % MAP) * MAP + (col + SHIFT) % MAP

    def region(c):
        return (c >= MAP - WIN).astype(np.int32) + (c >= MAP - SHIFT).astype(np.int32)

    ids = region(row) * 3 + region(col)
    return token, ids


def image_frames(images):
    starts = [PIX * i // 16 * 16 for i in range(images)]
    offsets = [PIX * i - s for i, s in enumerate(starts)]
    length = -(-(PIX + max(offsets)) // 16) * 16
    return starts, offsets, length


def placement(images):
    token, _ = window_sites()
    starts, offsets, length = image_frames(images)
    sel = np.zeros((images, NW * SEG, length), np.float32)
    for i in range(images):
        for w in range(NW):
            sel[i, w * SEG + np.arange(WIN * WIN), token[w] + offsets[i]] = 1.0
    return sel


def score_bias(table):
    size = WIN * WIN
    p = np.arange(size)
    a, b = p // WIN, p % WIN
    off = (a[None, :] - a[:, None] + WIN - 1) * SPAN + b[None, :] - b[:, None] + WIN - 1
    one_hot = np.zeros((size, size, SPAN * SPAN), np.float32)
    one_hot[np.arange(size)[:, None], np.arange(size)[None, :], off] = 1.0
    _, ids = window_sites()
    full_mask = np.full((NW, SEG, SEG), 0.0, np.float32)
    full_mask[:, size:, :] = -1e30
    full_mask[:, :size, :size] = np.where(ids[:, :, None] == ids[:, None, :], 0.0, mask_fill)
    onehot = jnp.asarray(one_hot.reshape(size * size, -1), bf16)
    bias = jnp.dot(table.T.astype(bf16), onehot.T, preferred_element_type=f32)
    bias = bias.reshape(NG, GH, size, size)
    bias = jnp.pad(bias, ((0, 0), (0, 0), (0, SEG - size), (0, SEG - size)))
    bias = bias.transpose(0, 2, 1, 3)
    out = bias[None] + jnp.asarray(full_mask)[:, None, :, None, :]
    return out.reshape(NW * NG, SEG, GH * SEG)


def table_back(acc):
    size = WIN * WIN
    p = np.arange(size)
    a, b = p // WIN, p % WIN
    off = (a[None, :] - a[:, None] + WIN - 1) * SPAN + b[None, :] - b[:, None] + WIN - 1
    one_hot = np.zeros((size * size, SPAN * SPAN), np.float32)
    one_hot[np.arange(size * size), off.reshape(-1)] = 1.0
    acc = acc.reshape(NG, SEG, GH, SEG)[:, :size, :, :size].transpose(0, 2, 1, 3).reshape(HEADS, size * size)
    hi = acc.astype(bf16)
    lo = (acc - hi.astype(f32)).astype(bf16)
    oh = jnp.asarray(one_hot, bf16)
    return (
        jnp.dot(hi, oh, preferred_element_type=f32) + jnp.dot(lo, oh, preferred_element_type=f32)
    ).T


def lane_head_mask():
    return lax.broadcasted_iota(jnp.int32, (SEG, GH * HD), 1) // HD


def block_diag(part, head_of_lane):
    zero = jnp.zeros_like(part)
    return jnp.concatenate([jnp.where(head_of_lane == h, part, zero) for h in range(GH)], axis=0)


def diag_pick(full, head_of_lane):
    out = full[:SEG]
    for h in range(1, GH):
        out = jnp.where(head_of_lane == h, full[h * SEG : (h + 1) * SEG], out)
    return out


def compute_kernel(
    images, rows, block, length,
    nlive, x, cot, wqkv, wproj, w1, w2, vecs, b1, bias, sel,
    out, gin, gqkv_w, gproj_w, g1_w, g2_w, gvec, gb1, acc,
    ln1, qkv, wq, probs, mixw, mixed, ln2, act, gpre, gresb, gres, gmix, gwin,
):
    blocks = rows // block
    frame = image_frames(images)[0]
    head_of_lane = lane_head_mask()

    def vec(i):
        return vecs[i : i + 1, :]

    gvec[...] = jnp.zeros_like(gvec)
    gb1[...] = jnp.zeros_like(gb1)
    acc[...] = jnp.zeros_like(acc)
    mixed[...] = jnp.zeros_like(mixed)

    def norm_rows(t, _):
        sl = pl.ds(pl.multiple_of(t * block, 16), block)
        xin = x[sl, :].astype(f32)
        center, scale = norm_stats(xin)
        normed = ((xin - center) * scale * vec(0) + vec(1)).astype(bf16)
        ln1[sl, :] = normed
        qkv[sl, 0:C] = ((mm_t(normed, wqkv[0:C, :]) + vec(2)) * HD ** (-0.5)).astype(bf16)
        qkv[sl, C : 2 * C] = mm_t(normed, wqkv[C : 2 * C, :]).astype(bf16)
        qkv[sl, 2 * C : 3 * C] = (mm_t(normed, wqkv[2 * C : 3 * C, :]) + vec(3)).astype(bf16)
        return 0

    lax.fori_loop(0, blocks, norm_rows, 0)

    for i in range(images):
        fr = pl.ds(frame[i], length)
        wq[i] = mm(sel[i], qkv[fr, :]).astype(bf16)

        def window(w, _):
            ws = pl.ds(pl.multiple_of(w * SEG, SEG), SEG)
            for g in range(NG):
                q = wq[i, ws, g * 128 : (g + 1) * 128]
                k = wq[i, ws, C + g * 128 : C + (g + 1) * 128]
                v = wq[i, ws, 2 * C + g * 128 : 2 * C + (g + 1) * 128]
                st = mm_t(k, block_diag(q, head_of_lane)) + bias[w * NG + g]
                e = jnp.exp(st - jnp.max(st, axis=0, keepdims=True))
                pt = (e * (1.0 / jnp.sum(e, axis=0, keepdims=True))).astype(bf16)
                probs[i, w * NG + g] = pt
                mixw[ws, g * 128 : (g + 1) * 128] = diag_pick(mm_r(pt, v), head_of_lane).astype(bf16)
            return 0

        lax.fori_loop(0, NW, window, 0)
        mixed[fr, :] = (mixed[fr, :].astype(f32) + mm_r(sel[i], mixw[...])).astype(bf16)

    def middle(t, _):
        sl = pl.ds(pl.multiple_of(t * block, 16), block)
        xin = x[sl, :].astype(f32)
        res = xin + (mm(mixed[sl, :], wproj[...]) + vec(4))
        center, scale = norm_stats(res)
        unit = (res - center) * scale
        normed = (unit * vec(5) + vec(6)).astype(bf16)
        ln2[sl, :] = normed
        live = (
            lax.broadcasted_iota(jnp.int32, (block, 1), 0) + t * block < nlive[0]
        ).astype(f32)
        gout = live * cot[sl, :].astype(f32)
        goutb = gout.astype(bf16)
        feed = jnp.zeros((block, C), f32)
        gln = jnp.zeros((block, C), f32)
        for j in range(4):
            js = slice(j * 512, (j + 1) * 512)
            pre = mm(normed, w1[:, js]) + b1[:, js]
            phi, e = phi_parts(pre)
            av = (pre * phi).astype(bf16)
            act[sl, js] = av
            feed = feed + mm(av, w2[js, :])
            gp = mm_t(goutb, w2[js, :]) * (phi + pre * (e * (1.0 / math.sqrt(2.0 * math.pi))))
            gb1[:, js] += jnp.sum(gp, axis=0, keepdims=True)
            gpb = gp.astype(bf16)
            gpre[sl, js] = gpb
            gln = gln + mm_t(gpb, w1[:, js])
        out[sl, :] = (live * (res + feed + vec(7))).astype(bf16)
        gr = gout + norm_back(gln * vec(5), unit, scale)
        gres[sl, :] = gr
        grb = gr.astype(bf16)
        gresb[sl, :] = grb
        gmix[sl, :] = mm_t(grb, wproj[...]).astype(bf16)
        gvec[4:5, :] += jnp.sum(gr, axis=0, keepdims=True)
        gvec[5:6, :] += jnp.sum(gln * unit, axis=0, keepdims=True)
        gvec[6:7, :] += jnp.sum(gln, axis=0, keepdims=True)
        gvec[7:8, :] += jnp.sum(gout, axis=0, keepdims=True)
        return 0

    lax.fori_loop(0, blocks, middle, 0)

    def masked_cot():
        live = (lax.broadcasted_iota(jnp.int32, (rows, 1), 0) < nlive[0]).astype(bf16)
        return cot[...] * live

    gout_all = masked_cot()

    def ff_grads(j, _):
        js = pl.ds(pl.multiple_of(j * 256, 256), 256)
        g2_w[:, js] = mm_r(gout_all, act[:, js]).astype(g2_w.dtype)
        g1_w[:, js] = mm_r(ln2[...], gpre[:, js]).astype(g1_w.dtype)
        return 0

    lax.fori_loop(0, FF // 256, ff_grads, 0)
    gproj_w[...] = mm_r(mixed[...], gresb[...]).astype(gproj_w.dtype)

    qkv[...] = jnp.zeros_like(qkv)
    for i in range(images):
        fr = pl.ds(frame[i], length)
        mixw[...] = mm(sel[i], gmix[fr, :]).astype(bf16)

        def window(w, _):
            ws = pl.ds(pl.multiple_of(w * SEG, SEG), SEG)
            for g in range(NG):
                q = wq[i, ws, g * 128 : (g + 1) * 128]
                k = wq[i, ws, C + g * 128 : C + (g + 1) * 128]
                v = wq[i, ws, 2 * C + g * 128 : 2 * C + (g + 1) * 128]
                pt = probs[i, w * NG + g]
                dod = block_diag(mixw[ws, g * 128 : (g + 1) * 128], head_of_lane)
                gv = mm(pt, dod)
                dpt = mm_t(v, dod)
                ptf = pt.astype(f32)
                prod = ptf * dpt
                dst = prod - ptf * jnp.sum(prod, axis=0, keepdims=True)
                acc[g] += dst
                dsb = dst.astype(bf16)
                gk = mm(dsb, block_diag(q, head_of_lane))
                gq = diag_pick(mm_r(dsb, k), head_of_lane) * HD ** (-0.5)
                gl = slice(g * 128, (g + 1) * 128)
                gvec[2:3, gl] += jnp.sum(gq, axis=0, keepdims=True)
                gvec[3:4, gl] += jnp.sum(gv, axis=0, keepdims=True)
                gwin[ws, g * 128 : (g + 1) * 128] = gq.astype(bf16)
                gwin[ws, C + g * 128 : C + (g + 1) * 128] = gk.astype(bf16)
                gwin[ws, 2 * C + g * 128 : 2 * C + (g + 1) * 128] = gv.astype(bf16)
            return 0

        lax.fori_loop(0, NW, window, 0)
        qkv[fr, :] = (qkv[fr, :].astype(f32) + mm_r(sel[i], gwin[...])).astype(bf16)

    def last(t, _):
        sl = pl.ds(pl.multiple_of(t * block, 16), block)
        gln = mm(qkv[sl, :], wqkv[...])
        xin = x[sl, :].astype(f32)
        center, scale = norm_stats(xin)
        unit = (xin - center) * scale
        gvec[0:1, :] += jnp.sum(gln * unit, axis=0, keepdims=True)
        gvec[1:2, :] += jnp.sum(gln, axis=0, keepdims=True)
        gin[sl, :] = (gres[sl, :] + norm_back(gln * vec(0), unit, scale)).astype(bf16)
        return 0

    lax.fori_loop(0, blocks, last, 0)

    def qkv_grads(j, _):
        js = pl.ds(pl.multiple_of(j * 256, 256), 256)
        gqkv_w[js, :] = mm_r(qkv[:, js], ln1[...]).astype(gqkv_w.dtype)
        return 0

    lax.fori_loop(0, 3 * C // 256, qkv_grads, 0)


def block_size(rows):
    for cand in (112, 80, 64, 48, 32, 16):
        if rows % cand == 0:
            return cand
    return rows


def block_compute(x, cot, nlive, wqkv, wproj, w1, w2, vecs, b1, bias, interpret=False):
    tokens = x.shape[0]
    images = tokens // PIX
    rows = -(-tokens // 16) * 16
    if rows != tokens:
        x = jnp.pad(x, ((0, rows - tokens), (0, 0)))
        cot = jnp.pad(cot, ((0, rows - tokens), (0, 0)))
    block = block_size(rows)
    starts, _, length = image_frames(images)
    assert starts[-1] + length <= rows
    sel = jnp.asarray(placement(images), bf16)
    vmem = pl.BlockSpec(memory_space=pltpu.VMEM)
    smem = pl.BlockSpec(memory_space=pltpu.SMEM)
    s = jax.ShapeDtypeStruct
    outs = pl.pallas_call(
        functools.partial(compute_kernel, images, rows, block, length),
        out_shape=(
            s((rows, C), bf16),
            s((rows, C), bf16),
            s((3 * C, C), bf16),
            s((C, C), bf16),
            s((C, FF), bf16),
            s((C, FF), bf16),
            s((8, C), f32),
            s((1, FF), f32),
            s((NG, SEG, GH * SEG), f32),
        ),
        in_specs=[smem] + [vmem] * 10,
        out_specs=(vmem,) * 9,
        scratch_shapes=[
            pltpu.VMEM((rows, C), bf16),
            pltpu.VMEM((rows, 3 * C), bf16),
            pltpu.VMEM((images, NW * SEG, 3 * C), bf16),
            pltpu.VMEM((images, NW * NG, SEG, GH * SEG), bf16),
            pltpu.VMEM((NW * SEG, C), bf16),
            pltpu.VMEM((rows, C), bf16),
            pltpu.VMEM((rows, C), bf16),
            pltpu.VMEM((rows, FF), bf16),
            pltpu.VMEM((rows, FF), bf16),
            pltpu.VMEM((rows, C), bf16),
            pltpu.VMEM((rows, C), f32),
            pltpu.VMEM((rows, C), bf16),
            pltpu.VMEM((NW * SEG, 3 * C), bf16),
        ],
        compiler_params=pltpu.CompilerParams(vmem_limit_bytes=60 * 1024 * 1024),
        interpret=interpret,
    )(nlive, x, cot, wqkv, wproj, w1, w2, vecs, b1, bias, sel)
    return (outs[0][:tokens], outs[1][:tokens]) + outs[2:]

LINES = 4
MPS = 8
DPS = 4
QROWS = 384
QUART = QROWS * 256
FLAT = 776
MESH = pl.DeviceIdType.MESH


def base_of(p):
    return (p // WIN) * SPAN + p % WIN


def iota(shape, dim):
    return lax.broadcasted_iota(jnp.int32, shape, dim)


def as_bf(mask):
    return jnp.where(mask, 1.0, 0.0).astype(bf16)


def spread_queries():
    row = iota((GH * 256, GH * SEG), 0)
    lane = iota((GH * 256, GH * SEG), 1)
    q = lane % SEG
    return as_bf((row // 256 == lane // SEG) & (row % 256 == base_of(q)) & (q < WIN * WIN))


def key_rows(reverse):
    k = iota((SEG, 8 * WIN), 0)
    row = iota((SEG, 8 * WIN), 1)
    b = WIN - 1 - k % WIN if reverse else k % WIN
    return as_bf((row == (k // WIN) * 8 + b) & (k < WIN * WIN))


def table_lanes():
    row = iota((384, 512), 0)
    lane = iota((384, 512), 1)
    return as_bf((row == 2 * (lane % 256) + lane // 256) & (lane % 256 < SPAN * SPAN))


def split_mm(op, exact, value):
    hi = value.astype(bf16)
    lo = (value - hi.astype(f32)).astype(bf16)
    return op(exact, hi) + op(exact, lo)


def split_mm_left(op, value, exact):
    hi = value.astype(bf16)
    lo = (value - hi.astype(f32)).astype(bf16)
    return op(hi, exact) + op(lo, exact)


def turn_rows(part):
    return pltpu.roll(part, 0, 1, stride=1, stride_axis=0)


def gather_smalls(sm, vecs, b1, tabs, bias, mask):
    lane = iota((16, 128), 1)
    low = lane < 64
    for g in range(4):
        first, second = sm[2 * g].astype(f32), sm[2 * g + 1].astype(f32)
        turned = [pltpu.roll(first, 64, 1), pltpu.roll(second, 64, 1)]
        los = jnp.where(low, first, turned[1])
        his = jnp.where(low, turned[0], second)
        gl = slice(g * 128, (g + 1) * 128)
        for i, src, row in (
            (0, los, 0), (1, his, 0), (2, los, 1), (3, his, 1), (4, los, 2), (5, his, 2), (6, los, 3), (7, his, 5),
        ):
            vecs[i : i + 1, gl] = src[row : row + 1]
        for k in range(2):
            r = 2 * g + k
            full = (first, second)[k]
            rot = turned[k]
            b1[:, r * 256 : r * 256 + 128] = jnp.where(low[:1], rot[3:4], rot[4:5])
            b1[:, r * 256 + 128 : r * 256 + 256] = jnp.where(low[:1], rot[4:5], rot[5:6])
            for j in range(3):
                tabs[r : r + 1, j * 128 : (j + 1) * 128] = full[6 + j : 7 + j]
    tab = mm(tabs[...].astype(bf16), table_lanes())
    spread = spread_queries()
    keys = key_rows(False)
    for g in range(NG):
        parts = []
        for h in range(GH):
            r, i = divmod(g * GH + h, 2)
            t = jnp.broadcast_to(tab[r : r + 1, i * 256 : (i + 1) * 256], (8, 256))
            rows = [
                turn_rows(pltpu.roll(t, (SPAN * a - 84) % 256, 1)) for a in range(WIN)
            ]
            parts.append(jnp.concatenate(rows, axis=0))
        line = jnp.concatenate(parts, axis=1).astype(bf16)
        placed = mm(line, spread).astype(bf16)
        bt = mm(keys, placed)
        for w in range(NW):
            bias[w * NG + g] = bt + mask[w]


def scatter_smalls(gvec, gb1, acc, gsm, tabs):
    lane = iota((1, 128), 1)
    low = lane < 64
    spread = spread_queries()
    keys = key_rows(True)
    tabs[...] = jnp.zeros_like(tabs)
    for g in range(NG):
        z = split_mm(mm_r, keys, acc[g])
        y = split_mm_left(mm_t, z, spread)
        for h in range(GH):
            r, i = divmod(g * GH + h, 2)
            total = jnp.zeros((8, 256), f32)
            for a in range(WIN):
                part = y[8 * a : 8 * a + 8, h * 256 : (h + 1) * 256]
                total = total + turn_rows(pltpu.roll(part, (78 - SPAN * a) % 256, 1))
            tabs[r : r + 1, i * 256 : (i + 1) * 256] = jnp.sum(total, axis=0, keepdims=True)
    flat = split_mm_left(mm_t, tabs[...], table_lanes())

    def half(i, r):
        g, k = divmod(r, 2)
        v = gvec[i : i + 1, g * 128 : (g + 1) * 128]
        turned = pltpu.roll(v, 64, 1)
        return (v, turned) if k == 0 else (turned, v)

    zero = jnp.zeros((1, 128), f32)
    for r in range(MPS):
        fb0 = gb1[:, r * 256 : r * 256 + 128]
        fb1 = gb1[:, r * 256 + 128 : r * 256 + 256]
        t0, t1 = pltpu.roll(fb0, 64, 1), pltpu.roll(fb1, 64, 1)
        rows = [
            jnp.where(low, half(0, r)[0], half(1, r)[1]),
            jnp.where(low, half(2, r)[0], half(3, r)[1]),
            jnp.where(low, half(4, r)[0], half(5, r)[1]),
            jnp.where(low, half(6, r)[0], t0),
            jnp.where(low, t0, t1),
            jnp.where(low, t1, half(7, r)[1]),
        ]
        for j, row in enumerate(rows):
            gsm[r, j : j + 1, :] = row
        for j in range(3):
            gsm[r, 6 + j : 7 + j, :] = flat[r : r + 1, j * 128 : (j + 1) * 128]
        for j in range(9, 16):
            gsm[r, j : j + 1, :] = zero


def slot(m, d):
    return m * DPS + d


def w_qkv(wb, kind, quad, half):
    return jnp.concatenate(
        [wb[slot(4 * quad + r, 0), half * 192 + kind * 64 : half * 192 + kind * 64 + 64, :] for r in range(4)], axis=0
    )


def w_proj(wb, quad, half):
    return jnp.concatenate([wb[slot(4 * quad + r, 1), half * 64 : half * 64 + 64, :] for r in range(4)], axis=0)


def w_one(wb, r, half):
    return wb[slot(r, 1), 128:384, :] if half == 0 else wb[slot(r, 2), 0:256, :]


def w_two(wb, r, half):
    return jnp.concatenate(
        [
            wb[slot(r, 2), 256 + half * 64 : 256 + half * 64 + 64, :],
            wb[slot(r, 3), half * 192 : half * 192 + 192, :],
        ],
        axis=0,
    )


HALVES = (slice(0, 256), slice(256, 512))


def mega_compute(images, rows, block, length, live_rows, x, cot, wb, vecs, b1, bias, sel, out, gin, gb, gvec, gb1, acc, sc):
    blocks = rows // block
    frame = image_frames(images)[0]
    head_of_lane = lane_head_mask()
    ln1, qkv, wq, probs, mixw, mixed, ln2, act, gpre, gresb, gres, gmix, gwin, goutb = sc

    def vec(i):
        return vecs[i : i + 1, :]

    gvec[...] = jnp.zeros_like(gvec)
    gb1[...] = jnp.zeros_like(gb1)
    acc[...] = jnp.zeros_like(acc)
    mixed[...] = jnp.zeros_like(mixed)

    def norm_rows(t, _):
        sl = pl.ds(pl.multiple_of(t * block, 16), block)
        xin = x[sl, :].astype(f32)
        center, scale = norm_stats(xin)
        normed = ((xin - center) * scale * vec(0) + vec(1)).astype(bf16)
        ln1[sl, :] = normed
        for kind in range(3):
            for quad in range(2):
                cols = slice(kind * C + quad * 256, kind * C + quad * 256 + 256)
                val = mm_t(normed[:, HALVES[0]], w_qkv(wb, kind, quad, 0)) + mm_t(
                    normed[:, HALVES[1]], w_qkv(wb, kind, quad, 1)
                )
                qs = slice(quad * 256, quad * 256 + 256)
                if kind == 0:
                    val = (val + vecs[2:3, qs]) * HD ** (-0.5)
                if kind == 2:
                    val = val + vecs[3:4, qs]
                qkv[sl, cols] = val.astype(bf16)
        return 0

    lax.fori_loop(0, blocks, norm_rows, 0)

    for i in range(images):
        fr = pl.ds(frame[i], length)
        wq[i] = mm(sel[i], qkv[fr, :]).astype(bf16)

        def window(w, _):
            ws = pl.ds(pl.multiple_of(w * SEG, SEG), SEG)
            for g in range(NG):
                q = wq[i, ws, g * 128 : (g + 1) * 128]
                k = wq[i, ws, C + g * 128 : C + (g + 1) * 128]
                v = wq[i, ws, 2 * C + g * 128 : 2 * C + (g + 1) * 128]
                st = mm_t(k, block_diag(q, head_of_lane)) + bias[w * NG + g]
                e = jnp.exp(st - jnp.max(st, axis=0, keepdims=True))
                pt = (e * (1.0 / jnp.sum(e, axis=0, keepdims=True))).astype(bf16)
                probs[i, w * NG + g] = pt
                mixw[ws, g * 128 : (g + 1) * 128] = diag_pick(mm_r(pt, v), head_of_lane).astype(bf16)
            return 0

        lax.fori_loop(0, NW, window, 0)
        mixed[fr, :] = (mixed[fr, :].astype(f32) + mm_r(sel[i], mixw[...])).astype(bf16)

    def middle(t, _):
        sl = pl.ds(pl.multiple_of(t * block, 16), block)
        xin = x[sl, :].astype(f32)
        att = [
            mm(mixed[sl, HALVES[0]], w_proj(wb, 0, h)) + mm(mixed[sl, HALVES[1]], w_proj(wb, 1, h)) for h in range(2)
        ]
        res = xin + (jnp.concatenate(att, axis=1) + vec(4))
        center, scale = norm_stats(res)
        unit = (res - center) * scale
        normed = (unit * vec(5) + vec(6)).astype(bf16)
        ln2[sl, :] = normed
        live = (iota((block, 1), 0) + t * block < live_rows).astype(f32)
        gout = live * cot[sl, :].astype(f32)
        gob = gout.astype(bf16)
        goutb[sl, :] = gob
        feed = [jnp.zeros((block, 256), f32)] * 2
        gln = [jnp.zeros((block, 256), f32)] * 2
        for r in range(MPS):
            js = slice(r * 256, (r + 1) * 256)
            pre = mm(normed[:, HALVES[0]], w_one(wb, r, 0)) + mm(normed[:, HALVES[1]], w_one(wb, r, 1)) + b1[:, js]
            phi, e = phi_parts(pre)
            av = (pre * phi).astype(bf16)
            act[sl, js] = av
            feed = [feed[h] + mm(av, w_two(wb, r, h)) for h in range(2)]
            ga = mm_t(gob[:, HALVES[0]], w_two(wb, r, 0)) + mm_t(gob[:, HALVES[1]], w_two(wb, r, 1))
            gp = ga * (phi + pre * (e * (1.0 / math.sqrt(2.0 * math.pi))))
            gb1[:, js] += jnp.sum(gp, axis=0, keepdims=True)
            gpb = gp.astype(bf16)
            gpre[sl, js] = gpb
            gln = [gln[h] + mm_t(gpb, w_one(wb, r, h)) for h in range(2)]
        feed = jnp.concatenate(feed, axis=1)
        gln = jnp.concatenate(gln, axis=1)
        out[sl, :] = (live * (res + feed + vec(7))).astype(bf16)
        gr = gout + norm_back(gln * vec(5), unit, scale)
        gres[sl, :] = gr
        grb = gr.astype(bf16)
        gresb[sl, :] = grb
        for quad in range(2):
            gmix[sl, HALVES[quad]] = (
                mm_t(grb[:, HALVES[0]], w_proj(wb, quad, 0)) + mm_t(grb[:, HALVES[1]], w_proj(wb, quad, 1))
            ).astype(bf16)
        gvec[4:5, :] += jnp.sum(gr, axis=0, keepdims=True)
        gvec[5:6, :] += jnp.sum(gln * unit, axis=0, keepdims=True)
        gvec[6:7, :] += jnp.sum(gln, axis=0, keepdims=True)
        gvec[7:8, :] += jnp.sum(gout, axis=0, keepdims=True)
        return 0

    lax.fori_loop(0, blocks, middle, 0)

    def ff_grads(r, _):
        js = pl.ds(pl.multiple_of(r * 256, 256), 256)
        two = mm_r(act[:, js], goutb[...]).astype(bf16)
        for h in range(2):
            gb[slot(r, 2), 256 + h * 64 : 256 + h * 64 + 64, :] = two[0:64, HALVES[h]]
            gb[slot(r, 3), h * 192 : h * 192 + 192, :] = two[64:256, HALVES[h]]
        one = mm_r(ln2[...], gpre[:, js]).astype(bf16)
        gb[slot(r, 1), 128:384, :] = one[0:256]
        gb[slot(r, 2), 0:256, :] = one[256:512]
        return 0

    lax.fori_loop(0, MPS, ff_grads, 0)
    gproj = mm_r(mixed[...], gresb[...]).astype(bf16)
    for r in range(MPS):
        for h in range(2):
            gb[slot(r, 1), h * 64 : h * 64 + 64, :] = gproj[r * 64 : r * 64 + 64, HALVES[h]]

    qkv[...] = jnp.zeros_like(qkv)
    for i in range(images):
        fr = pl.ds(frame[i], length)
        mixw[...] = mm(sel[i], gmix[fr, :]).astype(bf16)

        def window(w, _):
            ws = pl.ds(pl.multiple_of(w * SEG, SEG), SEG)
            for g in range(NG):
                q = wq[i, ws, g * 128 : (g + 1) * 128]
                k = wq[i, ws, C + g * 128 : C + (g + 1) * 128]
                v = wq[i, ws, 2 * C + g * 128 : 2 * C + (g + 1) * 128]
                pt = probs[i, w * NG + g]
                dod = block_diag(mixw[ws, g * 128 : (g + 1) * 128], head_of_lane)
                gv = mm(pt, dod)
                dpt = mm_t(v, dod)
                ptf = pt.astype(f32)
                prod = ptf * dpt
                dst = prod - ptf * jnp.sum(prod, axis=0, keepdims=True)
                acc[g] += dst
                dsb = dst.astype(bf16)
                gk = mm(dsb, block_diag(q, head_of_lane))
                gq = diag_pick(mm_r(dsb, k), head_of_lane) * HD ** (-0.5)
                gl = slice(g * 128, (g + 1) * 128)
                gvec[2:3, gl] += jnp.sum(gq, axis=0, keepdims=True)
                gvec[3:4, gl] += jnp.sum(gv, axis=0, keepdims=True)
                gwin[ws, g * 128 : (g + 1) * 128] = gq.astype(bf16)
                gwin[ws, C + g * 128 : C + (g + 1) * 128] = gk.astype(bf16)
                gwin[ws, 2 * C + g * 128 : 2 * C + (g + 1) * 128] = gv.astype(bf16)
            return 0

        lax.fori_loop(0, NW, window, 0)
        qkv[fr, :] = (qkv[fr, :].astype(f32) + mm_r(sel[i], gwin[...])).astype(bf16)

    def last(t, _):
        sl = pl.ds(pl.multiple_of(t * block, 16), block)
        gln = [jnp.zeros((block, 256), f32)] * 2
        for kind in range(3):
            for quad in range(2):
                part = qkv[sl, kind * C + quad * 256 : kind * C + quad * 256 + 256]
                gln = [gln[h] + mm(part, w_qkv(wb, kind, quad, h)) for h in range(2)]
        gln = jnp.concatenate(gln, axis=1)
        xin = x[sl, :].astype(f32)
        center, scale = norm_stats(xin)
        unit = (xin - center) * scale
        gvec[0:1, :] += jnp.sum(gln * unit, axis=0, keepdims=True)
        gvec[1:2, :] += jnp.sum(gln, axis=0, keepdims=True)
        gin[sl, :] = (gres[sl, :] + norm_back(gln * vec(0), unit, scale)).astype(bf16)
        return 0

    lax.fori_loop(0, blocks, last, 0)

    for kind in range(3):
        for quad in range(2):
            cols = slice(kind * C + quad * 256, kind * C + quad * 256 + 256)
            part = mm_r(qkv[:, cols], ln1[...]).astype(bf16)
            for r in range(4):
                for h in range(2):
                    gb[slot(4 * quad + r, 0), h * 192 + kind * 64 : h * 192 + kind * 64 + 64, :] = part[
                        r * 64 : r * 64 + 64, HALVES[h]
                    ]


def mega_scratch(images, rows):
    return [
        pltpu.VMEM((rows, C), bf16),
        pltpu.VMEM((rows, 3 * C), bf16),
        pltpu.VMEM((images, NW * SEG, 3 * C), bf16),
        pltpu.VMEM((images, NW * NG, SEG, GH * SEG), bf16),
        pltpu.VMEM((NW * SEG, C), bf16),
        pltpu.VMEM((rows, C), bf16),
        pltpu.VMEM((rows, C), bf16),
        pltpu.VMEM((rows, FF), bf16),
        pltpu.VMEM((rows, FF), bf16),
        pltpu.VMEM((rows, C), bf16),
        pltpu.VMEM((rows, C), f32),
        pltpu.VMEM((rows, C), bf16),
        pltpu.VMEM((NW * SEG, 3 * C), bf16),
        pltpu.VMEM((rows, C), bf16),
    ]


def score_masks():
    _, ids = window_sites()
    size = WIN * WIN
    full = np.zeros((NW, SEG, SEG), np.float32)
    full[:, size:, :] = -1e30
    full[:, :size, :size] = np.where(ids[:, :, None] == ids[:, None, :], 0.0, mask_fill)
    return np.tile(full, (1, 1, GH))


def place():
    d, m = lax.axis_index("dp"), lax.axis_index("mp")
    return d, m, d // 2, d % 2, m // 2, m % 2


def twin(a, j):
    if j == 0:
        return a
    if j == 1:
        return a + 1 - 2 * (a % 2)
    if j == 2:
        return (a + 2) % LINES
    return LINES - 1 - a


def remote(src, dst, send, recv, dev):
    return pltpu.make_async_remote_copy(
        src_ref=src, dst_ref=dst, send_sem=send, recv_sem=recv, device_id=dev, device_id_type=MESH
    )


def peers():
    d, m, *_ = place()
    return [{"dp": (d + k) % DPS, "mp": m} for k in range(1, DPS)] + [
        {"dp": d, "mp": (m + k) % MPS} for k in range(1, MPS)
    ]


def greet():
    barrier = pltpu.get_barrier_semaphore()
    group = peers()
    for dev in group:
        pl.semaphore_signal(barrier, inc=1, device_id=dev, device_id_type=MESH)
    pl.semaphore_wait(barrier, len(group))


OFFSET = 277


def flatten_params(pf, fl, roll, head, head_sem, wide, wb, sm):
    d, m, *_ = place()
    lane = iota((FLAT, 128), 1)
    roll[0:8, :] = jnp.zeros((8, 128), f32)
    fl[FLAT : FLAT + 16, :] = jnp.zeros((16, 128), f32)
    for k in range(DPS):

        @pl.when(d == k)
        def _(k=k):
            lanes, down = OFFSET * k % 128, OFFSET * k // 128
            if k == 0:
                fl[0:FLAT, :] = pf[...]
            else:
                roll[8 : 8 + FLAT, :] = pltpu.roll(pf[...], lanes, 1)
                fl[down : down + FLAT, :] = jnp.where(
                    lane >= lanes, roll[8 : 8 + FLAT, :], roll[7 : 7 + FLAT, :]
                )

    over = remote(fl.at[768:784], head.at[0], head_sem.at[0], head_sem.at[1], {"dp": (d + 1) % DPS, "mp": m})

    @pl.when(d < DPS - 1)
    def _():
        over.start()

    @pl.when(d > 0)
    def _():
        over.wait_recv()
        pos = iota((8, 128), 0) * 128 + iota((8, 128), 1)
        fl[0:8, :] = jnp.where(pos < OFFSET * d, head[0, 0:8, :], fl[0:8, :])

    def cut(start, size, step):
        return fl[pl.ds(start, size, stride=step), :]

    @pl.when(d == 0)
    def _():
        low = iota((256, 128), 1) < 64
        one, two = pltpu.roll(cut(1, 256, 3), 64, 1), pltpu.roll(cut(2, 256, 3), 64, 1)
        wide[pl.ds(0, 256, stride=2), :] = cut(0, 256, 3)
        wide[pl.ds(C, 256, stride=2), :] = cut(1, 256, 3)
        wide[pl.ds(1, 256, stride=2), :] = jnp.where(low, one, two)
        wide[pl.ds(C + 1, 256, stride=2), :] = two
        turned = jnp.concatenate([wide[0:C, :].T, wide[C : 2 * C, :].T], axis=0).astype(bf16)
        s = slot(m, 0)
        for half in range(2):
            for kind in range(3):
                for i in range(2):
                    to = half * 192 + kind * 64 + i * 32
                    frm = i * 96 + kind * 32
                    wb[s, to : to + 32, :] = turned[frm : frm + 32, HALVES[half]]

    @pl.when(d == 1)
    def _():
        s = slot(m, 1)
        for j in range(2):
            js = slice(j * 128, (j + 1) * 128)
            for half in range(2):
                wb[s, half * 64 : half * 64 + 64, js] = cut(2 * half + j, 64, 4).astype(bf16)
            wb[s, 128:384, js] = cut(256 + j, 256, 2).astype(bf16)

    @pl.when(d == 2)
    def _():
        s = slot(m, 2)
        for j in range(2):
            js = slice(j * 128, (j + 1) * 128)
            wb[s, 0:256, js] = cut(j, 256, 2).astype(bf16)
            for half in range(2):
                at = 256 + half * 64
                wb[s, at : at + 64, js] = cut(512 + 2 * half + j, 64, 4).astype(bf16)

    @pl.when(d == 3)
    def _():
        s = slot(m, 3)
        for j in range(2):
            js = slice(j * 128, (j + 1) * 128)
            for half in range(2):
                wb[s, half * 192 : half * 192 + 192, js] = cut(2 * half + j, 192, 4).astype(bf16)
        sm[m] = fl[768:784, :].astype(bf16)

    @pl.when(d < DPS - 1)
    def _():
        over.wait_send()


def smalls_out(sm, ssem, rsem):
    d, m, *_ = place()

    def over_dp(k):
        return remote(sm.at[m], sm.at[m], ssem.at[k], rsem.at[m], {"dp": k, "mp": m})

    def over_mp(k):
        return remote(sm.at[m], sm.at[m], ssem.at[3 + k], rsem.at[m], {"dp": d, "mp": (m + k) % MPS})

    @pl.when(d == DPS - 1)
    def _():
        for k in range(DPS - 1):
            over_dp(k).start()

    @pl.when(d < DPS - 1)
    def _():
        over_dp(0).wait_recv()

    for k in range(1, MPS):
        over_mp(k).start()

    def finish():
        for k in range(1, MPS):
            src = (m + k) % MPS
            remote(sm.at[src], sm.at[src], ssem.at[0], rsem.at[src], {"dp": d, "mp": src}).wait_recv()

    def drain():
        @pl.when(d == DPS - 1)
        def _():
            for k in range(DPS - 1):
                over_dp(k).wait_send()

        for k in range(1, MPS):
            over_mp(k).wait_send()

    return finish, drain


RIGHT, LEFT, SIDE_Y, SIDE_X, CORE = range(5)


def blocks_out(wb, ssem, rsem):
    d, m, x, c, a, b = place()
    dev = {
        RIGHT: {"dp": d, "mp": (m + 2) % MPS},
        LEFT: {"dp": d, "mp": (m + MPS - 2) % MPS},
        SIDE_Y: {"dp": d, "mp": m + 1 - 2 * b},
        SIDE_X: {"dp": (d + 2) % DPS, "mp": m},
        CORE: {"dp": d + 1 - 2 * c, "mp": m},
    }
    d_far = (d + 2) % DPS
    d_twin = d + 1 - 2 * c
    sends = []

    def copy(s, way):
        return remote(wb.at[s], wb.at[s], ssem.at[s, way], rsem.at[s], dev[way])

    def go(s, way, cond=None):
        sends.append((s, way, cond))
        if cond is None:
            copy(s, way).start()
        else:
            pl.when(cond)(lambda: copy(s, way).start())

    def arrive(s):
        copy(s, CORE).wait_recv()

    def line_step(j):
        far = twin(a, j)
        s = slot(2 * far + b, d)
        if j == 0:
            go(s, RIGHT, a < LINES - 1)
            go(s, LEFT, a > 0)
        else:
            arrive(s)
            go(s, RIGHT, (far < a) & (a < LINES - 1))
            go(s, LEFT, (far > a) & (a > 0))
        go(s, SIDE_X)
        go(s, SIDE_Y)
        go(s, CORE)

    def y_step(j):
        s = slot(2 * twin(a, j) + 1 - b, d)
        arrive(s)
        go(s, SIDE_X)
        go(s, CORE)

    def x_step(j, same):
        row = 2 * twin(a, j) + (b if same else 1 - b)
        s = slot(row, d_far)
        arrive(s)
        go(s, CORE)

    def core_step(row, dd):
        arrive(slot(row, dd))

    def drain():
        for s, way, cond in sends:
            if cond is None:
                copy(s, way).wait_send()
            else:
                pl.when(cond)(lambda: copy(s, way).wait_send())

    steps = [
        lambda: line_step(0),
        lambda: line_step(1),
        lambda: y_step(0),
        lambda: x_step(0, True),
        lambda: line_step(2),
        lambda: y_step(1),
        lambda: x_step(1, True),
        lambda: line_step(3),
        lambda: x_step(0, False),
        lambda: y_step(2),
        lambda: x_step(2, True),
        lambda: y_step(3),
        lambda: x_step(1, False),
        lambda: x_step(3, True),
        lambda: x_step(2, False),
        lambda: x_step(3, False),
    ]
    for row in range(MPS):
        for dd in (d_twin, (d_twin + 2) % DPS):
            steps.append(functools.partial(core_step, row, dd))
    return steps, drain


def blocks_in(gb, rc, rx, ry, rz, total, s_core, r_core, s_x, r_x, s_y, r_y, s_z, r_z):
    d, m, x, c, a, b = place()
    d_far = (d + 2) % DPS
    d_twin = d + 1 - 2 * c
    to_core = {"dp": d_twin, "mp": m}
    to_x = {"dp": d_far, "mp": m}
    to_y = {"dp": d, "mp": m + 1 - 2 * b}
    to_left = {"dp": d, "mp": (m + MPS - 2) % MPS}
    to_right = {"dp": d, "mp": (m + 2) % MPS}

    def by_core(j, row):
        dd = (d_twin + 2) % DPS if j == 0 else d_twin
        k = j * MPS + row
        return remote(gb.at[slot(row, dd)], rc.at[k], s_core.at[k], r_core.at[k], to_core)

    def by_x(row):
        return remote(gb.at[slot(row, d_far)], rx.at[row], s_x.at[row], r_x.at[row], to_x)

    def by_y(t):
        return remote(gb.at[slot(2 * t + 1 - b, d)], ry.at[t], s_y.at[t], r_y.at[t], to_y)

    def by_z(t, side, dev):
        return remote(gb.at[slot(2 * t + b, d)], rz.at[t, side], s_z.at[t], r_z.at[t, side], dev)

    def add(s, got):
        gb[s] = (gb[s].astype(f32) + got[...].astype(f32)).astype(bf16)

    def start_core():
        for j in range(2):
            lax.fori_loop(0, MPS, lambda row, _: (by_core(j, row).start(), 0)[1], 0)

    def over_x(row, _):
        by_core(0, row).wait_recv()
        add(slot(row, d_far), rc.at[row])
        by_x(row).start()
        return 0

    def keep(row, _):
        by_core(1, row).wait_recv()
        add(slot(row, d), rc.at[MPS + row])
        return 0

    def over_y(t, _):
        row = 2 * t + 1 - b
        by_x(row).wait_recv()
        add(slot(row, d), rx.at[row])
        by_y(t).start()
        return 0

    def own_y(t, _):
        row = 2 * t + b
        by_x(row).wait_recv()
        add(slot(row, d), rx.at[row])
        by_y(t).wait_recv()
        add(slot(row, d), ry.at[t])
        return 0

    def along_z(t):
        s = slot(2 * t + b, d)

        @pl.when((t < a) & (a < LINES - 1))
        def _():
            by_z(t, 1, to_left).wait_recv()
            add(s, rz.at[t, 1])

        @pl.when((t > a) & (a > 0))
        def _():
            by_z(t, 0, to_right).wait_recv()
            add(s, rz.at[t, 0])

        @pl.when(t < a)
        def _():
            by_z(t, 1, to_left).start()

        @pl.when(t > a)
        def _():
            by_z(t, 0, to_right).start()

    def finish():
        for t in (0, LINES - 1, 1, LINES - 2):
            along_z(t)
        total[...] = gb[slot(m, d)].astype(f32)

        @pl.when(a < LINES - 1)
        def _():
            by_z(a, 1, to_left).wait_recv()
            total[...] += rz[a, 1].astype(f32)

        @pl.when(a > 0)
        def _():
            by_z(a, 0, to_right).wait_recv()
            total[...] += rz[a, 0].astype(f32)

    def drain():
        for j in range(2):
            lax.fori_loop(0, MPS, lambda row, _: (by_core(j, row).wait_send(), 0)[1], 0)
        lax.fori_loop(0, MPS, lambda row, _: (by_x(row).wait_send(), 0)[1], 0)
        lax.fori_loop(0, LINES, lambda t, _: (by_y(t).wait_send(), 0)[1], 0)
        for t in range(LINES):

            @pl.when(t != a)
            def _(t=t):
                by_z(t, 0, to_right).wait_send()

    start_core()
    lax.fori_loop(0, MPS, over_x, 0)
    lax.fori_loop(0, MPS, keep, 0)
    lax.fori_loop(0, LINES, over_y, 0)
    lax.fori_loop(0, LINES, own_y, 0)
    finish()
    drain()


def smalls_in(gsm, got, part, got2, total, ssem, rsem, rsem2):
    d, m, *_ = place()

    def over_mp(k):
        dst = (m + k) % MPS
        return remote(gsm.at[dst], got.at[k], ssem.at[k], rsem.at[k], {"dp": d, "mp": dst})

    def over_dp(k):
        return remote(part, got2.at[k], ssem.at[0], rsem2.at[k], {"dp": DPS - 1, "mp": m})

    for k in range(1, MPS):
        over_mp(k).start()
    value = gsm[m]
    for k in range(1, MPS):
        over_mp(k).wait_recv()
        value = value + got[k]
    part[...] = value
    for k in range(DPS - 1):

        @pl.when(d == k)
        def _(k=k):
            over_dp(k).start()

    @pl.when(d == DPS - 1)
    def _():
        total[...] = part[...]
        for k in range(DPS - 1):
            over_dp(k).wait_recv()
            total[...] += got2[k]

    for k in range(DPS - 1):

        @pl.when(d == k)
        def _(k=k):
            over_dp(k).wait_send()

    for k in range(1, MPS):
        over_mp(k).wait_send()


def flat_grads(total, smalls, fl, roll, head, head_sem, wide, tall, gflat):
    d, m, *_ = place()
    fl[768:792, :] = jnp.zeros((24, 128), f32)

    def put(start, size, step, val):
        fl[pl.ds(start, size, stride=step), :] = val

    @pl.when(d == 0)
    def _():
        tall[192:256, :] = jnp.zeros((64, C), f32)
        for half in range(2):
            for kind in range(3):
                for i in range(2):
                    frm = half * 192 + kind * 64 + i * 32
                    to = i * 96 + kind * 32
                    tall[to : to + 32, HALVES[half]] = total[frm : frm + 32, :]
        wide[0:C, :] = tall[0:128, :].T
        wide[C : 2 * C, :] = tall[128:256, :].T
        low = iota((256, 128), 1) < 64

        def every(start):
            return wide[pl.ds(start, 256, stride=2), :]

        one, two = pltpu.roll(every(1), 64, 1), pltpu.roll(every(C + 1), 64, 1)
        put(0, 256, 3, every(0))
        put(1, 256, 3, jnp.where(low, every(C), one))
        put(2, 256, 3, jnp.where(low, one, two))

    @pl.when(d == 1)
    def _():
        for j in range(2):
            js = slice(j * 128, (j + 1) * 128)
            for half in range(2):
                put(2 * half + j, 64, 4, total[half * 64 : half * 64 + 64, js])
            put(256 + j, 256, 2, total[128:384, js])

    @pl.when(d == 2)
    def _():
        for j in range(2):
            js = slice(j * 128, (j + 1) * 128)
            put(j, 256, 2, total[0:256, js])
            for half in range(2):
                at = 256 + half * 64
                put(512 + 2 * half + j, 64, 4, total[at : at + 64, js])

    @pl.when(d == 3)
    def _():
        for j in range(2):
            js = slice(j * 128, (j + 1) * 128)
            for half in range(2):
                put(2 * half + j, 192, 4, total[half * 192 : half * 192 + 192, js])
        fl[768:784, :] = smalls[...]

    back = remote(fl.at[0:8], head.at[1, 0:8], head_sem.at[2], head_sem.at[3], {"dp": (d + DPS - 1) % DPS, "mp": m})

    @pl.when(d > 0)
    def _():
        back.start()

    @pl.when(d < DPS - 1)
    def _():
        back.wait_recv()
        fl[768:776, :] = head[1, 0:8, :]

    lane = iota((FLAT, 128), 1)
    for k in range(DPS):

        @pl.when(d == k)
        def _(k=k):
            lanes, down = OFFSET * k % 128, OFFSET * k // 128
            if k == 0:
                gflat[...] = fl[0:FLAT, :]
            else:
                roll[0:784, :] = pltpu.roll(fl[0:784, :], 128 - lanes, 1)
                roll[784:792, :] = jnp.zeros((8, 128), f32)
                gflat[...] = jnp.where(lane < 128 - lanes, roll[down : down + FLAT, :], roll[down + 1 : down + 1 + FLAT, :])

    @pl.when(d > 0)
    def _():
        back.wait_send()


def step_kernel(images, rows, block, length, *refs):
    (nlive, x, cot, pf, sel, mask) = refs[:6]
    (out, gin, gflat) = refs[6:9]
    (
        fl, roll, head, wide, tall, wb, sm, vecs, b1, tabs, tabs2, bias, gvec, gb1, acc, gb, gsm, got, part, got2,
        stotal, rc, rx, ry, rz, total,
        head_sem, sm_s, sm_r, ag_s, ag_r, rsm_s, rsm_r, rsm_r2, s_core, r_core, s_x, r_x, s_y, r_y, s_z, r_z,
    ) = refs[9:51]
    sc = refs[51:]
    greet()
    flatten_params(pf, fl, roll, head, head_sem, wide, wb, sm)
    steps, drain = blocks_out(wb, ag_s, ag_r)
    steps[0]()
    finish_sm, drain_sm = smalls_out(sm, sm_s, sm_r)
    for step in steps[1:]:
        step()
    finish_sm()
    gather_smalls(sm, vecs, b1, tabs, bias, mask)
    mega_compute(images, rows, block, length, nlive[0], x, cot, wb, vecs, b1, bias, sel, out, gin, gb, gvec, gb1, acc, sc)
    scatter_smalls(gvec, gb1, acc, gsm, tabs2)
    blocks_in(gb, rc, rx, ry, rz, total, s_core, r_core, s_x, r_x, s_y, r_y, s_z, r_z)
    smalls_in(gsm, got, part, got2, stotal, rsm_s, rsm_r, rsm_r2)
    flat_grads(total, stotal, fl, roll, head, head_sem, wide, tall, gflat)
    drain()
    drain_sm()


def step_call(x, cot, nlive, pf):
    rows = x.shape[0]
    images = rows // PIX
    block = block_size(rows)
    length = image_frames(images)[2]
    sel = jnp.asarray(placement(images), bf16)
    mask = jnp.asarray(score_masks(), f32)
    vmem = pl.BlockSpec(memory_space=pltpu.VMEM)
    smem = pl.BlockSpec(memory_space=pltpu.SMEM)
    s = jax.ShapeDtypeStruct
    dma = pltpu.SemaphoreType.DMA
    nb = MPS * DPS
    return pl.pallas_call(
        functools.partial(step_kernel, images, rows, block, length),
        out_shape=(s((rows, C), bf16), s((rows, C), bf16), s((FLAT, 128), f32)),
        in_specs=[smem] + [vmem] * 5,
        out_specs=(vmem,) * 3,
        scratch_shapes=[
            pltpu.VMEM((792, 128), f32),
            pltpu.VMEM((792, 128), f32),
            pltpu.VMEM((2, 16, 128), f32),
            pltpu.VMEM((2 * C, 128), f32),
            pltpu.VMEM((256, C), f32),
            pltpu.VMEM((nb, QROWS, 256), bf16),
            pltpu.VMEM((MPS, 16, 128), bf16),
            pltpu.VMEM((8, C), f32),
            pltpu.VMEM((1, FF), f32),
            pltpu.VMEM((MPS, 384), f32),
            pltpu.VMEM((MPS, 512), f32),
            pltpu.VMEM((NW * NG, SEG, GH * SEG), f32),
            pltpu.VMEM((8, C), f32),
            pltpu.VMEM((1, FF), f32),
            pltpu.VMEM((NG, SEG, GH * SEG), f32),
            pltpu.VMEM((nb, QROWS, 256), bf16),
            pltpu.VMEM((MPS, 16, 128), f32),
            pltpu.VMEM((MPS, 16, 128), f32),
            pltpu.VMEM((16, 128), f32),
            pltpu.VMEM((DPS, 16, 128), f32),
            pltpu.VMEM((16, 128), f32),
            pltpu.VMEM((2 * MPS, QROWS, 256), bf16),
            pltpu.VMEM((MPS, QROWS, 256), bf16),
            pltpu.VMEM((LINES, QROWS, 256), bf16),
            pltpu.VMEM((LINES, 2, QROWS, 256), bf16),
            pltpu.VMEM((QROWS, 256), f32),
            dma((4,)),
            dma((3 + MPS,)),
            dma((MPS,)),
            dma((nb, 5)),
            dma((nb,)),
            dma((MPS,)),
            dma((MPS,)),
            dma((DPS,)),
            dma((2 * MPS,)),
            dma((2 * MPS,)),
            dma((MPS,)),
            dma((MPS,)),
            dma((LINES,)),
            dma((LINES,)),
            dma((LINES,)),
            dma((LINES, 2)),
        ]
        + mega_scratch(images, rows),
        compiler_params=pltpu.CompilerParams(
            vmem_limit_bytes=62 * 1024 * 1024, collective_id=0, has_side_effects=True
        ),
    )(nlive, x, cot, pf, sel, mask)


VEC_LABELS = [
    "norm1_gain",
    "norm1_bias",
    "query_bias",
    "value_bias",
    "proj_bias",
    "norm2_gain",
    "norm2_bias",
    "fc2_bias",
]


def segment_shapes(width_rank, hidden_rank):
    return [
        ("qkv_weight", (C, 3 * width_rank)),
        ("proj_weight", (width_rank, C)),
        ("fc1_weight", (C, hidden_rank)),
        ("fc2_weight", (hidden_rank, C)),
        ("norm1_gain", (width_rank,)),
        ("norm1_bias", (width_rank,)),
        ("query_bias", (width_rank,)),
        ("value_bias", (width_rank,)),
        ("proj_bias", (width_rank,)),
        ("norm2_gain", (width_rank,)),
        ("norm2_bias", (width_rank,)),
        ("fc1_bias", (hidden_rank,)),
        ("fc2_bias", (width_rank,)),
        ("table", (SPAN * SPAN, width_rank // HD)),
    ]


def unpack(flat, width_rank, hidden_rank):
    pieces = {}
    offset = 0
    for label, shape in segment_shapes(width_rank, hidden_rank):
        amount = math.prod(shape)
        pieces[label] = flat[:, offset : offset + amount].reshape((flat.shape[0],) + shape)
        offset = offset + amount
    return pieces


def finish(output, grad_input, grad_shard, params, moment_one, moment_two):
    group = lax.axis_index("dp")
    shard_length = params.shape[1]
    weights_rank = (4 * C * C + 2 * C * FF) // lax.axis_size("mp")
    position = group * shard_length + jnp.arange(shard_length, dtype=jnp.int32)[None, :]
    decays = (position < weights_rank).astype(jnp.float32)
    new_one = beta_one * moment_one + (1.0 - beta_one) * grad_shard
    new_two = second_decay_rate * moment_two + (1.0 - second_decay_rate) * grad_shard * grad_shard
    corrected_one = new_one / (1.0 - beta_one**adam_step)
    corrected_two = new_two / (1.0 - second_decay_rate**adam_step)
    new_params = params - learn_rate * (
        corrected_one / (jnp.sqrt(corrected_two) + adam_eps) + weight_decay * decays * params
    )
    return (output, grad_input, grad_shard, new_params, new_one, new_two)


def local_xla(tokens, cotangent, image_counts, params, moment_one, moment_two):
    ranks = lax.axis_size("mp")
    rank = lax.axis_index("mp")
    group = lax.axis_index("dp")
    width = C // ranks
    hidden = FF // ranks
    heads = width // HD
    rows = tokens.shape[0]
    shard_length = params.shape[1]
    length = shard_length * lax.axis_size("dp")
    owned = lax.all_gather(params.astype(bf16), "mp", axis=0, tiled=True)
    owned = lax.all_gather(owned, "dp", axis=1, tiled=True)
    op = unpack(owned, width, hidden)
    wqkv = op["qkv_weight"].reshape(ranks, C, heads, 3, HD).transpose(3, 0, 2, 4, 1).reshape(3 * C, C)
    wproj = op["proj_weight"].reshape(C, C)
    w1 = op["fc1_weight"].transpose(1, 0, 2).reshape(C, FF)
    w2 = op["fc2_weight"].reshape(FF, C)
    vecs = jnp.stack([op[n].reshape(C) for n in VEC_LABELS]).astype(f32)
    b1 = op["fc1_bias"].reshape(1, FF).astype(f32)
    bias = score_bias(op["table"].transpose(1, 0, 2).reshape(-1, HEADS))
    limit = jnp.sum(
        jnp.where(jnp.arange(image_counts.shape[0], dtype=jnp.int32) == group, image_counts, 0)
    )
    nlive = jnp.clip(limit * PIX - rank * rows, 0, rows).reshape(1)
    output, grad_input, gqkv, gproj, g1, g2, gvec, gb1, acc = block_compute(
        tokens, cotangent, nlive, wqkv, wproj, w1, w2, vecs, b1, bias
    )
    gtable = table_back(acc)
    gvec = gvec.reshape(8, ranks, width)
    pieces = [
        gqkv.reshape(3, ranks, heads, HD, C).transpose(1, 4, 2, 0, 3).reshape(ranks, -1),
        gproj.reshape(ranks, -1),
        g1.reshape(C, ranks, hidden).transpose(1, 0, 2).reshape(ranks, -1),
        g2.T.reshape(ranks, -1),
    ]
    pieces += [gvec[i].astype(bf16) for i in range(7)]
    pieces += [gb1.reshape(ranks, hidden).astype(bf16), gvec[7].astype(bf16)]
    pieces += [gtable.reshape(-1, ranks, heads).transpose(1, 0, 2).reshape(ranks, -1).astype(bf16)]
    used = sum(p.shape[1] for p in pieces)
    pieces.append(jnp.zeros((ranks, length - used), bf16))
    flat = jnp.concatenate(pieces, axis=1)
    flat = lax.psum_scatter(flat, "mp", scatter_dimension=0, tiled=True)
    grad_shard = lax.psum_scatter(flat, "dp", scatter_dimension=1, tiled=True).astype(f32)
    return finish(output, grad_input, grad_shard, params, moment_one, moment_two)


def local(tokens, cotangent, image_counts, params, moment_one, moment_two):
    ranks = lax.axis_size("mp")
    rows = tokens.shape[0]
    shard = params.shape[1]
    fits = (
        ranks == MPS
        and lax.axis_size("dp") == DPS
        and rows % 16 == 0
        and image_frames(rows // PIX)[0][-1] + image_frames(rows // PIX)[2] <= rows
        and shard == QUART + OFFSET
    )
    if not fits:
        return local_xla(tokens, cotangent, image_counts, params, moment_one, moment_two)
    rank = lax.axis_index("mp")
    group = lax.axis_index("dp")
    limit = jnp.sum(
        jnp.where(jnp.arange(image_counts.shape[0], dtype=jnp.int32) == group, image_counts, 0)
    )
    nlive = jnp.clip(limit * PIX - rank * rows, 0, rows).reshape(1)
    pf = jnp.pad(params, ((0, 0), (0, FLAT * 128 - shard))).reshape(FLAT, 128)
    output, grad_input, gflat = step_call(tokens, cotangent, nlive, pf)
    grad_shard = gflat.reshape(1, -1)[:, :shard]
    return finish(output, grad_input, grad_shard, params, moment_one, moment_two)


def solution(mesh):
    return jax.shard_map(
        local,
        mesh=mesh,
        in_specs=(
            P(("dp", "mp"), None),
            P(("dp", "mp"), None),
            P(),
            P("mp", "dp"),
            P("mp", "dp"),
            P("mp", "dp"),
        ),
        out_specs=(
            P(("dp", "mp"), None),
            P(("dp", "mp"), None),
            P("mp", "dp"),
            P("mp", "dp"),
            P("mp", "dp"),
            P("mp", "dp"),
        ),
        check_vma=False,
    )
```

```python
import functools
import math

import jax
import jax.numpy as jnp
import numpy as np
from jax import lax
from jax.experimental import pallas as pl
from jax.experimental.pallas import tpu as pltpu
from jax.sharding import PartitionSpec as P

C = 512
FF = 2048
HD = 32
WIN = 7
MAP = 14
SHIFT = 3
PIX = MAP * MAP
HEADS = C // HD
SEG = 64
GH = 4
NG = HEADS // GH
SIDE = MAP // WIN
NW = SIDE * SIDE
SPAN = 2 * WIN - 1

norm_eps = 1e-05
mask_fill = -100.0
learn_rate = 0.05
beta_one = 0.9
second_decay_rate = 0.999
adam_eps = 1e-08
weight_decay = 0.05
adam_step = 2.0
f32 = jnp.float32
bf16 = jnp.bfloat16


def mm(a, b):
    return lax.dot_general(a, b, (((1,), (0,)), ((), ())), preferred_element_type=f32)


def mm_t(a, b):
    return lax.dot_general(a, b, (((1,), (1,)), ((), ())), preferred_element_type=f32)


def mm_r(a, b):
    return lax.dot_general(a, b, (((0,), (0,)), ((), ())), preferred_element_type=f32)


def norm_stats(values):
    center = jnp.mean(values, axis=1, keepdims=True)
    spread = jnp.mean(jnp.square(values - center), axis=1, keepdims=True)
    return center, lax.rsqrt(spread + norm_eps)


def norm_back(scaled, unit, scale):
    return scale * (
        scaled
        - jnp.mean(scaled, axis=1, keepdims=True)
        - unit * jnp.mean(scaled * unit, axis=1, keepdims=True)
    )


def phi_parts(v):
    return 0.5 * (1.0 + lax.erf(v * (1.0 / math.sqrt(2.0)))), jnp.exp(-0.5 * v * v)


def window_sites():
    w = np.arange(NW)[:, None]
    p = np.arange(WIN * WIN)[None, :]
    row = (w // SIDE) * WIN + p // WIN
    col = (w % SIDE) * WIN + p % WIN
    token = ((row + SHIFT) % MAP) * MAP + (col + SHIFT) % MAP

    def region(c):
        return (c >= MAP - WIN).astype(np.int32) + (c >= MAP - SHIFT).astype(np.int32)

    ids = region(row) * 3 + region(col)
    return token, ids


def image_frames(images):
    starts = [PIX * i // 16 * 16 for i in range(images)]
    offsets = [PIX * i - s for i, s in enumerate(starts)]
    length = -(-(PIX + max(offsets)) // 16) * 16
    return starts, offsets, length


def placement(images):
    token, _ = window_sites()
    starts, offsets, length = image_frames(images)
    sel = np.zeros((images, NW * SEG, length), np.float32)
    for i in range(images):
        for w in range(NW):
            sel[i, w * SEG + np.arange(WIN * WIN), token[w] + offsets[i]] = 1.0
    return sel


def score_bias(table):
    size = WIN * WIN
    p = np.arange(size)
    a, b = p // WIN, p % WIN
    off = (a[None, :] - a[:, None] + WIN - 1) * SPAN + b[None, :] - b[:, None] + WIN - 1
    one_hot = np.zeros((size, size, SPAN * SPAN), np.float32)
    one_hot[np.arange(size)[:, None], np.arange(size)[None, :], off] = 1.0
    _, ids = window_sites()
    full_mask = np.full((NW, SEG, SEG), 0.0, np.float32)
    full_mask[:, size:, :] = -1e30
    full_mask[:, :size, :size] = np.where(ids[:, :, None] == ids[:, None, :], 0.0, mask_fill)
    onehot = jnp.asarray(one_hot.reshape(size * size, -1), bf16)
    bias = jnp.dot(table.T.astype(bf16), onehot.T, preferred_element_type=f32)
    bias = bias.reshape(NG, GH, size, size)
    bias = jnp.pad(bias, ((0, 0), (0, 0), (0, SEG - size), (0, SEG - size)))
    bias = bias.transpose(0, 2, 1, 3)
    out = bias[None] + jnp.asarray(full_mask)[:, None, :, None, :]
    return out.reshape(NW * NG, SEG, GH * SEG)


def table_back(acc):
    size = WIN * WIN
    p = np.arange(size)
    a, b = p // WIN, p % WIN
    off = (a[None, :] - a[:, None] + WIN - 1) * SPAN + b[None, :] - b[:, None] + WIN - 1
    one_hot = np.zeros((size * size, SPAN * SPAN), np.float32)
    one_hot[np.arange(size * size), off.reshape(-1)] = 1.0
    acc = acc.reshape(NG, SEG, GH, SEG)[:, :size, :, :size].transpose(0, 2, 1, 3).reshape(HEADS, size * size)
    hi = acc.astype(bf16)
    lo = (acc - hi.astype(f32)).astype(bf16)
    oh = jnp.asarray(one_hot, bf16)
    return (
        jnp.dot(hi, oh, preferred_element_type=f32) + jnp.dot(lo, oh, preferred_element_type=f32)
    ).T


def lane_head_mask():
    return lax.broadcasted_iota(jnp.int32, (SEG, GH * HD), 1) // HD


def block_diag(part, head_of_lane):
    zero = jnp.zeros_like(part)
    return jnp.concatenate([jnp.where(head_of_lane == h, part, zero) for h in range(GH)], axis=0)


def diag_pick(full, head_of_lane):
    out = full[:SEG]
    for h in range(1, GH):
        out = jnp.where(head_of_lane == h, full[h * SEG : (h + 1) * SEG], out)
    return out


def compute_kernel(
    images, rows, block, length,
    nlive, x, cot, wqkv, wproj, w1, w2, vecs, b1, bias, sel,
    out, gin, gqkv_w, gproj_w, g1_w, g2_w, gvec, gb1, acc,
    ln1, qkv, wq, probs, mixw, mixed, ln2, act, gpre, gresb, gres, gmix, gwin,
):
    blocks = rows // block
    frame = image_frames(images)[0]
    head_of_lane = lane_head_mask()

    def vec(i):
        return vecs[i : i + 1, :]

    gvec[...] = jnp.zeros_like(gvec)
    gb1[...] = jnp.zeros_like(gb1)
    acc[...] = jnp.zeros_like(acc)
    mixed[...] = jnp.zeros_like(mixed)

    def norm_rows(t, _):
        sl = pl.ds(pl.multiple_of(t * block, 16), block)
        xin = x[sl, :].astype(f32)
        center, scale = norm_stats(xin)
        normed = ((xin - center) * scale * vec(0) + vec(1)).astype(bf16)
        ln1[sl, :] = normed
        qkv[sl, 0:C] = ((mm_t(normed, wqkv[0:C, :]) + vec(2)) * HD ** (-0.5)).astype(bf16)
        qkv[sl, C : 2 * C] = mm_t(normed, wqkv[C : 2 * C, :]).astype(bf16)
        qkv[sl, 2 * C : 3 * C] = (mm_t(normed, wqkv[2 * C : 3 * C, :]) + vec(3)).astype(bf16)
        return 0

    lax.fori_loop(0, blocks, norm_rows, 0)

    for i in range(images):
        fr = pl.ds(frame[i], length)
        wq[i] = mm(sel[i], qkv[fr, :]).astype(bf16)

        def window(w, _):
            ws = pl.ds(pl.multiple_of(w * SEG, SEG), SEG)
            for g in range(NG):
                q = wq[i, ws, g * 128 : (g + 1) * 128]
                k = wq[i, ws, C + g * 128 : C + (g + 1) * 128]
                v = wq[i, ws, 2 * C + g * 128 : 2 * C + (g + 1) * 128]
                st = mm_t(k, block_diag(q, head_of_lane)) + bias[w * NG + g]
                e = jnp.exp(st - jnp.max(st, axis=0, keepdims=True))
                pt = (e * (1.0 / jnp.sum(e, axis=0, keepdims=True))).astype(bf16)
                probs[i, w * NG + g] = pt
                mixw[ws, g * 128 : (g + 1) * 128] = diag_pick(mm_r(pt, v), head_of_lane).astype(bf16)
            return 0

        lax.fori_loop(0, NW, window, 0)
        mixed[fr, :] = (mixed[fr, :].astype(f32) + mm_r(sel[i], mixw[...])).astype(bf16)

    def middle(t, _):
        sl = pl.ds(pl.multiple_of(t * block, 16), block)
        xin = x[sl, :].astype(f32)
        res = xin + (mm(mixed[sl, :], wproj[...]) + vec(4))
        center, scale = norm_stats(res)
        unit = (res - center) * scale
        normed = (unit * vec(5) + vec(6)).astype(bf16)
        ln2[sl, :] = normed
        live = (
            lax.broadcasted_iota(jnp.int32, (block, 1), 0) + t * block < nlive[0]
        ).astype(f32)
        gout = live * cot[sl, :].astype(f32)
        goutb = gout.astype(bf16)
        feed = jnp.zeros((block, C), f32)
        gln = jnp.zeros((block, C), f32)
        for j in range(4):
            js = slice(j * 512, (j + 1) * 512)
            pre = mm(normed, w1[:, js]) + b1[:, js]
            phi, e = phi_parts(pre)
            av = (pre * phi).astype(bf16)
            act[sl, js] = av
            feed = feed + mm(av, w2[js, :])
            gp = mm_t(goutb, w2[js, :]) * (phi + pre * (e * (1.0 / math.sqrt(2.0 * math.pi))))
            gb1[:, js] += jnp.sum(gp, axis=0, keepdims=True)
            gpb = gp.astype(bf16)
            gpre[sl, js] = gpb
            gln = gln + mm_t(gpb, w1[:, js])
        out[sl, :] = (live * (res + feed + vec(7))).astype(bf16)
        gr = gout + norm_back(gln * vec(5), unit, scale)
        gres[sl, :] = gr
        grb = gr.astype(bf16)
        gresb[sl, :] = grb
        gmix[sl, :] = mm_t(grb, wproj[...]).astype(bf16)
        gvec[4:5, :] += jnp.sum(gr, axis=0, keepdims=True)
        gvec[5:6, :] += jnp.sum(gln * unit, axis=0, keepdims=True)
        gvec[6:7, :] += jnp.sum(gln, axis=0, keepdims=True)
        gvec[7:8, :] += jnp.sum(gout, axis=0, keepdims=True)
        return 0

    lax.fori_loop(0, blocks, middle, 0)

    def masked_cot():
        live = (lax.broadcasted_iota(jnp.int32, (rows, 1), 0) < nlive[0]).astype(bf16)
        return cot[...] * live

    gout_all = masked_cot()

    def ff_grads(j, _):
        js = pl.ds(pl.multiple_of(j * 256, 256), 256)
        g2_w[:, js] = mm_r(gout_all, act[:, js]).astype(g2_w.dtype)
        g1_w[:, js] = mm_r(ln2[...], gpre[:, js]).astype(g1_w.dtype)
        return 0

    lax.fori_loop(0, FF // 256, ff_grads, 0)
    gproj_w[...] = mm_r(mixed[...], gresb[...]).astype(gproj_w.dtype)

    qkv[...] = jnp.zeros_like(qkv)
    for i in range(images):
        fr = pl.ds(frame[i], length)
        mixw[...] = mm(sel[i], gmix[fr, :]).astype(bf16)

        def window(w, _):
            ws = pl.ds(pl.multiple_of(w * SEG, SEG), SEG)
            for g in range(NG):
                q = wq[i, ws, g * 128 : (g + 1) * 128]
                k = wq[i, ws, C + g * 128 : C + (g + 1) * 128]
                v = wq[i, ws, 2 * C + g * 128 : 2 * C + (g + 1) * 128]
                pt = probs[i, w * NG + g]
                dod = block_diag(mixw[ws, g * 128 : (g + 1) * 128], head_of_lane)
                gv = mm(pt, dod)
                dpt = mm_t(v, dod)
                ptf = pt.astype(f32)
                prod = ptf * dpt
                dst = prod - ptf * jnp.sum(prod, axis=0, keepdims=True)
                acc[g] += dst
                dsb = dst.astype(bf16)
                gk = mm(dsb, block_diag(q, head_of_lane))
                gq = diag_pick(mm_r(dsb, k), head_of_lane) * HD ** (-0.5)
                gl = slice(g * 128, (g + 1) * 128)
                gvec[2:3, gl] += jnp.sum(gq, axis=0, keepdims=True)
                gvec[3:4, gl] += jnp.sum(gv, axis=0, keepdims=True)
                gwin[ws, g * 128 : (g + 1) * 128] = gq.astype(bf16)
                gwin[ws, C + g * 128 : C + (g + 1) * 128] = gk.astype(bf16)
                gwin[ws, 2 * C + g * 128 : 2 * C + (g + 1) * 128] = gv.astype(bf16)
            return 0

        lax.fori_loop(0, NW, window, 0)
        qkv[fr, :] = (qkv[fr, :].astype(f32) + mm_r(sel[i], gwin[...])).astype(bf16)

    def last(t, _):
        sl = pl.ds(pl.multiple_of(t * block, 16), block)
        gln = mm(qkv[sl, :], wqkv[...])
        xin = x[sl, :].astype(f32)
        center, scale = norm_stats(xin)
        unit = (xin - center) * scale
        gvec[0:1, :] += jnp.sum(gln * unit, axis=0, keepdims=True)
        gvec[1:2, :] += jnp.sum(gln, axis=0, keepdims=True)
        gin[sl, :] = (gres[sl, :] + norm_back(gln * vec(0), unit, scale)).astype(bf16)
        return 0

    lax.fori_loop(0, blocks, last, 0)

    def qkv_grads(j, _):
        js = pl.ds(pl.multiple_of(j * 256, 256), 256)
        gqkv_w[js, :] = mm_r(qkv[:, js], ln1[...]).astype(gqkv_w.dtype)
        return 0

    lax.fori_loop(0, 3 * C // 256, qkv_grads, 0)


def block_size(rows):
    for cand in (112, 80, 64, 48, 32, 16):
        if rows % cand == 0:
            return cand
    return rows


def block_compute(x, cot, nlive, wqkv, wproj, w1, w2, vecs, b1, bias, interpret=False):
    tokens = x.shape[0]
    images = tokens // PIX
    rows = -(-tokens // 16) * 16
    if rows != tokens:
        x = jnp.pad(x, ((0, rows - tokens), (0, 0)))
        cot = jnp.pad(cot, ((0, rows - tokens), (0, 0)))
    block = block_size(rows)
    starts, _, length = image_frames(images)
    assert starts[-1] + length <= rows
    sel = jnp.asarray(placement(images), bf16)
    vmem = pl.BlockSpec(memory_space=pltpu.VMEM)
    smem = pl.BlockSpec(memory_space=pltpu.SMEM)
    s = jax.ShapeDtypeStruct
    outs = pl.pallas_call(
        functools.partial(compute_kernel, images, rows, block, length),
        out_shape=(
            s((rows, C), bf16),
            s((rows, C), bf16),
            s((3 * C, C), bf16),
            s((C, C), bf16),
            s((C, FF), bf16),
            s((C, FF), bf16),
            s((8, C), f32),
            s((1, FF), f32),
            s((NG, SEG, GH * SEG), f32),
        ),
        in_specs=[smem] + [vmem] * 10,
        out_specs=(vmem,) * 9,
        scratch_shapes=[
            pltpu.VMEM((rows, C), bf16),
            pltpu.VMEM((rows, 3 * C), bf16),
            pltpu.VMEM((images, NW * SEG, 3 * C), bf16),
            pltpu.VMEM((images, NW * NG, SEG, GH * SEG), bf16),
            pltpu.VMEM((NW * SEG, C), bf16),
            pltpu.VMEM((rows, C), bf16),
            pltpu.VMEM((rows, C), bf16),
            pltpu.VMEM((rows, FF), bf16),
            pltpu.VMEM((rows, FF), bf16),
            pltpu.VMEM((rows, C), bf16),
            pltpu.VMEM((rows, C), f32),
            pltpu.VMEM((rows, C), bf16),
            pltpu.VMEM((NW * SEG, 3 * C), bf16),
        ],
        compiler_params=pltpu.CompilerParams(vmem_limit_bytes=60 * 1024 * 1024),
        interpret=interpret,
    )(nlive, x, cot, wqkv, wproj, w1, w2, vecs, b1, bias, sel)
    return (outs[0][:tokens], outs[1][:tokens]) + outs[2:]

LINES = 4
MPS = 8
DPS = 4
QROWS = 384
QUART = QROWS * 256
FLAT = 776
MESH = pl.DeviceIdType.MESH


def base_of(p):
    return (p // WIN) * SPAN + p % WIN


def iota(shape, dim):
    return lax.broadcasted_iota(jnp.int32, shape, dim)


def as_bf(mask):
    return jnp.where(mask, 1.0, 0.0).astype(bf16)


def spread_queries():
    row = iota((GH * 256, GH * SEG), 0)
    lane = iota((GH * 256, GH * SEG), 1)
    q = lane % SEG
    return as_bf((row // 256 == lane // SEG) & (row % 256 == base_of(q)) & (q < WIN * WIN))


def key_rows(reverse):
    k = iota((SEG, 8 * WIN), 0)
    row = iota((SEG, 8 * WIN), 1)
    b = WIN - 1 - k % WIN if reverse else k % WIN
    return as_bf((row == (k // WIN) * 8 + b) & (k < WIN * WIN))


def table_lanes():
    row = iota((384, 512), 0)
    lane = iota((384, 512), 1)
    return as_bf((row == 2 * (lane % 256) + lane // 256) & (lane % 256 < SPAN * SPAN))


def split_mm(op, exact, value):
    hi = value.astype(bf16)
    lo = (value - hi.astype(f32)).astype(bf16)
    return op(exact, hi) + op(exact, lo)


def split_mm_left(op, value, exact):
    hi = value.astype(bf16)
    lo = (value - hi.astype(f32)).astype(bf16)
    return op(hi, exact) + op(lo, exact)


def turn_rows(part):
    return pltpu.roll(part, 0, 1, stride=1, stride_axis=0)


def gather_smalls(sm, vecs, b1, tabs, bias, mask):
    lane = iota((16, 128), 1)
    low = lane < 64
    for g in range(4):
        first, second = sm[2 * g].astype(f32), sm[2 * g + 1].astype(f32)
        turned = [pltpu.roll(first, 64, 1), pltpu.roll(second, 64, 1)]
        los = jnp.where(low, first, turned[1])
        his = jnp.where(low, turned[0], second)
        gl = slice(g * 128, (g + 1) * 128)
        for i, src, row in (
            (0, los, 0), (1, his, 0), (2, los, 1), (3, his, 1), (4, los, 2), (5, his, 2), (6, los, 3), (7, his, 5),
        ):
            vecs[i : i + 1, gl] = src[row : row + 1]
        for k in range(2):
            r = 2 * g + k
            full = (first, second)[k]
            rot = turned[k]
            b1[:, r * 256 : r * 256 + 128] = jnp.where(low[:1], rot[3:4], rot[4:5])
            b1[:, r * 256 + 128 : r * 256 + 256] = jnp.where(low[:1], rot[4:5], rot[5:6])
            for j in range(3):
                tabs[r : r + 1, j * 128 : (j + 1) * 128] = full[6 + j : 7 + j]
    tab = mm(tabs[...].astype(bf16), table_lanes())
    spread = spread_queries()
    keys = key_rows(False)
    for g in range(NG):
        parts = []
        for h in range(GH):
            r, i = divmod(g * GH + h, 2)
            t = jnp.broadcast_to(tab[r : r + 1, i * 256 : (i + 1) * 256], (8, 256))
            rows = [
                turn_rows(pltpu.roll(t, (SPAN * a - 84) % 256, 1)) for a in range(WIN)
            ]
            parts.append(jnp.concatenate(rows, axis=0))
        line = jnp.concatenate(parts, axis=1).astype(bf16)
        placed = mm(line, spread).astype(bf16)
        bt = mm(keys, placed)
        for w in range(NW):
            bias[w * NG + g] = bt + mask[w]


def scatter_smalls(gvec, gb1, acc, gsm, tabs):
    lane = iota((1, 128), 1)
    low = lane < 64
    spread = spread_queries()
    keys = key_rows(True)
    tabs[...] = jnp.zeros_like(tabs)
    for g in range(NG):
        z = split_mm(mm_r, keys, acc[g])
        y = split_mm_left(mm_t, z, spread)
        for h in range(GH):
            r, i = divmod(g * GH + h, 2)
            total = jnp.zeros((8, 256), f32)
            for a in range(WIN):
                part = y[8 * a : 8 * a + 8, h * 256 : (h + 1) * 256]
                total = total + turn_rows(pltpu.roll(part, (78 - SPAN * a) % 256, 1))
            tabs[r : r + 1, i * 256 : (i + 1) * 256] = jnp.sum(total, axis=0, keepdims=True)
    flat = split_mm_left(mm_t, tabs[...], table_lanes())

    def half(i, r):
        g, k = divmod(r, 2)
        v = gvec[i : i + 1, g * 128 : (g + 1) * 128]
        turned = pltpu.roll(v, 64, 1)
        return (v, turned) if k == 0 else (turned, v)

    zero = jnp.zeros((1, 128), f32)
    for r in range(MPS):
        fb0 = gb1[:, r * 256 : r * 256 + 128]
        fb1 = gb1[:, r * 256 + 128 : r * 256 + 256]
        t0, t1 = pltpu.roll(fb0, 64, 1), pltpu.roll(fb1, 64, 1)
        rows = [
            jnp.where(low, half(0, r)[0], half(1, r)[1]),
            jnp.where(low, half(2, r)[0], half(3, r)[1]),
            jnp.where(low, half(4, r)[0], half(5, r)[1]),
            jnp.where(low, half(6, r)[0], t0),
            jnp.where(low, t0, t1),
            jnp.where(low, t1, half(7, r)[1]),
        ]
        for j, row in enumerate(rows):
            gsm[r, j : j + 1, :] = row
        for j in range(3):
            gsm[r, 6 + j : 7 + j, :] = flat[r : r + 1, j * 128 : (j + 1) * 128]
        for j in range(9, 16):
            gsm[r, j : j + 1, :] = zero


def slot(m, d):
    return m * DPS + d


def w_qkv(wb, kind, quad, half):
    return jnp.concatenate(
        [wb[slot(4 * quad + r, 0), half * 192 + kind * 64 : half * 192 + kind * 64 + 64, :] for r in range(4)], axis=0
    )


def w_proj(wb, quad, half):
    return jnp.concatenate([wb[slot(4 * quad + r, 1), half * 64 : half * 64 + 64, :] for r in range(4)], axis=0)


def w_one(wb, r, half):
    return wb[slot(r, 1), 128:384, :] if half == 0 else wb[slot(r, 2), 0:256, :]


def w_two(wb, r, half):
    return jnp.concatenate(
        [
            wb[slot(r, 2), 256 + half * 64 : 256 + half * 64 + 64, :],
            wb[slot(r, 3), half * 192 : half * 192 + 192, :],
        ],
        axis=0,
    )


HALVES = (slice(0, 256), slice(256, 512))


def first_norm(x, vecs, ln1):
    xin = x[...].astype(f32)
    center, scale = norm_stats(xin)
    ln1[...] = ((xin - center) * scale * vecs[0:1, :] + vecs[1:2, :]).astype(bf16)


def project_qkv(wb, vecs, ln1, qkv, poll):
    for kind in range(3):
        for quad in range(2):
            poll(2 * kind + quad)
            qs = HALVES[quad]
            val = mm_t(ln1[:, HALVES[0]], w_qkv(wb, kind, quad, 0)) + mm_t(
                ln1[:, HALVES[1]], w_qkv(wb, kind, quad, 1)
            )
            if kind == 0:
                val = (val + vecs[2:3, qs]) * HD ** (-0.5)
            if kind == 2:
                val = val + vecs[3:4, qs]
            qkv[:, kind * C + quad * 256 : kind * C + quad * 256 + 256] = val.astype(bf16)


def attention_forward(images, length, sel, bias, qkv, wq, probs, mixw, mixed, poll):
    head_of_lane = lane_head_mask()
    frame = image_frames(images)[0]
    mixed[...] = jnp.zeros_like(mixed)
    for i in range(images):
        fr = pl.ds(frame[i], length)
        wq[i] = mm(sel[i], qkv[fr, :]).astype(bf16)

        def window(w, _):
            poll(i, w)
            ws = pl.ds(pl.multiple_of(w * SEG, SEG), SEG)
            for g in range(NG):
                q = wq[i, ws, g * 128 : (g + 1) * 128]
                k = wq[i, ws, C + g * 128 : C + (g + 1) * 128]
                v = wq[i, ws, 2 * C + g * 128 : 2 * C + (g + 1) * 128]
                st = mm_t(k, block_diag(q, head_of_lane)) + bias[w * NG + g]
                e = jnp.exp(st - jnp.max(st, axis=0, keepdims=True))
                pt = (e * (1.0 / jnp.sum(e, axis=0, keepdims=True))).astype(bf16)
                probs[i, w * NG + g] = pt
                mixw[ws, g * 128 : (g + 1) * 128] = diag_pick(mm_r(pt, v), head_of_lane).astype(bf16)
            return 0

        lax.fori_loop(0, NW, window, 0)
        mixed[fr, :] = (mixed[fr, :].astype(f32) + mm_r(sel[i], mixw[...])).astype(bf16)


def feed_forward(rows, live_rows, x, cot, wb, vecs, b1, out, gvec, gb1, mixed, ln2, act, gpre, gresb, gres, gmix, goutb):
    def vec(i):
        return vecs[i : i + 1, :]

    att = [mm(mixed[:, HALVES[0]], w_proj(wb, 0, h)) + mm(mixed[:, HALVES[1]], w_proj(wb, 1, h)) for h in range(2)]
    res = x[...].astype(f32) + (jnp.concatenate(att, axis=1) + vec(4))
    center, scale = norm_stats(res)
    unit = (res - center) * scale
    ln2[...] = (unit * vec(5) + vec(6)).astype(bf16)
    live = (iota((rows, 1), 0) < live_rows).astype(f32)
    gout = live * cot[...].astype(f32)
    goutb[...] = gout.astype(bf16)
    feed = [jnp.zeros((rows, 256), f32)] * 2
    gln = [jnp.zeros((rows, 256), f32)] * 2
    for r in range(MPS):
        js = slice(r * 256, (r + 1) * 256)
        pre = mm(ln2[:, HALVES[0]], w_one(wb, r, 0)) + mm(ln2[:, HALVES[1]], w_one(wb, r, 1)) + b1[:, js]
        phi, e = phi_parts(pre)
        av = (pre * phi).astype(bf16)
        act[:, js] = av
        feed = [feed[h] + mm(av, w_two(wb, r, h)) for h in range(2)]
        ga = mm_t(goutb[:, HALVES[0]], w_two(wb, r, 0)) + mm_t(goutb[:, HALVES[1]], w_two(wb, r, 1))
        gp = ga * (phi + pre * (e * (1.0 / math.sqrt(2.0 * math.pi))))
        gb1[:, js] = jnp.sum(gp, axis=0, keepdims=True)
        gpb = gp.astype(bf16)
        gpre[:, js] = gpb
        gln = [gln[h] + mm_t(gpb, w_one(wb, r, h)) for h in range(2)]
    feed = jnp.concatenate(feed, axis=1)
    gln = jnp.concatenate(gln, axis=1)
    out[...] = (live * (res + feed + vec(7))).astype(bf16)
    gr = gout + norm_back(gln * vec(5), unit, scale)
    gres[...] = gr
    grb = gr.astype(bf16)
    gresb[...] = grb
    for quad in range(2):
        gmix[:, HALVES[quad]] = (
            mm_t(grb[:, HALVES[0]], w_proj(wb, quad, 0)) + mm_t(grb[:, HALVES[1]], w_proj(wb, quad, 1))
        ).astype(bf16)
    gvec[4:5, :] = jnp.sum(gr, axis=0, keepdims=True)
    gvec[5:6, :] = jnp.sum(gln * unit, axis=0, keepdims=True)
    gvec[6:7, :] = jnp.sum(gln, axis=0, keepdims=True)
    gvec[7:8, :] = jnp.sum(gout, axis=0, keepdims=True)


def proj_grads(gb, mixed, gresb):
    gproj = mm_r(mixed[...], gresb[...]).astype(bf16)
    for r in range(MPS):
        for h in range(2):
            gb[slot(r, 1), h * 64 : h * 64 + 64, :] = gproj[r * 64 : r * 64 + 64, HALVES[h]]


def feed_forward_grads(r, gb, act, goutb, ln2, gpre):
    js = pl.ds(pl.multiple_of(r * 256, 256), 256)
    two = mm_r(act[:, js], goutb[...]).astype(bf16)
    for h in range(2):
        gb[slot(r, 2), 256 + h * 64 : 256 + h * 64 + 64, :] = two[0:64, HALVES[h]]
        gb[slot(r, 3), h * 192 : h * 192 + 192, :] = two[64:256, HALVES[h]]
    one = mm_r(ln2[...], gpre[:, js]).astype(bf16)
    gb[slot(r, 1), 128:384, :] = one[0:256]
    gb[slot(r, 2), 0:256, :] = one[256:512]


def attention_backward(images, length, sel, gmix, wq, probs, mixw, gwin, qkv, acc, gvec, poll):
    head_of_lane = lane_head_mask()
    frame = image_frames(images)[0]
    qkv[...] = jnp.zeros_like(qkv)
    acc[...] = jnp.zeros_like(acc)
    gvec[2:4, :] = jnp.zeros((2, C), f32)
    for i in range(images):
        fr = pl.ds(frame[i], length)
        mixw[...] = mm(sel[i], gmix[fr, :]).astype(bf16)

        def window(w, _):
            poll(i, w)
            ws = pl.ds(pl.multiple_of(w * SEG, SEG), SEG)
            for g in range(NG):
                q = wq[i, ws, g * 128 : (g + 1) * 128]
                k = wq[i, ws, C + g * 128 : C + (g + 1) * 128]
                v = wq[i, ws, 2 * C + g * 128 : 2 * C + (g + 1) * 128]
                pt = probs[i, w * NG + g]
                dod = block_diag(mixw[ws, g * 128 : (g + 1) * 128], head_of_lane)
                gv = mm(pt, dod)
                dpt = mm_t(v, dod)
                ptf = pt.astype(f32)
                prod = ptf * dpt
                dst = prod - ptf * jnp.sum(prod, axis=0, keepdims=True)
                acc[g] += dst
                dsb = dst.astype(bf16)
                gk = mm(dsb, block_diag(q, head_of_lane))
                gq = diag_pick(mm_r(dsb, k), head_of_lane) * HD ** (-0.5)
                gl = slice(g * 128, (g + 1) * 128)
                gvec[2:3, gl] += jnp.sum(gq, axis=0, keepdims=True)
                gvec[3:4, gl] += jnp.sum(gv, axis=0, keepdims=True)
                gwin[ws, g * 128 : (g + 1) * 128] = gq.astype(bf16)
                gwin[ws, C + g * 128 : C + (g + 1) * 128] = gk.astype(bf16)
                gwin[ws, 2 * C + g * 128 : 2 * C + (g + 1) * 128] = gv.astype(bf16)
            return 0

        lax.fori_loop(0, NW, window, 0)
        qkv[fr, :] = (qkv[fr, :].astype(f32) + mm_r(sel[i], gwin[...])).astype(bf16)


def qkv_grads(quad, gb, qkv, ln1):
    for kind in range(3):
        cols = slice(kind * C + quad * 256, kind * C + quad * 256 + 256)
        part = mm_r(qkv[:, cols], ln1[...]).astype(bf16)
        for r in range(4):
            for h in range(2):
                gb[slot(4 * quad + r, 0), h * 192 + kind * 64 : h * 192 + kind * 64 + 64, :] = part[
                    r * 64 : r * 64 + 64, HALVES[h]
                ]


def first_norm_back(x, wb, vecs, qkv, gres, gin, gvec, poll):
    rows = x.shape[0]
    gln = [jnp.zeros((rows, 256), f32)] * 2
    for kind in range(3):
        for quad in range(2):
            poll(2 * kind + quad)
            part = qkv[:, kind * C + quad * 256 : kind * C + quad * 256 + 256]
            gln = [gln[h] + mm(part, w_qkv(wb, kind, quad, h)) for h in range(2)]
    gln = jnp.concatenate(gln, axis=1)
    xin = x[...].astype(f32)
    center, scale = norm_stats(xin)
    unit = (xin - center) * scale
    gvec[0:1, :] = jnp.sum(gln * unit, axis=0, keepdims=True)
    gvec[1:2, :] = jnp.sum(gln, axis=0, keepdims=True)
    gin[...] = (gres[...] + norm_back(gln * vecs[0:1, :], unit, scale)).astype(bf16)


def mega_scratch(images, rows):
    return [
        pltpu.VMEM((rows, C), bf16),
        pltpu.VMEM((rows, 3 * C), bf16),
        pltpu.VMEM((images, NW * SEG, 3 * C), bf16),
        pltpu.VMEM((images, NW * NG, SEG, GH * SEG), bf16),
        pltpu.VMEM((NW * SEG, C), bf16),
        pltpu.VMEM((rows, C), bf16),
        pltpu.VMEM((rows, C), bf16),
        pltpu.VMEM((rows, FF), bf16),
        pltpu.VMEM((rows, FF), bf16),
        pltpu.VMEM((rows, C), bf16),
        pltpu.VMEM((rows, C), f32),
        pltpu.VMEM((rows, C), bf16),
        pltpu.VMEM((NW * SEG, 3 * C), bf16),
        pltpu.VMEM((rows, C), bf16),
    ]


def score_masks():
    _, ids = window_sites()
    size = WIN * WIN
    full = np.zeros((NW, SEG, SEG), np.float32)
    full[:, size:, :] = -1e30
    full[:, :size, :size] = np.where(ids[:, :, None] == ids[:, None, :], 0.0, mask_fill)
    return np.tile(full, (1, 1, GH))


def place():
    d, m = lax.axis_index("dp"), lax.axis_index("mp")
    return d, m, d // 2, d % 2, m // 2, m % 2


def twin(a, j):
    if j == 0:
        return a
    if j == 1:
        return a + 1 - 2 * (a % 2)
    if j == 2:
        return (a + 2) % LINES
    return LINES - 1 - a


def remote(src, dst, send, recv, dev):
    return pltpu.make_async_remote_copy(
        src_ref=src, dst_ref=dst, send_sem=send, recv_sem=recv, device_id=dev, device_id_type=MESH
    )


def peers():
    d, m, *_ = place()
    return [{"dp": (d + k) % DPS, "mp": m} for k in range(1, DPS)] + [
        {"dp": d, "mp": (m + k) % MPS} for k in range(1, MPS)
    ]


def greet():
    barrier = pltpu.get_barrier_semaphore()
    group = peers()
    for dev in group:
        pl.semaphore_signal(barrier, inc=1, device_id=dev, device_id_type=MESH)
    pl.semaphore_wait(barrier, len(group))


OFFSET = 277


def flatten_params(pf, fl, roll, head, head_sem, wide, wb, sm):
    d, m, *_ = place()
    lane = iota((FLAT, 128), 1)
    roll[0:8, :] = jnp.zeros((8, 128), f32)
    fl[FLAT : FLAT + 16, :] = jnp.zeros((16, 128), f32)
    for k in range(DPS):

        @pl.when(d == k)
        def _(k=k):
            lanes, down = OFFSET * k % 128, OFFSET * k // 128
            if k == 0:
                fl[0:FLAT, :] = pf[...]
            else:
                roll[8 : 8 + FLAT, :] = pltpu.roll(pf[...], lanes, 1)
                fl[down : down + FLAT, :] = jnp.where(
                    lane >= lanes, roll[8 : 8 + FLAT, :], roll[7 : 7 + FLAT, :]
                )

    over = remote(fl.at[768:784], head.at[0], head_sem.at[0], head_sem.at[1], {"dp": (d + 1) % DPS, "mp": m})

    @pl.when(d < DPS - 1)
    def _():
        over.start()

    @pl.when(d > 0)
    def _():
        over.wait_recv()
        pos = iota((8, 128), 0) * 128 + iota((8, 128), 1)
        fl[0:8, :] = jnp.where(pos < OFFSET * d, head[0, 0:8, :], fl[0:8, :])

    def cut(start, size, step):
        return fl[pl.ds(start, size, stride=step), :]

    @pl.when(d == 0)
    def _():
        low = iota((256, 128), 1) < 64
        one, two = pltpu.roll(cut(1, 256, 3), 64, 1), pltpu.roll(cut(2, 256, 3), 64, 1)
        wide[pl.ds(0, 256, stride=2), :] = cut(0, 256, 3)
        wide[pl.ds(C, 256, stride=2), :] = cut(1, 256, 3)
        wide[pl.ds(1, 256, stride=2), :] = jnp.where(low, one, two)
        wide[pl.ds(C + 1, 256, stride=2), :] = two
        turned = jnp.concatenate([wide[0:C, :].T, wide[C : 2 * C, :].T], axis=0).astype(bf16)
        s = slot(m, 0)
        for half in range(2):
            for kind in range(3):
                for i in range(2):
                    to = half * 192 + kind * 64 + i * 32
                    frm = i * 96 + kind * 32
                    wb[s, to : to + 32, :] = turned[frm : frm + 32, HALVES[half]]

    @pl.when(d == 1)
    def _():
        s = slot(m, 1)
        for j in range(2):
            js = slice(j * 128, (j + 1) * 128)
            for half in range(2):
                wb[s, half * 64 : half * 64 + 64, js] = cut(2 * half + j, 64, 4).astype(bf16)
            wb[s, 128:384, js] = cut(256 + j, 256, 2).astype(bf16)

    @pl.when(d == 2)
    def _():
        s = slot(m, 2)
        for j in range(2):
            js = slice(j * 128, (j + 1) * 128)
            wb[s, 0:256, js] = cut(j, 256, 2).astype(bf16)
            for half in range(2):
                at = 256 + half * 64
                wb[s, at : at + 64, js] = cut(512 + 2 * half + j, 64, 4).astype(bf16)

    @pl.when(d == 3)
    def _():
        s = slot(m, 3)
        for j in range(2):
            js = slice(j * 128, (j + 1) * 128)
            for half in range(2):
                wb[s, half * 192 : half * 192 + 192, js] = cut(2 * half + j, 192, 4).astype(bf16)
        sm[m] = fl[768:784, :].astype(bf16)

    @pl.when(d < DPS - 1)
    def _():
        over.wait_send()


def smalls_out(sm, ssem, rsem):
    d, m, *_ = place()

    def over_dp(k):
        return remote(sm.at[m], sm.at[m], ssem.at[k], rsem.at[m], {"dp": k, "mp": m})

    def over_mp(k):
        return remote(sm.at[m], sm.at[m], ssem.at[3 + k], rsem.at[m], {"dp": d, "mp": (m + k) % MPS})

    @pl.when(d == DPS - 1)
    def _():
        for k in range(DPS - 1):
            over_dp(k).start()

    @pl.when(d < DPS - 1)
    def _():
        over_dp(0).wait_recv()

    for k in range(1, MPS):
        over_mp(k).start()

    def finish():
        for k in range(1, MPS):
            src = (m + k) % MPS
            remote(sm.at[src], sm.at[src], ssem.at[0], rsem.at[src], {"dp": d, "mp": src}).wait_recv()

    def drain():
        @pl.when(d == DPS - 1)
        def _():
            for k in range(DPS - 1):
                over_dp(k).wait_send()

        for k in range(1, MPS):
            over_mp(k).wait_send()

    return finish, drain


RIGHT, LEFT, SIDE_Y, SIDE_X, CORE = range(5)


class BlocksOut:
    def __init__(self, wb, ssem, rsem):
        self.wb, self.ssem, self.rsem = wb, ssem, rsem
        self.d, self.m, self.x, self.c, self.a, self.b = place()
        d, m, b, c = self.d, self.m, self.b, self.c
        self.far = (d + 2) % DPS
        self.dev = {
            RIGHT: {"dp": d, "mp": (m + 2) % MPS},
            LEFT: {"dp": d, "mp": (m + MPS - 2) % MPS},
            SIDE_Y: {"dp": d, "mp": m + 1 - 2 * b},
            SIDE_X: {"dp": self.far, "mp": m},
            CORE: {"dp": d + 1 - 2 * c, "mp": m},
        }

    def copy(self, s, way):
        return remote(self.wb.at[s], self.wb.at[s], self.ssem.at[s, way], self.rsem.at[s], self.dev[way])

    def arrive(self, s):
        self.copy(s, CORE).wait_recv()

    def ways_of_line(self, core, dd, j):
        a = self.a
        t = twin(a, j)
        if j == 0:
            ways = [(RIGHT, a < LINES - 1), (LEFT, a > 0)]
        else:
            ways = [(RIGHT, (t < a) & (a < LINES - 1)), (LEFT, (t > a) & (a > 0))]
        if core:
            ways.append((SIDE_X, None))
        elif j == 0:
            ways.insert(0, (SIDE_X, self.d == dd))
        return slot(2 * t + self.b, dd), ways + [(SIDE_Y, None), (CORE, None)]

    def ways_of_side(self, core, dd, j):
        ways = [(SIDE_X, None)] if core else []
        return slot(2 * twin(self.a, j) + 1 - self.b, dd), ways + [(CORE, None)]

    def ways_of_cross(self, j, same):
        return slot(2 * twin(self.a, j) + (self.b if same else 1 - self.b), self.far), [(CORE, None)]

    def start(self, s, ways):
        for way, cond in ways:
            if cond is None:
                self.copy(s, way).start()
            else:
                pl.when(cond)(functools.partial(lambda way: self.copy(s, way).start(), way))

    def settle(self, s, ways):
        for way, cond in ways:
            if cond is None:
                self.copy(s, way).wait_send()
            else:
                pl.when(cond)(functools.partial(lambda way: self.copy(s, way).wait_send(), way))

    def line(self, core, dd, j):
        s, ways = self.ways_of_line(core, dd, j)
        if j:
            self.arrive(s)
        elif core == 0:
            pl.when(self.d != dd)(lambda: self.arrive(s))
        self.start(s, ways)

    def side(self, core, dd, j):
        s, ways = self.ways_of_side(core, dd, j)
        self.arrive(s)
        self.start(s, ways)

    def cross(self, j, same):
        s, ways = self.ways_of_cross(j, same)
        self.arrive(s)
        self.start(s, ways)

    def from_core(self, dd):
        for row in range(MPS):
            self.arrive(slot(row, dd))

    def drain(self):
        @pl.when(self.c == 0)
        def _():
            for dd in (0, 2):
                for j in range(LINES):
                    self.settle(*self.ways_of_line(0, dd, j))
                    self.settle(*self.ways_of_side(0, dd, j))

        @pl.when(self.c == 1)
        def _():
            for j in range(LINES):
                self.settle(*self.ways_of_line(1, self.d, j))
                self.settle(*self.ways_of_side(1, self.d, j))
                self.settle(*self.ways_of_cross(j, True))
                self.settle(*self.ways_of_cross(j, False))


def in_turn(n):
    return (3 * n) % LINES


class BlocksIn:
    def __init__(self, gb, rc, rx, ry, rz, total, spare, sems):
        self.gb, self.rc, self.rx, self.ry, self.rz = gb, rc, rx, ry, rz
        self.total, self.spare = total, spare
        self.sems = sems
        self.d, self.m, self.x, self.c, self.a, self.b = place()
        d, m, b, c = self.d, self.m, self.b, self.c
        self.far = (d + 2) % DPS
        self.twin = d + 1 - 2 * c
        self.to_core = {"dp": self.twin, "mp": m}
        self.to_x = {"dp": self.far, "mp": m}
        self.to_y = {"dp": d, "mp": m + 1 - 2 * b}
        self.to_left = {"dp": d, "mp": (m + MPS - 2) % MPS}
        self.to_right = {"dp": d, "mp": (m + 2) % MPS}

    def move(self, s, dst, name, k, part, dev):
        ss, rs = self.sems[name]
        rows = pl.ds(*part[1:])
        return remote(self.gb.at[s, rows], dst.at[rows], ss.at[k, part[0]], rs.at[k, part[0]], dev)

    def by_core(self, row, dd, part):
        k = dd // 2 * MPS + row
        return self.move(slot(row, dd), self.rc.at[k], "core", k, part, self.to_core)

    def by_x(self, k, s, part):
        return self.move(s, self.rx.at[k], "x", k, part, self.to_x)

    def by_y(self, k, t, dd, part):
        return self.move(slot(2 * t + 1 - self.b, dd), self.ry.at[k * LINES + t], "y", k * LINES + t, part, self.to_y)

    def by_z(self, k, t, dd, side, part, dev):
        n = (k * LINES + t) * 2 + side
        return self.move(slot(2 * t + self.b, dd), self.rz.at[n], "z", n, part, dev)

    def add(self, s, part, *got):
        rows = pl.ds(*part[1:])
        value = self.gb[s, rows].astype(f32)
        for ref in got:
            value = value + ref[rows].astype(f32)
        self.gb[s, rows] = value.astype(bf16)

    def along_z(self, k, t, dd, part):
        a = self.a
        s = slot(2 * t + self.b, dd)

        @pl.when((t < a) & (a < LINES - 1))
        def _():
            self.by_z(k, t, dd, 1, part, self.to_left).wait_recv()
            self.add(s, part, self.rz.at[(k * LINES + t) * 2 + 1])

        @pl.when((t > a) & (a > 0))
        def _():
            self.by_z(k, t, dd, 0, part, self.to_right).wait_recv()
            self.add(s, part, self.rz.at[(k * LINES + t) * 2])

        pl.when(t < a)(lambda: self.by_z(k, t, dd, 1, part, self.to_left).start())
        pl.when(t > a)(lambda: self.by_z(k, t, dd, 0, part, self.to_right).start())

    def end_z(self, k, dd, part, to):
        a = self.a
        rows = pl.ds(*part[1:])
        to[rows, :] = self.gb[slot(self.m, dd), rows].astype(f32)

        @pl.when(a < LINES - 1)
        def _():
            self.by_z(k, a, dd, 1, part, self.to_left).wait_recv()
            to[rows, :] += self.rz[(k * LINES + a) * 2 + 1, rows].astype(f32)

        @pl.when(a > 0)
        def _():
            self.by_z(k, a, dd, 0, part, self.to_right).wait_recv()
            to[rows, :] += self.rz[(k * LINES + a) * 2, rows].astype(f32)

    def zero_over(self, dd, t, part):
        row = 2 * t + 1 - self.b
        self.by_core(row, dd, part).wait_recv()
        self.add(slot(row, dd), part, self.rc.at[dd // 2 * MPS + row])
        self.by_y(dd // 2, t, dd, part).start()

    def zero_own(self, dd, t, part):
        row = 2 * t + self.b
        k = dd // 2
        self.by_core(row, dd, part).wait_recv()
        self.by_y(k, t, dd, part).wait_recv()
        self.add(slot(row, dd), part, self.rc.at[k * MPS + row], self.ry.at[k * LINES + t])
        self.along_z(k, t, dd, part)

    def zero_end(self, dd, part):
        k = dd // 2
        s = slot(self.m, dd)
        rows = pl.ds(*part[1:])
        self.end_z(k, dd, part, self.spare)

        @pl.when(self.d != dd)
        def _():
            self.gb[s, rows] = self.spare[rows, :].astype(bf16)
            self.by_x(k, s, part).start()

        @pl.when(self.d == dd)
        def _():
            self.by_x(k, s, part).wait_recv()
            self.total[rows, :] = self.spare[rows, :] + self.rx[k, rows].astype(f32)

    def one_end(self, part):
        self.end_z(0, self.d, part, self.total)

    def one_far(self, n, part):
        t = in_turn(n)
        row = 2 * t + self.b + (1 - 2 * self.b) * (1 - n // LINES)
        dd = self.far
        self.by_core(row, dd, part).wait_recv()
        self.add(slot(row, dd), part, self.rc.at[dd // 2 * MPS + row])
        self.by_x(row, slot(row, dd), part).start()

    def one_over(self, t, part):
        row = 2 * t + 1 - self.b
        dd = self.d
        self.by_core(row, dd, part).wait_recv()
        self.by_x(row, slot(row, dd), part).wait_recv()
        self.add(slot(row, dd), part, self.rc.at[dd // 2 * MPS + row], self.rx.at[row])
        self.by_y(0, t, dd, part).start()

    def one_own(self, t, part):
        row = 2 * t + self.b
        dd = self.d
        self.by_core(row, dd, part).wait_recv()
        self.by_x(row, slot(row, dd), part).wait_recv()
        self.by_y(0, t, dd, part).wait_recv()
        self.add(slot(row, dd), part, self.rc.at[dd // 2 * MPS + row], self.rx.at[row], self.ry.at[t])
        self.along_z(0, t, dd, part)

    def drain_tree(self, core, dd, part):
        k = dd // 2 if core == 0 else 0
        a = self.a
        for t in range(LINES):
            self.by_y(k, t, dd, part).wait_send()
            pl.when(t < a)(functools.partial(self.wait_z, k, t, dd, 1, part))
            pl.when(t > a)(functools.partial(self.wait_z, k, t, dd, 0, part))
        if core == 0:
            pl.when(self.d != dd)(lambda: self.by_x(k, slot(self.m, dd), part).wait_send())
        else:
            for row in range(MPS):
                self.by_x(row, slot(row, self.far), part).wait_send()

    def wait_z(self, k, t, dd, side, part):
        self.by_z(k, t, dd, side, part, self.to_left if side else self.to_right).wait_send()


WHOLE = ((0, 0, QROWS),)
PARTS = ((0, 0, QROWS // 2), (1, QROWS // 2, QROWS // 2))


def smalls_in(gsm, got, part, got2, total, ssem, rsem, rsem2):
    d, m, *_ = place()

    def over_mp(k):
        dst = (m + k) % MPS
        return remote(gsm.at[dst], got.at[k], ssem.at[k], rsem.at[k], {"dp": d, "mp": dst})

    def over_dp(k):
        return remote(part, got2.at[k], ssem.at[0], rsem2.at[k], {"dp": DPS - 1, "mp": m})

    for k in range(1, MPS):
        over_mp(k).start()

    def middle():
        value = gsm[m]
        for k in range(1, MPS):
            over_mp(k).wait_recv()
            value = value + got[k]
        part[...] = value
        for k in range(DPS - 1):
            pl.when(d == k)(lambda k=k: over_dp(k).start())

    def end():
        @pl.when(d == DPS - 1)
        def _():
            total[...] = part[...]
            for k in range(DPS - 1):
                over_dp(k).wait_recv()
                total[...] += got2[k]

    def drain():
        for k in range(DPS - 1):
            pl.when(d == k)(lambda k=k: over_dp(k).wait_send())
        for k in range(1, MPS):
            over_mp(k).wait_send()

    return middle, end, drain


def flat_grads(total, smalls, fl, roll, head, head_sem, wide, tall, gflat):
    d, m, *_ = place()
    fl[768:792, :] = jnp.zeros((24, 128), f32)

    def put(start, size, step, val):
        fl[pl.ds(start, size, stride=step), :] = val

    @pl.when(d == 0)
    def _():
        tall[192:256, :] = jnp.zeros((64, C), f32)
        for half in range(2):
            for kind in range(3):
                for i in range(2):
                    frm = half * 192 + kind * 64 + i * 32
                    to = i * 96 + kind * 32
                    tall[to : to + 32, HALVES[half]] = total[frm : frm + 32, :]
        wide[0:C, :] = tall[0:128, :].T
        wide[C : 2 * C, :] = tall[128:256, :].T
        low = iota((256, 128), 1) < 64

        def every(start):
            return wide[pl.ds(start, 256, stride=2), :]

        one, two = pltpu.roll(every(1), 64, 1), pltpu.roll(every(C + 1), 64, 1)
        put(0, 256, 3, every(0))
        put(1, 256, 3, jnp.where(low, every(C), one))
        put(2, 256, 3, jnp.where(low, one, two))

    @pl.when(d == 1)
    def _():
        for j in range(2):
            js = slice(j * 128, (j + 1) * 128)
            for half in range(2):
                put(2 * half + j, 64, 4, total[half * 64 : half * 64 + 64, js])
            put(256 + j, 256, 2, total[128:384, js])

    @pl.when(d == 2)
    def _():
        for j in range(2):
            js = slice(j * 128, (j + 1) * 128)
            put(j, 256, 2, total[0:256, js])
            for half in range(2):
                at = 256 + half * 64
                put(512 + 2 * half + j, 64, 4, total[at : at + 64, js])

    @pl.when(d == 3)
    def _():
        for j in range(2):
            js = slice(j * 128, (j + 1) * 128)
            for half in range(2):
                put(2 * half + j, 192, 4, total[half * 192 : half * 192 + 192, js])
        fl[768:784, :] = smalls[...]

    back = remote(fl.at[0:8], head.at[1, 0:8], head_sem.at[2], head_sem.at[3], {"dp": (d + DPS - 1) % DPS, "mp": m})

    @pl.when(d > 0)
    def _():
        back.start()

    @pl.when(d < DPS - 1)
    def _():
        back.wait_recv()
        fl[768:776, :] = head[1, 0:8, :]

    lane = iota((FLAT, 128), 1)
    for k in range(DPS):

        @pl.when(d == k)
        def _(k=k):
            lanes, down = OFFSET * k % 128, OFFSET * k // 128
            if k == 0:
                gflat[...] = fl[0:FLAT, :]
            else:
                roll[0:784, :] = pltpu.roll(fl[0:784, :], 128 - lanes, 1)
                roll[784:792, :] = jnp.zeros((8, 128), f32)
                gflat[...] = jnp.where(lane < 128 - lanes, roll[down : down + FLAT, :], roll[down + 1 : down + 1 + FLAT, :])

    @pl.when(d > 0)
    def _():
        back.wait_send()


def step_kernel(images, rows, length, *refs):
    (nlive, x, cot, pf, sel, mask) = refs[:6]
    (out, gin, gflat) = refs[6:9]
    (
        fl, roll, head, wide, tall, wb, sm, vecs, b1, tabs, tabs2, bias, gvec, gb1, acc, gb, gsm, got, part, got2,
        stotal, rc, rx, ry, rz, total, spare,
        head_sem, sm_s, sm_r, ag_s, ag_r, rsm_s, rsm_r, rsm_r2, s_core, r_core, s_x, r_x, s_y, r_y, s_z, r_z,
    ) = refs[9:52]
    ln1, qkv, wq, probs, mixw, mixed, ln2, act, gpre, gresb, gres, gmix, gwin, goutb = refs[52:]
    greet()
    flatten_params(pf, fl, roll, head, head_sem, wide, wb, sm)
    outs = BlocksOut(wb, ag_s, ag_r)
    c = outs.c
    zero, one = c == 0, c == 1
    pl.when(zero)(lambda: outs.line(0, 0, 0))
    finish_sm, drain_sm = smalls_out(sm, sm_s, sm_r)

    @pl.when(zero)
    def _():
        outs.line(0, 0, 1)
        outs.side(0, 0, 0)

    finish_sm()
    gather_smalls(sm, vecs, b1, tabs, bias, mask)

    @pl.when(zero)
    def _():
        outs.line(0, 0, 2)
        outs.side(0, 0, 1)

    first_norm(x, vecs, ln1)

    @pl.when(zero)
    def _():
        outs.line(0, 0, 3)
        outs.side(0, 0, 2)
        outs.side(0, 0, 3)

    @pl.when(one)
    def _():
        outs.from_core(0)
        outs.line(1, outs.d, 0)

    def two(fn, *args):
        return functools.partial(fn, 0, 2, *args)

    def mine(fn, *args):
        return functools.partial(fn, 1, outs.d, *args)

    def cross(j, same):
        return functools.partial(outs.cross, j, same)

    zero_at = {
        1: [two(outs.line, 0)],
        4: [two(outs.line, 1)],
        5: [two(outs.side, 0)],
        8: [two(outs.line, 2)],
        9: [two(outs.side, 1)],
        12: [two(outs.line, 3)],
        13: [two(outs.side, 2)],
        17: [two(outs.side, 3)],
    }
    one_at = {
        4: [mine(outs.line, 1)],
        5: [mine(outs.side, 0)],
        6: [cross(0, True)],
        8: [mine(outs.line, 2)],
        9: [mine(outs.side, 1)],
        10: [cross(1, True), cross(0, False)],
        12: [mine(outs.line, 3), mine(outs.side, 2)],
        14: [cross(2, True), cross(1, False)],
        17: [mine(outs.side, 3)],
        19: [cross(3, True), cross(2, False)],
        21: [cross(3, False)],
    }

    def run(zeros, ones):
        if zeros:
            pl.when(zero)(lambda: [fn() for fn in zeros] and None)
        if ones:
            pl.when(one)(lambda: [fn() for fn in ones] and None)

    def at_point(zero_table, one_table, point):
        run(zero_table.get(point), one_table.get(point))

    def poll_project(n):
        at_point(zero_at, one_at, n)

    def poll_forward(i, w):
        for k in range(NW):
            point = 6 + NW * i + k
            if point in zero_at or point in one_at:
                pl.when(w == k)(functools.partial(at_point, zero_at, one_at, point))

    project_qkv(wb, vecs, ln1, qkv, poll_project)
    attention_forward(images, length, sel, bias, qkv, wq, probs, mixw, mixed, poll_forward)

    @pl.when(zero)
    def _():
        outs.from_core(1)
        outs.from_core(3)

    pl.when(one)(lambda: outs.from_core(2))

    feed_forward(
        rows, nlive[0], x, cot, wb, vecs, b1, out, gvec, gb1, mixed, ln2, act, gpre, gresb, gres, gmix, goutb
    )
    proj_grads(gb, mixed, gresb)
    ins = BlocksIn(
        gb, rc, rx, ry, rz, total, spare, {"core": (s_core, r_core), "x": (s_x, r_x), "y": (s_y, r_y), "z": (s_z, r_z)}
    )
    whole = WHOLE[0]

    def hand_over(row):
        @pl.when(zero)
        def _():
            for dd in (1, 3):
                ins.by_core(row, dd, whole).start()

        pl.when(one)(lambda: ins.by_core(row, 2, whole).start())

    def grads(n, _):
        t = in_turn(n)
        row = 2 * t + ins.b + (1 - 2 * ins.b) * (1 - n // LINES)
        feed_forward_grads(row, gb, act, goutb, ln2, gpre)
        hand_over(row)

        @pl.when((n >= 1) & one)
        def _():
            ins.one_far(n - 1, whole)

        @pl.when((n >= 1) & (n <= LINES) & zero)
        def _():
            ins.zero_over(2, in_turn(n - 1), whole)

        return 0

    lax.fori_loop(0, MPS, grads, 0)

    turn = [in_turn(n) for n in range(LINES)]
    zero_at = {
        3: [functools.partial(ins.zero_own, 2, turn[0], whole)],
        5: [functools.partial(ins.zero_own, 2, turn[1], whole)],
        7: [functools.partial(ins.zero_own, 2, turn[2], whole)],
        9: [functools.partial(ins.zero_own, 2, turn[3], whole)],
        13: [functools.partial(ins.zero_end, 2, whole)],
    }
    one_at = {
        0: [functools.partial(ins.one_far, MPS - 1, whole)],
        1: [functools.partial(ins.one_over, turn[0], whole)],
        2: [functools.partial(ins.one_over, turn[1], whole)],
        4: [functools.partial(ins.one_over, turn[2], whole)],
        5: [functools.partial(ins.one_over, turn[3], whole)],
        8: [functools.partial(ins.one_own, turn[0], whole)],
        10: [functools.partial(ins.one_own, turn[1], whole)],
        12: [functools.partial(ins.one_own, turn[2], whole)],
        14: [functools.partial(ins.one_own, turn[3], whole)],
    }

    def poll_backward(i, w):
        for k in range(NW):
            point = NW * i + k
            if point in zero_at or point in one_at:
                pl.when(w == k)(functools.partial(at_point, zero_at, one_at, point))

    attention_backward(images, length, sel, gmix, wq, probs, mixw, gwin, qkv, acc, gvec, poll_backward)

    order = (0, 1, 3, 2)

    def hand_first(rows_of):
        @pl.when(one)
        def _():
            for row in rows_of:
                for part in PARTS:
                    ins.by_core(row, 0, part).start()

    qkv_grads(0, gb, qkv, ln1)
    hand_first(range(MPS // 2))
    qkv_grads(1, gb, qkv, ln1)
    hand_first(range(MPS // 2, MPS))
    def both_parts(fn, t):
        return [functools.partial(fn, 0, t, part) for part in PARTS]

    zero_at = {
        0: both_parts(ins.zero_over, order[0]),
        1: both_parts(ins.zero_over, order[1]),
        2: both_parts(ins.zero_over, order[2]),
        3: both_parts(ins.zero_over, order[3]),
        5: both_parts(ins.zero_own, order[0]),
    }
    one_at = {0: [functools.partial(ins.one_end, whole)]}
    first_norm_back(x, wb, vecs, qkv, gres, gin, gvec, functools.partial(at_point, zero_at, one_at))
    scatter_smalls(gvec, gb1, acc, gsm, tabs2)
    mid_sm, end_sm, drain_in = smalls_in(gsm, got, part, got2, stotal, rsm_s, rsm_r, rsm_r2)

    @pl.when(zero)
    def _():
        for fn in both_parts(ins.zero_own, order[1]):
            fn()

    mid_sm()

    @pl.when(zero)
    def _():
        for t in order[2:]:
            for fn in both_parts(ins.zero_own, t):
                fn()

    end_sm()

    @pl.when(zero)
    def _():
        for part in PARTS:
            ins.zero_end(0, part)

    flat_grads(total, stotal, fl, roll, head, head_sem, wide, tall, gflat)

    @pl.when(zero)
    def _():
        for row in range(MPS):
            for dd in (1, 3):
                ins.by_core(row, dd, whole).wait_send()
        ins.drain_tree(0, 2, whole)
        for part in PARTS:
            ins.drain_tree(0, 0, part)

    @pl.when(one)
    def _():
        for row in range(MPS):
            ins.by_core(row, 2, whole).wait_send()
            for part in PARTS:
                ins.by_core(row, 0, part).wait_send()
        ins.drain_tree(1, ins.d, whole)

    drain_in()
    outs.drain()
    drain_sm()


def step_call(x, cot, nlive, pf):
    rows = x.shape[0]
    images = rows // PIX
    length = image_frames(images)[2]
    sel = jnp.asarray(placement(images), bf16)
    mask = jnp.asarray(score_masks(), f32)
    vmem = pl.BlockSpec(memory_space=pltpu.VMEM)
    smem = pl.BlockSpec(memory_space=pltpu.SMEM)
    s = jax.ShapeDtypeStruct
    dma = pltpu.SemaphoreType.DMA
    nb = MPS * DPS
    return pl.pallas_call(
        functools.partial(step_kernel, images, rows, length),
        out_shape=(s((rows, C), bf16), s((rows, C), bf16), s((FLAT, 128), f32)),
        in_specs=[smem] + [vmem] * 5,
        out_specs=(vmem,) * 3,
        scratch_shapes=[
            pltpu.VMEM((792, 128), f32),
            pltpu.VMEM((792, 128), f32),
            pltpu.VMEM((2, 16, 128), f32),
            pltpu.VMEM((2 * C, 128), f32),
            pltpu.VMEM((256, C), f32),
            pltpu.VMEM((nb, QROWS, 256), bf16),
            pltpu.VMEM((MPS, 16, 128), bf16),
            pltpu.VMEM((8, C), f32),
            pltpu.VMEM((1, FF), f32),
            pltpu.VMEM((MPS, 384), f32),
            pltpu.VMEM((MPS, 512), f32),
            pltpu.VMEM((NW * NG, SEG, GH * SEG), f32),
            pltpu.VMEM((8, C), f32),
            pltpu.VMEM((1, FF), f32),
            pltpu.VMEM((NG, SEG, GH * SEG), f32),
            pltpu.VMEM((nb, QROWS, 256), bf16),
            pltpu.VMEM((MPS, 16, 128), f32),
            pltpu.VMEM((MPS, 16, 128), f32),
            pltpu.VMEM((16, 128), f32),
            pltpu.VMEM((DPS, 16, 128), f32),
            pltpu.VMEM((16, 128), f32),
            pltpu.VMEM((2 * MPS, QROWS, 256), bf16),
            pltpu.VMEM((MPS, QROWS, 256), bf16),
            pltpu.VMEM((2 * LINES, QROWS, 256), bf16),
            pltpu.VMEM((4 * LINES, QROWS, 256), bf16),
            pltpu.VMEM((QROWS, 256), f32),
            pltpu.VMEM((QROWS, 256), f32),
            dma((4,)),
            dma((3 + MPS,)),
            dma((MPS,)),
            dma((nb, 5)),
            dma((nb,)),
            dma((MPS,)),
            dma((MPS,)),
            dma((DPS,)),
            dma((2 * MPS, 2)),
            dma((2 * MPS, 2)),
            dma((MPS, 2)),
            dma((MPS, 2)),
            dma((2 * LINES, 2)),
            dma((2 * LINES, 2)),
            dma((4 * LINES, 2)),
            dma((4 * LINES, 2)),
        ]
        + mega_scratch(images, rows),
        compiler_params=pltpu.CompilerParams(
            vmem_limit_bytes=62 * 1024 * 1024, collective_id=0, has_side_effects=True
        ),
    )(nlive, x, cot, pf, sel, mask)


VEC_LABELS = [
    "norm1_gain",
    "norm1_bias",
    "query_bias",
    "value_bias",
    "proj_bias",
    "norm2_gain",
    "norm2_bias",
    "fc2_bias",
]


def segment_shapes(width_rank, hidden_rank):
    return [
        ("qkv_weight", (C, 3 * width_rank)),
        ("proj_weight", (width_rank, C)),
        ("fc1_weight", (C, hidden_rank)),
        ("fc2_weight", (hidden_rank, C)),
        ("norm1_gain", (width_rank,)),
        ("norm1_bias", (width_rank,)),
        ("query_bias", (width_rank,)),
        ("value_bias", (width_rank,)),
        ("proj_bias", (width_rank,)),
        ("norm2_gain", (width_rank,)),
        ("norm2_bias", (width_rank,)),
        ("fc1_bias", (hidden_rank,)),
        ("fc2_bias", (width_rank,)),
        ("table", (SPAN * SPAN, width_rank // HD)),
    ]


def unpack(flat, width_rank, hidden_rank):
    pieces = {}
    offset = 0
    for label, shape in segment_shapes(width_rank, hidden_rank):
        amount = math.prod(shape)
        pieces[label] = flat[:, offset : offset + amount].reshape((flat.shape[0],) + shape)
        offset = offset + amount
    return pieces


def finish(output, grad_input, grad_shard, params, moment_one, moment_two):
    group = lax.axis_index("dp")
    shard_length = params.shape[1]
    weights_rank = (4 * C * C + 2 * C * FF) // lax.axis_size("mp")
    position = group * shard_length + jnp.arange(shard_length, dtype=jnp.int32)[None, :]
    decays = (position < weights_rank).astype(jnp.float32)
    new_one = beta_one * moment_one + (1.0 - beta_one) * grad_shard
    new_two = second_decay_rate * moment_two + (1.0 - second_decay_rate) * grad_shard * grad_shard
    corrected_one = new_one / (1.0 - beta_one**adam_step)
    corrected_two = new_two / (1.0 - second_decay_rate**adam_step)
    new_params = params - learn_rate * (
        corrected_one / (jnp.sqrt(corrected_two) + adam_eps) + weight_decay * decays * params
    )
    return (output, grad_input, grad_shard, new_params, new_one, new_two)


def local_xla(tokens, cotangent, image_counts, params, moment_one, moment_two):
    ranks = lax.axis_size("mp")
    rank = lax.axis_index("mp")
    group = lax.axis_index("dp")
    width = C // ranks
    hidden = FF // ranks
    heads = width // HD
    rows = tokens.shape[0]
    shard_length = params.shape[1]
    length = shard_length * lax.axis_size("dp")
    owned = lax.all_gather(params.astype(bf16), "mp", axis=0, tiled=True)
    owned = lax.all_gather(owned, "dp", axis=1, tiled=True)
    op = unpack(owned, width, hidden)
    wqkv = op["qkv_weight"].reshape(ranks, C, heads, 3, HD).transpose(3, 0, 2, 4, 1).reshape(3 * C, C)
    wproj = op["proj_weight"].reshape(C, C)
    w1 = op["fc1_weight"].transpose(1, 0, 2).reshape(C, FF)
    w2 = op["fc2_weight"].reshape(FF, C)
    vecs = jnp.stack([op[n].reshape(C) for n in VEC_LABELS]).astype(f32)
    b1 = op["fc1_bias"].reshape(1, FF).astype(f32)
    bias = score_bias(op["table"].transpose(1, 0, 2).reshape(-1, HEADS))
    limit = jnp.sum(
        jnp.where(jnp.arange(image_counts.shape[0], dtype=jnp.int32) == group, image_counts, 0)
    )
    nlive = jnp.clip(limit * PIX - rank * rows, 0, rows).reshape(1)
    output, grad_input, gqkv, gproj, g1, g2, gvec, gb1, acc = block_compute(
        tokens, cotangent, nlive, wqkv, wproj, w1, w2, vecs, b1, bias
    )
    gtable = table_back(acc)
    gvec = gvec.reshape(8, ranks, width)
    pieces = [
        gqkv.reshape(3, ranks, heads, HD, C).transpose(1, 4, 2, 0, 3).reshape(ranks, -1),
        gproj.reshape(ranks, -1),
        g1.reshape(C, ranks, hidden).transpose(1, 0, 2).reshape(ranks, -1),
        g2.T.reshape(ranks, -1),
    ]
    pieces += [gvec[i].astype(bf16) for i in range(7)]
    pieces += [gb1.reshape(ranks, hidden).astype(bf16), gvec[7].astype(bf16)]
    pieces += [gtable.reshape(-1, ranks, heads).transpose(1, 0, 2).reshape(ranks, -1).astype(bf16)]
    used = sum(p.shape[1] for p in pieces)
    pieces.append(jnp.zeros((ranks, length - used), bf16))
    flat = jnp.concatenate(pieces, axis=1)
    flat = lax.psum_scatter(flat, "mp", scatter_dimension=0, tiled=True)
    grad_shard = lax.psum_scatter(flat, "dp", scatter_dimension=1, tiled=True).astype(f32)
    return finish(output, grad_input, grad_shard, params, moment_one, moment_two)


def local(tokens, cotangent, image_counts, params, moment_one, moment_two):
    ranks = lax.axis_size("mp")
    rows = tokens.shape[0]
    shard = params.shape[1]
    fits = (
        ranks == MPS
        and lax.axis_size("dp") == DPS
        and rows % 16 == 0
        and image_frames(rows // PIX)[0][-1] + image_frames(rows // PIX)[2] <= rows
        and shard == QUART + OFFSET
    )
    if not fits:
        return local_xla(tokens, cotangent, image_counts, params, moment_one, moment_two)
    rank = lax.axis_index("mp")
    group = lax.axis_index("dp")
    limit = jnp.sum(
        jnp.where(jnp.arange(image_counts.shape[0], dtype=jnp.int32) == group, image_counts, 0)
    )
    nlive = jnp.clip(limit * PIX - rank * rows, 0, rows).reshape(1)
    pf = jnp.pad(params, ((0, 0), (0, FLAT * 128 - shard))).reshape(FLAT, 128)
    output, grad_input, gflat = step_call(tokens, cotangent, nlive, pf)
    grad_shard = gflat.reshape(1, -1)[:, :shard]
    return finish(output, grad_input, grad_shard, params, moment_one, moment_two)


def solution(mesh):
    return jax.shard_map(
        local,
        mesh=mesh,
        in_specs=(
            P(("dp", "mp"), None),
            P(("dp", "mp"), None),
            P(),
            P("mp", "dp"),
            P("mp", "dp"),
            P("mp", "dp"),
        ),
        out_specs=(
            P(("dp", "mp"), None),
            P(("dp", "mp"), None),
            P("mp", "dp"),
            P("mp", "dp"),
            P("mp", "dp"),
            P("mp", "dp"),
        ),
        check_vma=False,
    )
```

```python
import functools
import math

import jax
import jax.numpy as jnp
import numpy as np
from jax import lax
from jax.experimental import pallas as pl
from jax.experimental.pallas import tpu as pltpu
from jax.sharding import PartitionSpec as P

C = 512
FF = 2048
HD = 32
WIN = 7
MAP = 14
SHIFT = 3
PIX = MAP * MAP
HEADS = C // HD
SEG = 64
GH = 4
NG = HEADS // GH
SIDE = MAP // WIN
NW = SIDE * SIDE
SPAN = 2 * WIN - 1

norm_eps = 1e-05
mask_fill = -100.0
learn_rate = 0.05
beta_one = 0.9
second_decay_rate = 0.999
adam_eps = 1e-08
weight_decay = 0.05
adam_step = 2.0
f32 = jnp.float32
bf16 = jnp.bfloat16


def mm(a, b):
    return lax.dot_general(a, b, (((1,), (0,)), ((), ())), preferred_element_type=f32)


def mm_t(a, b):
    return lax.dot_general(a, b, (((1,), (1,)), ((), ())), preferred_element_type=f32)


def mm_r(a, b):
    return lax.dot_general(a, b, (((0,), (0,)), ((), ())), preferred_element_type=f32)


def norm_stats(values):
    center = jnp.mean(values, axis=1, keepdims=True)
    spread = jnp.mean(jnp.square(values - center), axis=1, keepdims=True)
    return center, lax.rsqrt(spread + norm_eps)


def norm_back(scaled, unit, scale):
    return scale * (
        scaled
        - jnp.mean(scaled, axis=1, keepdims=True)
        - unit * jnp.mean(scaled * unit, axis=1, keepdims=True)
    )


def phi_parts(v):
    return 0.5 * (1.0 + lax.erf(v * (1.0 / math.sqrt(2.0)))), jnp.exp(-0.5 * v * v)


def window_sites():
    w = np.arange(NW)[:, None]
    p = np.arange(WIN * WIN)[None, :]
    row = (w // SIDE) * WIN + p // WIN
    col = (w % SIDE) * WIN + p % WIN
    token = ((row + SHIFT) % MAP) * MAP + (col + SHIFT) % MAP

    def region(c):
        return (c >= MAP - WIN).astype(np.int32) + (c >= MAP - SHIFT).astype(np.int32)

    ids = region(row) * 3 + region(col)
    return token, ids


def image_frames(images):
    starts = [PIX * i // 16 * 16 for i in range(images)]
    offsets = [PIX * i - s for i, s in enumerate(starts)]
    length = -(-(PIX + max(offsets)) // 16) * 16
    return starts, offsets, length


def placement(images):
    token, _ = window_sites()
    starts, offsets, length = image_frames(images)
    sel = np.zeros((images, NW * SEG, length), np.float32)
    for i in range(images):
        for w in range(NW):
            sel[i, w * SEG + np.arange(WIN * WIN), token[w] + offsets[i]] = 1.0
    return sel


def score_bias(table):
    size = WIN * WIN
    p = np.arange(size)
    a, b = p // WIN, p % WIN
    off = (a[None, :] - a[:, None] + WIN - 1) * SPAN + b[None, :] - b[:, None] + WIN - 1
    one_hot = np.zeros((size, size, SPAN * SPAN), np.float32)
    one_hot[np.arange(size)[:, None], np.arange(size)[None, :], off] = 1.0
    _, ids = window_sites()
    full_mask = np.full((NW, SEG, SEG), 0.0, np.float32)
    full_mask[:, size:, :] = -1e30
    full_mask[:, :size, :size] = np.where(ids[:, :, None] == ids[:, None, :], 0.0, mask_fill)
    onehot = jnp.asarray(one_hot.reshape(size * size, -1), bf16)
    bias = jnp.dot(table.T.astype(bf16), onehot.T, preferred_element_type=f32)
    bias = bias.reshape(NG, GH, size, size)
    bias = jnp.pad(bias, ((0, 0), (0, 0), (0, SEG - size), (0, SEG - size)))
    bias = bias.transpose(0, 2, 1, 3)
    out = bias[None] + jnp.asarray(full_mask)[:, None, :, None, :]
    return out.reshape(NW * NG, SEG, GH * SEG)


def table_back(acc):
    size = WIN * WIN
    p = np.arange(size)
    a, b = p // WIN, p % WIN
    off = (a[None, :] - a[:, None] + WIN - 1) * SPAN + b[None, :] - b[:, None] + WIN - 1
    one_hot = np.zeros((size * size, SPAN * SPAN), np.float32)
    one_hot[np.arange(size * size), off.reshape(-1)] = 1.0
    acc = acc.reshape(NG, SEG, GH, SEG)[:, :size, :, :size].transpose(0, 2, 1, 3).reshape(HEADS, size * size)
    hi = acc.astype(bf16)
    lo = (acc - hi.astype(f32)).astype(bf16)
    oh = jnp.asarray(one_hot, bf16)
    return (
        jnp.dot(hi, oh, preferred_element_type=f32) + jnp.dot(lo, oh, preferred_element_type=f32)
    ).T


def lane_head_mask():
    return lax.broadcasted_iota(jnp.int32, (SEG, GH * HD), 1) // HD


def block_diag(part, head_of_lane):
    zero = jnp.zeros_like(part)
    return jnp.concatenate([jnp.where(head_of_lane == h, part, zero) for h in range(GH)], axis=0)


def diag_pick(full, head_of_lane):
    out = full[:SEG]
    for h in range(1, GH):
        out = jnp.where(head_of_lane == h, full[h * SEG : (h + 1) * SEG], out)
    return out


def compute_kernel(
    images, rows, block, length,
    nlive, x, cot, wqkv, wproj, w1, w2, vecs, b1, bias, sel,
    out, gin, gqkv_w, gproj_w, g1_w, g2_w, gvec, gb1, acc,
    ln1, qkv, wq, probs, mixw, mixed, ln2, act, gpre, gresb, gres, gmix, gwin,
):
    blocks = rows // block
    frame = image_frames(images)[0]
    head_of_lane = lane_head_mask()

    def vec(i):
        return vecs[i : i + 1, :]

    gvec[...] = jnp.zeros_like(gvec)
    gb1[...] = jnp.zeros_like(gb1)
    acc[...] = jnp.zeros_like(acc)
    mixed[...] = jnp.zeros_like(mixed)

    def norm_rows(t, _):
        sl = pl.ds(pl.multiple_of(t * block, 16), block)
        xin = x[sl, :].astype(f32)
        center, scale = norm_stats(xin)
        normed = ((xin - center) * scale * vec(0) + vec(1)).astype(bf16)
        ln1[sl, :] = normed
        qkv[sl, 0:C] = ((mm_t(normed, wqkv[0:C, :]) + vec(2)) * HD ** (-0.5)).astype(bf16)
        qkv[sl, C : 2 * C] = mm_t(normed, wqkv[C : 2 * C, :]).astype(bf16)
        qkv[sl, 2 * C : 3 * C] = (mm_t(normed, wqkv[2 * C : 3 * C, :]) + vec(3)).astype(bf16)
        return 0

    lax.fori_loop(0, blocks, norm_rows, 0)

    for i in range(images):
        fr = pl.ds(frame[i], length)
        wq[i] = mm(sel[i], qkv[fr, :]).astype(bf16)

        def window(w, _):
            ws = pl.ds(pl.multiple_of(w * SEG, SEG), SEG)
            for g in range(NG):
                q = wq[i, ws, g * 128 : (g + 1) * 128]
                k = wq[i, ws, C + g * 128 : C + (g + 1) * 128]
                v = wq[i, ws, 2 * C + g * 128 : 2 * C + (g + 1) * 128]
                st = mm_t(k, block_diag(q, head_of_lane)) + bias[w * NG + g]
                e = jnp.exp(st - jnp.max(st, axis=0, keepdims=True))
                pt = (e * (1.0 / jnp.sum(e, axis=0, keepdims=True))).astype(bf16)
                probs[i, w * NG + g] = pt
                mixw[ws, g * 128 : (g + 1) * 128] = diag_pick(mm_r(pt, v), head_of_lane).astype(bf16)
            return 0

        lax.fori_loop(0, NW, window, 0)
        mixed[fr, :] = (mixed[fr, :].astype(f32) + mm_r(sel[i], mixw[...])).astype(bf16)

    def middle(t, _):
        sl = pl.ds(pl.multiple_of(t * block, 16), block)
        xin = x[sl, :].astype(f32)
        res = xin + (mm(mixed[sl, :], wproj[...]) + vec(4))
        center, scale = norm_stats(res)
        unit = (res - center) * scale
        normed = (unit * vec(5) + vec(6)).astype(bf16)
        ln2[sl, :] = normed
        live = (
            lax.broadcasted_iota(jnp.int32, (block, 1), 0) + t * block < nlive[0]
        ).astype(f32)
        gout = live * cot[sl, :].astype(f32)
        goutb = gout.astype(bf16)
        feed = jnp.zeros((block, C), f32)
        gln = jnp.zeros((block, C), f32)
        for j in range(4):
            js = slice(j * 512, (j + 1) * 512)
            pre = mm(normed, w1[:, js]) + b1[:, js]
            phi, e = phi_parts(pre)
            av = (pre * phi).astype(bf16)
            act[sl, js] = av
            feed = feed + mm(av, w2[js, :])
            gp = mm_t(goutb, w2[js, :]) * (phi + pre * (e * (1.0 / math.sqrt(2.0 * math.pi))))
            gb1[:, js] += jnp.sum(gp, axis=0, keepdims=True)
            gpb = gp.astype(bf16)
            gpre[sl, js] = gpb
            gln = gln + mm_t(gpb, w1[:, js])
        out[sl, :] = (live * (res + feed + vec(7))).astype(bf16)
        gr = gout + norm_back(gln * vec(5), unit, scale)
        gres[sl, :] = gr
        grb = gr.astype(bf16)
        gresb[sl, :] = grb
        gmix[sl, :] = mm_t(grb, wproj[...]).astype(bf16)
        gvec[4:5, :] += jnp.sum(gr, axis=0, keepdims=True)
        gvec[5:6, :] += jnp.sum(gln * unit, axis=0, keepdims=True)
        gvec[6:7, :] += jnp.sum(gln, axis=0, keepdims=True)
        gvec[7:8, :] += jnp.sum(gout, axis=0, keepdims=True)
        return 0

    lax.fori_loop(0, blocks, middle, 0)

    def masked_cot():
        live = (lax.broadcasted_iota(jnp.int32, (rows, 1), 0) < nlive[0]).astype(bf16)
        return cot[...] * live

    gout_all = masked_cot()

    def ff_grads(j, _):
        js = pl.ds(pl.multiple_of(j * 256, 256), 256)
        g2_w[:, js] = mm_r(gout_all, act[:, js]).astype(g2_w.dtype)
        g1_w[:, js] = mm_r(ln2[...], gpre[:, js]).astype(g1_w.dtype)
        return 0

    lax.fori_loop(0, FF // 256, ff_grads, 0)
    gproj_w[...] = mm_r(mixed[...], gresb[...]).astype(gproj_w.dtype)

    qkv[...] = jnp.zeros_like(qkv)
    for i in range(images):
        fr = pl.ds(frame[i], length)
        mixw[...] = mm(sel[i], gmix[fr, :]).astype(bf16)

        def window(w, _):
            ws = pl.ds(pl.multiple_of(w * SEG, SEG), SEG)
            for g in range(NG):
                q = wq[i, ws, g * 128 : (g + 1) * 128]
                k = wq[i, ws, C + g * 128 : C + (g + 1) * 128]
                v = wq[i, ws, 2 * C + g * 128 : 2 * C + (g + 1) * 128]
                pt = probs[i, w * NG + g]
                dod = block_diag(mixw[ws, g * 128 : (g + 1) * 128], head_of_lane)
                gv = mm(pt, dod)
                dpt = mm_t(v, dod)
                ptf = pt.astype(f32)
                prod = ptf * dpt
                dst = prod - ptf * jnp.sum(prod, axis=0, keepdims=True)
                acc[g] += dst
                dsb = dst.astype(bf16)
                gk = mm(dsb, block_diag(q, head_of_lane))
                gq = diag_pick(mm_r(dsb, k), head_of_lane) * HD ** (-0.5)
                gl = slice(g * 128, (g + 1) * 128)
                gvec[2:3, gl] += jnp.sum(gq, axis=0, keepdims=True)
                gvec[3:4, gl] += jnp.sum(gv, axis=0, keepdims=True)
                gwin[ws, g * 128 : (g + 1) * 128] = gq.astype(bf16)
                gwin[ws, C + g * 128 : C + (g + 1) * 128] = gk.astype(bf16)
                gwin[ws, 2 * C + g * 128 : 2 * C + (g + 1) * 128] = gv.astype(bf16)
            return 0

        lax.fori_loop(0, NW, window, 0)
        qkv[fr, :] = (qkv[fr, :].astype(f32) + mm_r(sel[i], gwin[...])).astype(bf16)

    def last(t, _):
        sl = pl.ds(pl.multiple_of(t * block, 16), block)
        gln = mm(qkv[sl, :], wqkv[...])
        xin = x[sl, :].astype(f32)
        center, scale = norm_stats(xin)
        unit = (xin - center) * scale
        gvec[0:1, :] += jnp.sum(gln * unit, axis=0, keepdims=True)
        gvec[1:2, :] += jnp.sum(gln, axis=0, keepdims=True)
        gin[sl, :] = (gres[sl, :] + norm_back(gln * vec(0), unit, scale)).astype(bf16)
        return 0

    lax.fori_loop(0, blocks, last, 0)

    def qkv_grads(j, _):
        js = pl.ds(pl.multiple_of(j * 256, 256), 256)
        gqkv_w[js, :] = mm_r(qkv[:, js], ln1[...]).astype(gqkv_w.dtype)
        return 0

    lax.fori_loop(0, 3 * C // 256, qkv_grads, 0)


def block_size(rows):
    for cand in (112, 80, 64, 48, 32, 16):
        if rows % cand == 0:
            return cand
    return rows


def block_compute(x, cot, nlive, wqkv, wproj, w1, w2, vecs, b1, bias, interpret=False):
    tokens = x.shape[0]
    images = tokens // PIX
    rows = -(-tokens // 16) * 16
    if rows != tokens:
        x = jnp.pad(x, ((0, rows - tokens), (0, 0)))
        cot = jnp.pad(cot, ((0, rows - tokens), (0, 0)))
    block = block_size(rows)
    starts, _, length = image_frames(images)
    assert starts[-1] + length <= rows
    sel = jnp.asarray(placement(images), bf16)
    vmem = pl.BlockSpec(memory_space=pltpu.VMEM)
    smem = pl.BlockSpec(memory_space=pltpu.SMEM)
    s = jax.ShapeDtypeStruct
    outs = pl.pallas_call(
        functools.partial(compute_kernel, images, rows, block, length),
        out_shape=(
            s((rows, C), bf16),
            s((rows, C), bf16),
            s((3 * C, C), bf16),
            s((C, C), bf16),
            s((C, FF), bf16),
            s((C, FF), bf16),
            s((8, C), f32),
            s((1, FF), f32),
            s((NG, SEG, GH * SEG), f32),
        ),
        in_specs=[smem] + [vmem] * 10,
        out_specs=(vmem,) * 9,
        scratch_shapes=[
            pltpu.VMEM((rows, C), bf16),
            pltpu.VMEM((rows, 3 * C), bf16),
            pltpu.VMEM((images, NW * SEG, 3 * C), bf16),
            pltpu.VMEM((images, NW * NG, SEG, GH * SEG), bf16),
            pltpu.VMEM((NW * SEG, C), bf16),
            pltpu.VMEM((rows, C), bf16),
            pltpu.VMEM((rows, C), bf16),
            pltpu.VMEM((rows, FF), bf16),
            pltpu.VMEM((rows, FF), bf16),
            pltpu.VMEM((rows, C), bf16),
            pltpu.VMEM((rows, C), f32),
            pltpu.VMEM((rows, C), bf16),
            pltpu.VMEM((NW * SEG, 3 * C), bf16),
        ],
        compiler_params=pltpu.CompilerParams(vmem_limit_bytes=60 * 1024 * 1024),
        interpret=interpret,
    )(nlive, x, cot, wqkv, wproj, w1, w2, vecs, b1, bias, sel)
    return (outs[0][:tokens], outs[1][:tokens]) + outs[2:]

LINES = 4
MPS = 8
DPS = 4
QROWS = 384
QUART = QROWS * 256
FLAT = 776
MESH = pl.DeviceIdType.MESH


def base_of(p):
    return (p // WIN) * SPAN + p % WIN


def iota(shape, dim):
    return lax.broadcasted_iota(jnp.int32, shape, dim)


def as_bf(mask):
    return jnp.where(mask, 1.0, 0.0).astype(bf16)


def spread_queries():
    row = iota((GH * 256, GH * SEG), 0)
    lane = iota((GH * 256, GH * SEG), 1)
    q = lane % SEG
    return as_bf((row // 256 == lane // SEG) & (row % 256 == base_of(q)) & (q < WIN * WIN))


def key_rows(reverse):
    k = iota((SEG, 8 * WIN), 0)
    row = iota((SEG, 8 * WIN), 1)
    b = WIN - 1 - k % WIN if reverse else k % WIN
    return as_bf((row == (k // WIN) * 8 + b) & (k < WIN * WIN))


def table_lanes():
    row = iota((384, 512), 0)
    lane = iota((384, 512), 1)
    return as_bf((row == 2 * (lane % 256) + lane // 256) & (lane % 256 < SPAN * SPAN))


def split_mm(op, exact, value):
    hi = value.astype(bf16)
    lo = (value - hi.astype(f32)).astype(bf16)
    return op(exact, hi) + op(exact, lo)


def split_mm_left(op, value, exact):
    hi = value.astype(bf16)
    lo = (value - hi.astype(f32)).astype(bf16)
    return op(hi, exact) + op(lo, exact)


def turn_rows(part):
    return pltpu.roll(part, 0, 1, stride=1, stride_axis=0)


def gather_smalls(sm, vecs, b1, tabs, bias, mask):
    lane = iota((16, 128), 1)
    low = lane < 64
    for g in range(4):
        first, second = sm[2 * g].astype(f32), sm[2 * g + 1].astype(f32)
        turned = [pltpu.roll(first, 64, 1), pltpu.roll(second, 64, 1)]
        los = jnp.where(low, first, turned[1])
        his = jnp.where(low, turned[0], second)
        gl = slice(g * 128, (g + 1) * 128)
        for i, src, row in (
            (0, los, 0), (1, his, 0), (2, los, 1), (3, his, 1), (4, los, 2), (5, his, 2), (6, los, 3), (7, his, 5),
        ):
            vecs[i : i + 1, gl] = src[row : row + 1]
        for k in range(2):
            r = 2 * g + k
            full = (first, second)[k]
            rot = turned[k]
            b1[:, r * 256 : r * 256 + 128] = jnp.where(low[:1], rot[3:4], rot[4:5])
            b1[:, r * 256 + 128 : r * 256 + 256] = jnp.where(low[:1], rot[4:5], rot[5:6])
            for j in range(3):
                tabs[r : r + 1, j * 128 : (j + 1) * 128] = full[6 + j : 7 + j]
    tab = mm(tabs[...].astype(bf16), table_lanes())
    spread = spread_queries()
    keys = key_rows(False)
    for g in range(NG):
        parts = []
        for h in range(GH):
            r, i = divmod(g * GH + h, 2)
            t = jnp.broadcast_to(tab[r : r + 1, i * 256 : (i + 1) * 256], (8, 256))
            rows = [
                turn_rows(pltpu.roll(t, (SPAN * a - 84) % 256, 1)) for a in range(WIN)
            ]
            parts.append(jnp.concatenate(rows, axis=0))
        line = jnp.concatenate(parts, axis=1).astype(bf16)
        placed = mm(line, spread).astype(bf16)
        bt = mm(keys, placed)
        for w in range(NW):
            bias[w * NG + g] = bt + mask[w]


def row_half(gvec, i, r):
    g, k = divmod(r, 2)
    v = gvec[i : i + 1, g * 128 : (g + 1) * 128]
    turned = pltpu.roll(v, 64, 1)
    return (v, turned) if k == 0 else (turned, v)


def scatter_first(gvec, gsm):
    low = iota((1, 128), 1) < 64
    for r in range(MPS):
        gsm[r, 0:1, :] = jnp.where(low, row_half(gvec, 0, r)[0], row_half(gvec, 1, r)[1])


def scatter_smalls(gvec, gb1, acc, gsm, tabs):
    lane = iota((1, 128), 1)
    low = lane < 64
    spread = spread_queries()
    keys = key_rows(True)
    tabs[...] = jnp.zeros_like(tabs)
    for g in range(NG):
        z = split_mm(mm_r, keys, acc[g])
        y = split_mm_left(mm_t, z, spread)
        for h in range(GH):
            r, i = divmod(g * GH + h, 2)
            total = jnp.zeros((8, 256), f32)
            for a in range(WIN):
                part = y[8 * a : 8 * a + 8, h * 256 : (h + 1) * 256]
                total = total + turn_rows(pltpu.roll(part, (78 - SPAN * a) % 256, 1))
            tabs[r : r + 1, i * 256 : (i + 1) * 256] = jnp.sum(total, axis=0, keepdims=True)
    flat = split_mm_left(mm_t, tabs[...], table_lanes())

    half = functools.partial(row_half, gvec)
    zero = jnp.zeros((1, 128), f32)
    for r in range(MPS):
        fb0 = gb1[:, r * 256 : r * 256 + 128]
        fb1 = gb1[:, r * 256 + 128 : r * 256 + 256]
        t0, t1 = pltpu.roll(fb0, 64, 1), pltpu.roll(fb1, 64, 1)
        rows = [
            jnp.where(low, half(2, r)[0], half(3, r)[1]),
            jnp.where(low, half(4, r)[0], half(5, r)[1]),
            jnp.where(low, half(6, r)[0], t0),
            jnp.where(low, t0, t1),
            jnp.where(low, t1, half(7, r)[1]),
        ]
        for j, row in enumerate(rows):
            gsm[r, 1 + j : 2 + j, :] = row
        for j in range(3):
            gsm[r, 6 + j : 7 + j, :] = flat[r : r + 1, j * 128 : (j + 1) * 128]
        for j in range(9, 16):
            gsm[r, j : j + 1, :] = zero


def slot(m, d):
    return m * DPS + d


def w_qkv(wb, kind, quad, half):
    return jnp.concatenate(
        [wb[slot(4 * quad + r, 0), half * 192 + kind * 64 : half * 192 + kind * 64 + 64, :] for r in range(4)], axis=0
    )


def w_proj(wb, quad, half):
    return jnp.concatenate([wb[slot(4 * quad + r, 1), half * 64 : half * 64 + 64, :] for r in range(4)], axis=0)


def w_one(wb, r, half):
    return wb[slot(r, 1), 128:384, :] if half == 0 else wb[slot(r, 2), 0:256, :]


def w_two(wb, r, half):
    return jnp.concatenate(
        [
            wb[slot(r, 2), 256 + half * 64 : 256 + half * 64 + 64, :],
            wb[slot(r, 3), half * 192 : half * 192 + 192, :],
        ],
        axis=0,
    )


HALVES = (slice(0, 256), slice(256, 512))


def first_norm(x, vecs, ln1):
    xin = x[...].astype(f32)
    center, scale = norm_stats(xin)
    ln1[...] = ((xin - center) * scale * vecs[0:1, :] + vecs[1:2, :]).astype(bf16)


def group_lanes(g):
    return pl.ds(pl.multiple_of(g * 128, 128), 128)


def group_qkv(wb, g, half):
    return jnp.concatenate(
        [
            wb[slot(2 * g + r, 0), half * 192 + kind * 64 : half * 192 + kind * 64 + 64, :]
            for kind in range(3)
            for r in range(2)
        ],
        axis=0,
    )


def project_group(g, wb, vecs, ln1, qkv):
    val = mm_t(ln1[:, HALVES[0]], group_qkv(wb, g, 0)) + mm_t(ln1[:, HALVES[1]], group_qkv(wb, g, 1))
    gl = group_lanes(g)
    qkv[:, 0:128] = ((val[:, 0:128] + vecs[2:3, gl]) * HD ** (-0.5)).astype(bf16)
    qkv[:, 128:256] = val[:, 128:256].astype(bf16)
    qkv[:, 256:384] = (val[:, 256:384] + vecs[3:4, gl]).astype(bf16)


def frame_rows(i, length):
    return pl.ds(pl.multiple_of(PIX * i // 16 * 16, 16), length)


def attend(i, g, length, sel, bias, qkv, wq, probs, mixed):
    head_of_lane = lane_head_mask()
    fr = frame_rows(i, length)
    wq[g, i] = mm(sel[i], qkv[fr, :]).astype(bf16)
    outs = []
    for w in range(NW):
        ws = slice(w * SEG, (w + 1) * SEG)
        q, k, v = (wq[g, i, ws, n * 128 : (n + 1) * 128] for n in range(3))
        st = mm_t(k, block_diag(q, head_of_lane)) + bias[w * NG + g]
        e = jnp.exp(st - jnp.max(st, axis=0, keepdims=True))
        pt = (e * (1.0 / jnp.sum(e, axis=0, keepdims=True))).astype(bf16)
        probs[g, i, w] = pt
        outs.append(diag_pick(mm_r(pt, v), head_of_lane).astype(bf16))
    gl = group_lanes(g)
    back = mm_r(sel[i], jnp.concatenate(outs, axis=0))
    mixed[fr, gl] = (mixed[fr, gl].astype(f32) + back).astype(bf16)


def attend_back(i, g, length, sel, gmix, wq, probs, gqkv, acc, gvec):
    head_of_lane = lane_head_mask()
    fr = frame_rows(i, length)
    gl = group_lanes(g)
    gwin = mm(sel[i], gmix[fr, gl]).astype(bf16)
    outs = []
    for w in range(NW):
        ws = slice(w * SEG, (w + 1) * SEG)
        q, k, v = (wq[g, i, ws, n * 128 : (n + 1) * 128] for n in range(3))
        pt = probs[g, i, w]
        dod = block_diag(gwin[ws, :], head_of_lane)
        gv = mm(pt, dod)
        dpt = mm_t(v, dod)
        ptf = pt.astype(f32)
        prod = ptf * dpt
        dst = prod - ptf * jnp.sum(prod, axis=0, keepdims=True)
        acc[g] += dst
        dsb = dst.astype(bf16)
        gk = mm(dsb, block_diag(q, head_of_lane))
        gq = diag_pick(mm_r(dsb, k), head_of_lane) * HD ** (-0.5)
        gvec[2:3, gl] += jnp.sum(gq, axis=0, keepdims=True)
        gvec[3:4, gl] += jnp.sum(gv, axis=0, keepdims=True)
        outs.append(jnp.concatenate([gq.astype(bf16), gk.astype(bf16), gv.astype(bf16)], axis=1))
    back = mm_r(sel[i], jnp.concatenate(outs, axis=0))
    gqkv[fr, :] = (gqkv[fr, :].astype(f32) + back).astype(bf16)


def group_grads(g, gb, gqkv, ln1):
    part = mm_r(gqkv[...], ln1[...]).astype(bf16)
    for kind in range(3):
        for r in range(2):
            at = kind * 128 + r * 64
            for h in range(2):
                to = h * 192 + kind * 64
                gb[slot(2 * g + r, 0), to : to + 64, :] = part[at : at + 64, HALVES[h]]


def group_norm_grad(g, wb, gqkv, gl1):
    for h in range(2):
        gl1[:, HALVES[h]] += mm(gqkv[...], group_qkv(wb, g, h))


def feed_forward(rows, live_rows, x, cot, wb, vecs, b1, out, gvec, gb1, mixed, ln2, act, gpre, gresb, gres, gmix, goutb):
    def vec(i):
        return vecs[i : i + 1, :]

    att = [mm(mixed[:, HALVES[0]], w_proj(wb, 0, h)) + mm(mixed[:, HALVES[1]], w_proj(wb, 1, h)) for h in range(2)]
    res = x[...].astype(f32) + (jnp.concatenate(att, axis=1) + vec(4))
    center, scale = norm_stats(res)
    unit = (res - center) * scale
    ln2[...] = (unit * vec(5) + vec(6)).astype(bf16)
    live = (iota((rows, 1), 0) < live_rows).astype(f32)
    gout = live * cot[...].astype(f32)
    goutb[...] = gout.astype(bf16)
    feed = [jnp.zeros((rows, 256), f32)] * 2
    gln = [jnp.zeros((rows, 256), f32)] * 2
    for r in range(MPS):
        js = slice(r * 256, (r + 1) * 256)
        pre = mm(ln2[:, HALVES[0]], w_one(wb, r, 0)) + mm(ln2[:, HALVES[1]], w_one(wb, r, 1)) + b1[:, js]
        phi, e = phi_parts(pre)
        av = (pre * phi).astype(bf16)
        act[:, js] = av
        feed = [feed[h] + mm(av, w_two(wb, r, h)) for h in range(2)]
        ga = mm_t(goutb[:, HALVES[0]], w_two(wb, r, 0)) + mm_t(goutb[:, HALVES[1]], w_two(wb, r, 1))
        gp = ga * (phi + pre * (e * (1.0 / math.sqrt(2.0 * math.pi))))
        gb1[:, js] = jnp.sum(gp, axis=0, keepdims=True)
        gpb = gp.astype(bf16)
        gpre[:, js] = gpb
        gln = [gln[h] + mm_t(gpb, w_one(wb, r, h)) for h in range(2)]
    feed = jnp.concatenate(feed, axis=1)
    gln = jnp.concatenate(gln, axis=1)
    out[...] = (live * (res + feed + vec(7))).astype(bf16)
    gr = gout + norm_back(gln * vec(5), unit, scale)
    gres[...] = gr
    grb = gr.astype(bf16)
    gresb[...] = grb
    for quad in range(2):
        gmix[:, HALVES[quad]] = (
            mm_t(grb[:, HALVES[0]], w_proj(wb, quad, 0)) + mm_t(grb[:, HALVES[1]], w_proj(wb, quad, 1))
        ).astype(bf16)
    gvec[4:5, :] = jnp.sum(gr, axis=0, keepdims=True)
    gvec[5:6, :] = jnp.sum(gln * unit, axis=0, keepdims=True)
    gvec[6:7, :] = jnp.sum(gln, axis=0, keepdims=True)
    gvec[7:8, :] = jnp.sum(gout, axis=0, keepdims=True)


def proj_grads(gb, mixed, gresb):
    gproj = mm_r(mixed[...], gresb[...]).astype(bf16)
    for r in range(MPS):
        for h in range(2):
            gb[slot(r, 1), h * 64 : h * 64 + 64, :] = gproj[r * 64 : r * 64 + 64, HALVES[h]]


def feed_forward_grads(r, gb, act, goutb, ln2, gpre):
    js = pl.ds(pl.multiple_of(r * 256, 256), 256)
    two = mm_r(act[:, js], goutb[...]).astype(bf16)
    for h in range(2):
        gb[slot(r, 2), 256 + h * 64 : 256 + h * 64 + 64, :] = two[0:64, HALVES[h]]
        gb[slot(r, 3), h * 192 : h * 192 + 192, :] = two[64:256, HALVES[h]]
    one = mm_r(ln2[...], gpre[:, js]).astype(bf16)
    gb[slot(r, 1), 128:384, :] = one[0:256]
    gb[slot(r, 2), 0:256, :] = one[256:512]


def first_norm_sums(x, gl1, gvec):
    xin = x[...].astype(f32)
    center, scale = norm_stats(xin)
    unit = (xin - center) * scale
    gln = gl1[...]
    gvec[0:1, :] = jnp.sum(gln * unit, axis=0, keepdims=True)
    gvec[1:2, :] = jnp.sum(gln, axis=0, keepdims=True)


def first_norm_back(x, vecs, gl1, gres, gin):
    xin = x[...].astype(f32)
    center, scale = norm_stats(xin)
    unit = (xin - center) * scale
    gin[...] = (gres[...] + norm_back(gl1[...] * vecs[0:1, :], unit, scale)).astype(bf16)


def mega_scratch(images, rows):
    return [
        pltpu.VMEM((rows, C), bf16),
        pltpu.VMEM((rows, 384), bf16),
        pltpu.VMEM((NG, images, NW * SEG, 384), bf16),
        pltpu.VMEM((NG, images, NW, SEG, GH * SEG), bf16),
        pltpu.VMEM((rows, C), bf16),
        pltpu.VMEM((rows, C), bf16),
        pltpu.VMEM((rows, FF), bf16),
        pltpu.VMEM((rows, FF), bf16),
        pltpu.VMEM((rows, C), bf16),
        pltpu.VMEM((rows, C), f32),
        pltpu.VMEM((rows, C), bf16),
        pltpu.VMEM((rows, C), f32),
        pltpu.VMEM((rows, C), bf16),
    ]


def score_masks():
    _, ids = window_sites()
    size = WIN * WIN
    full = np.zeros((NW, SEG, SEG), np.float32)
    full[:, size:, :] = -1e30
    full[:, :size, :size] = np.where(ids[:, :, None] == ids[:, None, :], 0.0, mask_fill)
    return np.tile(full, (1, 1, GH))


def place():
    d, m = lax.axis_index("dp"), lax.axis_index("mp")
    return d, m, d // 2, d % 2, m // 2, m % 2


def twin(a, j):
    return 2 * ((a // 2 + j // 2) % 2) + (a + j) % 2


def remote(src, dst, send, recv, dev):
    return pltpu.make_async_remote_copy(
        src_ref=src, dst_ref=dst, send_sem=send, recv_sem=recv, device_id=dev, device_id_type=MESH
    )


def peers():
    d, m, *_ = place()
    return [{"dp": (d + k) % DPS, "mp": m} for k in range(1, DPS)] + [
        {"dp": d, "mp": (m + k) % MPS} for k in range(1, MPS)
    ]


def greet():
    barrier = pltpu.get_barrier_semaphore()
    for dev in peers():
        pl.semaphore_signal(barrier, inc=1, device_id=dev, device_id_type=MESH)


def greeted():
    pl.semaphore_wait(pltpu.get_barrier_semaphore(), DPS - 1 + MPS - 1)


OFFSET = 277


def flatten_params(pf, fl, roll, head, head_sem, wide, wb, sm):
    d, m, *_ = place()
    lane = iota((FLAT, 128), 1)
    roll[0:8, :] = jnp.zeros((8, 128), f32)
    fl[FLAT : FLAT + 16, :] = jnp.zeros((16, 128), f32)
    for k in range(DPS):

        @pl.when(d == k)
        def _(k=k):
            lanes, down = OFFSET * k % 128, OFFSET * k // 128
            if k == 0:
                fl[0:FLAT, :] = pf[...]
            else:
                roll[8 : 8 + FLAT, :] = pltpu.roll(pf[...], lanes, 1)
                fl[down : down + FLAT, :] = jnp.where(
                    lane >= lanes, roll[8 : 8 + FLAT, :], roll[7 : 7 + FLAT, :]
                )

    greeted()
    over = remote(fl.at[768:784], head.at[0], head_sem.at[0], head_sem.at[1], {"dp": (d + 1) % DPS, "mp": m})

    @pl.when(d < DPS - 1)
    def _():
        over.start()

    @pl.when(d > 0)
    def _():
        over.wait_recv()
        pos = iota((8, 128), 0) * 128 + iota((8, 128), 1)
        fl[0:8, :] = jnp.where(pos < OFFSET * d, head[0, 0:8, :], fl[0:8, :])

    def cut(start, size, step):
        return fl[pl.ds(start, size, stride=step), :]

    @pl.when(d == 0)
    def _():
        low = iota((256, 128), 1) < 64
        one, two = pltpu.roll(cut(1, 256, 3), 64, 1), pltpu.roll(cut(2, 256, 3), 64, 1)
        wide[pl.ds(0, 256, stride=2), :] = cut(0, 256, 3)
        wide[pl.ds(C, 256, stride=2), :] = cut(1, 256, 3)
        wide[pl.ds(1, 256, stride=2), :] = jnp.where(low, one, two)
        wide[pl.ds(C + 1, 256, stride=2), :] = two
        turned = jnp.concatenate([wide[0:C, :].T, wide[C : 2 * C, :].T], axis=0).astype(bf16)
        s = slot(m, 0)
        for half in range(2):
            for kind in range(3):
                for i in range(2):
                    to = half * 192 + kind * 64 + i * 32
                    frm = i * 96 + kind * 32
                    wb[s, to : to + 32, :] = turned[frm : frm + 32, HALVES[half]]

    @pl.when(d == 1)
    def _():
        s = slot(m, 1)
        for j in range(2):
            js = slice(j * 128, (j + 1) * 128)
            for half in range(2):
                wb[s, half * 64 : half * 64 + 64, js] = cut(2 * half + j, 64, 4).astype(bf16)
            wb[s, 128:384, js] = cut(256 + j, 256, 2).astype(bf16)

    @pl.when(d == 2)
    def _():
        s = slot(m, 2)
        for j in range(2):
            js = slice(j * 128, (j + 1) * 128)
            wb[s, 0:256, js] = cut(j, 256, 2).astype(bf16)
            for half in range(2):
                at = 256 + half * 64
                wb[s, at : at + 64, js] = cut(512 + 2 * half + j, 64, 4).astype(bf16)

    @pl.when(d == 3)
    def _():
        s = slot(m, 3)
        for j in range(2):
            js = slice(j * 128, (j + 1) * 128)
            for half in range(2):
                wb[s, half * 192 : half * 192 + 192, js] = cut(2 * half + j, 192, 4).astype(bf16)
        sm[m] = fl[768:784, :].astype(bf16)

    @pl.when(d < DPS - 1)
    def _():
        over.wait_send()


def smalls_out(sm, ssem, rsem):
    d, m, *_ = place()

    def over_dp(k):
        return remote(sm.at[m], sm.at[m], ssem.at[k], rsem.at[m], {"dp": k, "mp": m})

    def over_mp(k):
        return remote(sm.at[m], sm.at[m], ssem.at[3 + k], rsem.at[m], {"dp": d, "mp": (m + k) % MPS})

    @pl.when(d == DPS - 1)
    def _():
        for k in range(DPS - 1):
            over_dp(k).start()

    @pl.when(d < DPS - 1)
    def _():
        over_dp(0).wait_recv()

    for k in range(1, MPS):
        over_mp(k).start()

    def finish():
        for k in range(1, MPS):
            src = (m + k) % MPS
            remote(sm.at[src], sm.at[src], ssem.at[0], rsem.at[src], {"dp": d, "mp": src}).wait_recv()

    def drain():
        @pl.when(d == DPS - 1)
        def _():
            for k in range(DPS - 1):
                over_dp(k).wait_send()

        for k in range(1, MPS):
            over_mp(k).wait_send()

    return finish, drain


SIDE_Z, SIDE_Y, SIDE_X, CORE = 0, 3, 4, 5


class BlocksOut:
    def __init__(self, wb, ssem, rsem):
        self.wb, self.ssem, self.rsem = wb, ssem, rsem
        self.d, self.m, self.x, self.c, self.a, self.b = place()
        d, m, b, c = self.d, self.m, self.b, self.c
        self.far = (d + 2) % DPS
        self.dev = {
            SIDE_Y: {"dp": d, "mp": m + 1 - 2 * b},
            SIDE_X: {"dp": self.far, "mp": m},
            CORE: {"dp": d + 1 - 2 * c, "mp": m},
        }
        for j in range(1, LINES):
            self.dev[SIDE_Z + j - 1] = {"dp": d, "mp": 2 * twin(self.a, j) + b}

    def copy(self, s, way):
        return remote(self.wb.at[s], self.wb.at[s], self.ssem.at[s, way], self.rsem.at[s], self.dev[way])

    def arrive(self, s):
        self.copy(s, CORE).wait_recv()

    def row(self, j, same):
        return 2 * twin(self.a, j) + (self.b if same else 1 - self.b)

    def own_ways(self, core):
        return [SIDE_Z, SIDE_Z + 1, SIDE_Z + 2, SIDE_Y] + ([SIDE_X] if core else []) + [CORE]

    def start(self, s, ways):
        for way in ways:
            self.copy(s, way).start()

    def settle(self, s, ways):
        for way in ways:
            self.copy(s, way).wait_send()

    def origin_out(self, dd):
        @pl.when(self.d == dd)
        def _():
            self.start(slot(self.m, dd), [SIDE_X] + self.own_ways(0))

    def origin_in(self, dd):
        @pl.when(self.d != dd)
        def _():
            s = slot(self.m, dd)
            self.arrive(s)
            self.start(s, self.own_ways(0))

    def own(self):
        self.start(slot(self.m, self.d), self.own_ways(1))

    def line_ways(self, core):
        return [SIDE_Y] + ([SIDE_X] if core else []) + [CORE]

    def side_ways(self, core):
        return ([SIDE_X] if core else []) + [CORE]

    def line(self, core, dd, j):
        s = slot(self.row(j, True), dd)
        self.arrive(s)
        self.start(s, self.line_ways(core))

    def side(self, core, dd, j):
        s = slot(self.row(j, False), dd)
        self.arrive(s)
        self.start(s, self.side_ways(core))

    def cross(self, j, same):
        s = slot(self.row(j, same), self.far)
        self.arrive(s)
        self.start(s, [CORE])

    def from_core(self, dd):
        for row in range(MPS):
            self.arrive(slot(row, dd))

    def group_from_core(self, dd, j):
        self.arrive(slot(self.row(j, True), dd))
        self.arrive(slot(self.row(j, False), dd))

    def drain(self):
        @pl.when(self.c == 0)
        def _():
            for dd in (0, 2):
                pl.when(self.d == dd)(lambda: self.copy(slot(self.m, dd), SIDE_X).wait_send())
                self.settle(slot(self.m, dd), self.own_ways(0))
                for j in range(LINES):
                    if j:
                        self.settle(slot(self.row(j, True), dd), self.line_ways(0))
                    self.settle(slot(self.row(j, False), dd), self.side_ways(0))

        @pl.when(self.c == 1)
        def _():
            self.settle(slot(self.m, self.d), self.own_ways(1))
            for j in range(LINES):
                if j:
                    self.settle(slot(self.row(j, True), self.d), self.line_ways(1))
                self.settle(slot(self.row(j, False), self.d), self.side_ways(1))
                for same in (True, False):
                    self.settle(slot(self.row(j, same), self.far), [CORE])


class BlocksIn:
    def __init__(self, gb, rc, rx, ry, rz, total, spare, sems):
        self.gb, self.rc, self.rx, self.ry, self.rz = gb, rc, rx, ry, rz
        self.total, self.spare = total, spare
        self.sems = sems
        self.d, self.m, self.x, self.c, self.a, self.b = place()
        d, m, b, c = self.d, self.m, self.b, self.c
        self.far = (d + 2) % DPS
        self.twin = d + 1 - 2 * c
        self.to_core = {"dp": self.twin, "mp": m}
        self.to_x = {"dp": self.far, "mp": m}
        self.to_y = {"dp": d, "mp": m + 1 - 2 * b}

    def move(self, s, dst, name, k, part, dev):
        ss, rs = self.sems[name]
        rows = pl.ds(*part[1:])
        return remote(self.gb.at[s, rows], dst.at[rows], ss.at[k, part[0]], rs.at[k, part[0]], dev)

    def by_core(self, row, dd, part):
        k = dd // 2 * MPS + row
        return self.move(slot(row, dd), self.rc.at[k], "core", k, part, self.to_core)

    def by_x(self, k, s, part):
        return self.move(s, self.rx.at[k], "x", k, part, self.to_x)

    def by_y(self, k, t, dd, part):
        return self.move(slot(2 * t + 1 - self.b, dd), self.ry.at[k * LINES + t], "y", k * LINES + t, part, self.to_y)

    def by_z(self, k, t, dd, part):
        ss, rs = self.sems["z"]
        rows = pl.ds(*part[1:])
        n = k * LINES + self.a
        return remote(
            self.gb.at[slot(2 * t + self.b, dd), rows],
            self.rz.at[n].at[rows],
            ss.at[k * LINES + t, part[0]],
            rs.at[n, part[0]],
            {"dp": self.d, "mp": 2 * t + self.b},
        )

    def from_z(self, k, t, part):
        _, rs = self.sems["z"]
        ref = self.rz.at[k * LINES + t].at[pl.ds(*part[1:])]
        remote(ref, ref, rs.at[k * LINES + t, part[0]], rs.at[k * LINES + t, part[0]], self.to_y).wait_recv()

    def add(self, s, part, *got):
        rows = pl.ds(*part[1:])
        value = self.gb[s, rows].astype(f32)
        for ref in got:
            value = value + ref[rows].astype(f32)
        self.gb[s, rows] = value.astype(bf16)

    def along_z(self, k, t, dd, part):
        pl.when(t != self.a)(lambda: self.by_z(k, t, dd, part).start())

    def line_here(self, k):
        for j in range(1, LINES):
            self.from_z(k, twin(self.a, j), WHOLE[0])

    def end_z(self, k, dd, part, to):
        rows = pl.ds(*part[1:])
        value = self.gb[slot(self.m, dd), rows].astype(f32)
        for j in range(1, LINES):
            value = value + self.rz[k * LINES + twin(self.a, j), rows].astype(f32)
        to[rows, :] = value

    def zero_over(self, dd, t, part):
        row = 2 * t + 1 - self.b
        self.by_core(row, dd, part).wait_recv()
        self.add(slot(row, dd), part, self.rc.at[dd // 2 * MPS + row])
        self.by_y(dd // 2, t, dd, part).start()

    def zero_own(self, dd, t, part):
        row = 2 * t + self.b
        k = dd // 2
        self.by_core(row, dd, part).wait_recv()
        self.by_y(k, t, dd, part).wait_recv()
        self.add(slot(row, dd), part, self.rc.at[k * MPS + row], self.ry.at[k * LINES + t])
        self.along_z(k, t, dd, part)

    def zero_end(self, dd, part):
        k = dd // 2
        s = slot(self.m, dd)
        rows = pl.ds(*part[1:])
        self.end_z(k, dd, part, self.spare)

        @pl.when(self.d != dd)
        def _():
            self.gb[s, rows] = self.spare[rows, :].astype(bf16)
            self.by_x(k, s, part).start()

        @pl.when(self.d == dd)
        def _():
            self.by_x(k, s, part).wait_recv()
            self.total[rows, :] = self.spare[rows, :] + self.rx[k, rows].astype(f32)

    def one_end(self, part):
        self.line_here(0)
        self.end_z(0, self.d, part, self.total)

    def turn(self, n):
        return twin(self.a, LINES - 1 - n % LINES)

    def row_turn(self, n):
        return 2 * self.turn(n) + self.b + (1 - 2 * self.b) * (1 - n // LINES)

    def one_far(self, n, part):
        row = self.row_turn(n)
        dd = self.far
        self.by_core(row, dd, part).wait_recv()
        self.add(slot(row, dd), part, self.rc.at[dd // 2 * MPS + row])
        self.by_x(row, slot(row, dd), part).start()

    def one_over(self, t, part):
        row = 2 * t + 1 - self.b
        dd = self.d
        self.by_core(row, dd, part).wait_recv()
        self.by_x(row, slot(row, dd), part).wait_recv()
        self.add(slot(row, dd), part, self.rc.at[dd // 2 * MPS + row], self.rx.at[row])
        self.by_y(0, t, dd, part).start()

    def one_own(self, t, part):
        row = 2 * t + self.b
        dd = self.d
        self.by_core(row, dd, part).wait_recv()
        self.by_x(row, slot(row, dd), part).wait_recv()
        self.by_y(0, t, dd, part).wait_recv()
        self.add(slot(row, dd), part, self.rc.at[dd // 2 * MPS + row], self.rx.at[row], self.ry.at[t])
        self.along_z(0, t, dd, part)

    def drain_tree(self, core, dd, part):
        k = dd // 2 if core == 0 else 0
        for n in range(LINES):
            self.drain_place(k, self.turn(n), dd, part)
        if core == 0:
            self.drain_end(dd, part)
        else:
            for row in range(MPS):
                self.by_x(row, slot(row, self.far), part).wait_send()

    def drain_place(self, k, t, dd, part):
        self.by_y(k, t, dd, part).wait_send()
        pl.when(t != self.a)(lambda: self.by_z(k, t, dd, part).wait_send())

    def drain_end(self, dd, part):
        pl.when(self.d != dd)(lambda: self.by_x(dd // 2, slot(self.m, dd), part).wait_send())


WHOLE = ((0, 0, QROWS),)
PARTS = ((0, 0, QROWS // 2), (1, QROWS // 2, QROWS // 2))


def smalls_in(gsm, got, part, got2, total, ssem, rsem, rsem2):
    d, m, *_ = place()

    def over_mp(k):
        dst = (m + k) % MPS
        return remote(gsm.at[dst], got.at[k], ssem.at[k], rsem.at[k], {"dp": d, "mp": dst})

    def over_dp(k):
        return remote(part, got2.at[k], ssem.at[0], rsem2.at[k], {"dp": DPS - 1, "mp": m})

    for k in range(1, MPS):
        over_mp(k).start()

    def middle():
        value = gsm[m]
        for k in range(1, MPS):
            over_mp(k).wait_recv()
            value = value + got[k]
        part[...] = value
        for k in range(DPS - 1):
            pl.when(d == k)(lambda k=k: over_dp(k).start())

    def end():
        @pl.when(d == DPS - 1)
        def _():
            total[...] = part[...]
            for k in range(DPS - 1):
                over_dp(k).wait_recv()
                total[...] += got2[k]

    def drain():
        for k in range(DPS - 1):
            pl.when(d == k)(lambda k=k: over_dp(k).wait_send())
        for k in range(1, MPS):
            over_mp(k).wait_send()

    return middle, end, drain


def flat_grads(total, smalls, fl, roll, head, head_sem, wide, tall, gflat):
    d, m, *_ = place()
    back = remote(fl.at[0:8], head.at[1, 0:8], head_sem.at[2], head_sem.at[3], {"dp": (d + DPS - 1) % DPS, "mp": m})

    def put(start, size, step, val):
        fl[pl.ds(start, size, stride=step), :] = val

    def rest():
        fl[768:792, :] = jnp.zeros((24, 128), f32)

        @pl.when(d == 1)
        def _():
            for j in range(2):
                js = slice(j * 128, (j + 1) * 128)
                for half in range(2):
                    put(2 * half + j, 64, 4, total[half * 64 : half * 64 + 64, js])
                put(256 + j, 256, 2, total[128:384, js])

        @pl.when(d == 2)
        def _():
            for j in range(2):
                js = slice(j * 128, (j + 1) * 128)
                put(j, 256, 2, total[0:256, js])
                for half in range(2):
                    at = 256 + half * 64
                    put(512 + 2 * half + j, 64, 4, total[at : at + 64, js])

        @pl.when(d == 3)
        def _():
            for j in range(2):
                js = slice(j * 128, (j + 1) * 128)
                for half in range(2):
                    put(2 * half + j, 192, 4, total[half * 192 : half * 192 + 192, js])

        pl.when(d > 0)(lambda: back.start())

    def first():
        @pl.when(d == 0)
        def _():
            tall[192:256, :] = jnp.zeros((64, C), f32)
            for half in range(2):
                for kind in range(3):
                    for i in range(2):
                        frm = half * 192 + kind * 64 + i * 32
                        to = i * 96 + kind * 32
                        tall[to : to + 32, HALVES[half]] = total[frm : frm + 32, :]
            wide[0:C, :] = tall[0:128, :].T
            wide[C : 2 * C, :] = tall[128:256, :].T
            low = iota((256, 128), 1) < 64

            def every(start):
                return wide[pl.ds(start, 256, stride=2), :]

            one, two = pltpu.roll(every(1), 64, 1), pltpu.roll(every(C + 1), 64, 1)
            put(0, 256, 3, every(0))
            put(1, 256, 3, jnp.where(low, every(C), one))
            put(2, 256, 3, jnp.where(low, one, two))

    def end():
        @pl.when(d == DPS - 1)
        def _():
            fl[768:784, :] = smalls[...]

        @pl.when(d < DPS - 1)
        def _():
            back.wait_recv()
            fl[768:776, :] = head[1, 0:8, :]

        lane = iota((FLAT, 128), 1)
        for k in range(DPS):

            @pl.when(d == k)
            def _(k=k):
                lanes, down = OFFSET * k % 128, OFFSET * k // 128
                if k == 0:
                    gflat[...] = fl[0:FLAT, :]
                else:
                    roll[0:784, :] = pltpu.roll(fl[0:784, :], 128 - lanes, 1)
                    roll[784:792, :] = jnp.zeros((8, 128), f32)
                    gflat[...] = jnp.where(lane < 128 - lanes, roll[down : down + FLAT, :], roll[down + 1 : down + 1 + FLAT, :])

    def drain():
        pl.when(d > 0)(lambda: back.wait_send())

    return rest, first, end, drain


def step_kernel(images, rows, length, *refs):
    (nlive, x, cot, pf, sel, mask) = refs[:6]
    (out, gin, gflat) = refs[6:9]
    (
        fl, roll, head, wide, tall, wb, sm, vecs, b1, tabs, tabs2, bias, gvec, gb1, acc, gb, gsm, got, part_sm, got2,
        stotal, rc, rx, ry, rz, total, spare,
        head_sem, sm_s, sm_r, ag_s, ag_r, rsm_s, rsm_r, rsm_r2, s_core, r_core, s_x, r_x, s_y, r_y, s_z, r_z,
    ) = refs[9:52]
    ln1, qkv, wq, probs, mixed, ln2, act, gpre, gresb, gres, gmix, gl1, goutb = refs[52:]
    greet()
    flatten_params(pf, fl, roll, head, head_sem, wide, wb, sm)
    outs = BlocksOut(wb, ag_s, ag_r)
    zero, one = outs.c == 0, outs.c == 1
    pl.when(zero)(lambda: outs.origin_out(0))
    finish_sm, drain_sm = smalls_out(sm, sm_s, sm_r)
    pl.when(zero)(lambda: outs.origin_in(0))
    finish_sm()
    gather_smalls(sm, vecs, b1, tabs, bias, mask)
    first_norm(x, vecs, ln1)

    def two(fn, *args):
        return functools.partial(fn, 0, 2, *args)

    def qk(fn, j):
        return functools.partial(fn, 0, 0, j)

    def mine(fn, *args):
        return functools.partial(fn, 1, outs.d, *args)

    def cross(j, same):
        return functools.partial(outs.cross, j, same)

    def run(fns):
        for fn in fns:
            fn()

    def at_point(zeros, ones, point):
        if point in zeros:
            pl.when(zero)(lambda: run(zeros[point]))
        if point in ones:
            pl.when(one)(lambda: run(ones[point]))

    def poll(zeros, ones, point, now):
        for k in sorted(set(zeros) | set(ones)):
            if 0 <= k < 4 * images:
                pl.when(now == k)(functools.partial(at_point, zeros, ones, k))

    zero_at = {
        0: [qk(outs.line, 1), qk(outs.side, 0)],
        1: [qk(outs.line, 2)],
        2: [qk(outs.line, 3), functools.partial(outs.origin_out, 2)],
        4: [qk(outs.side, 1)],
        7: [functools.partial(outs.origin_in, 2)],
        8: [qk(outs.side, 2)],
        10: [two(outs.line, 1)],
        11: [two(outs.side, 0)],
        12: [qk(outs.side, 3), two(outs.line, 2)],
        14: [two(outs.line, 3)],
        15: [two(outs.side, 1)],
        16: [two(outs.side, 2), two(outs.side, 3)],
    }
    one_at = {
        0: [functools.partial(outs.group_from_core, 0, 0)],
        1: [outs.own],
        4: [functools.partial(outs.group_from_core, 0, 1)],
        6: [mine(outs.line, 1)],
        7: [mine(outs.side, 0)],
        8: [functools.partial(outs.group_from_core, 0, 2), cross(0, True)],
        9: [mine(outs.line, 2)],
        10: [mine(outs.side, 1)],
        11: [mine(outs.line, 3)],
        12: [functools.partial(outs.group_from_core, 0, 3), cross(1, True), cross(0, False)],
        13: [mine(outs.side, 2)],
        14: [cross(1, False)],
        15: [mine(outs.side, 3), cross(2, True)],
        16: [cross(3, True), cross(2, False), cross(3, False)],
    }
    mixed[...] = jnp.zeros_like(mixed)

    def forward(n, _):
        j, i = n // images, n % images
        g = twin(outs.a, j)
        poll(zero_at, one_at, None, n)
        pl.when(i == 0)(lambda: project_group(g, wb, vecs, ln1, qkv))
        attend(i, g, length, sel, bias, qkv, wq, probs, mixed)
        return 0

    lax.fori_loop(0, NG * images, forward, 0)
    at_point(zero_at, one_at, 16)

    @pl.when(zero)
    def _():
        outs.from_core(1)
        outs.from_core(3)

    pl.when(one)(lambda: outs.from_core(2))

    feed_forward(
        rows, nlive[0], x, cot, wb, vecs, b1, out, gvec, gb1, mixed, ln2, act, gpre, gresb, gres, gmix, goutb
    )
    proj_grads(gb, mixed, gresb)
    ins = BlocksIn(
        gb, rc, rx, ry, rz, total, spare, {"core": (s_core, r_core), "x": (s_x, r_x), "y": (s_y, r_y), "z": (s_z, r_z)}
    )
    whole = WHOLE[0]

    def grads(n, _):
        row = ins.row_turn(n)
        feed_forward_grads(row, gb, act, goutb, ln2, gpre)

        @pl.when(zero)
        def _():
            for dd in (1, 3):
                ins.by_core(row, dd, whole).start()

        pl.when(one)(lambda: ins.by_core(row, 2, whole).start())
        pl.when((n >= 1) & one)(lambda: ins.one_far(n - 1, whole))
        pl.when((n >= 1) & (n <= LINES) & zero)(lambda: ins.zero_over(2, ins.turn(n - 1), whole))
        return 0

    lax.fori_loop(0, MPS, grads, 0)
    turn = [ins.turn(n) for n in range(LINES)]

    def step(fn, *args):
        return functools.partial(fn, *args, whole)

    lay_rest, lay_first, lay_end, drain_lay = flat_grads(
        total, stotal, fl, roll, head, head_sem, wide, tall, gflat
    )
    zero_at = {
        1: [step(ins.zero_own, 2, turn[0])],
        2: [step(ins.zero_own, 2, turn[1])],
        3: [step(ins.zero_own, 2, turn[2])],
        4: [step(ins.zero_own, 2, turn[3])],
        5: [step(ins.zero_over, 0, turn[0])],
        9: [step(ins.zero_own, 0, turn[0]), step(ins.zero_over, 0, turn[1])],
        11: [functools.partial(ins.line_here, 1), step(ins.zero_end, 2)],
        13: [step(ins.zero_own, 0, turn[1]), step(ins.zero_over, 0, turn[2])],
    }
    one_at = {
        0: [step(ins.one_far, MPS - 1)],
        1: [step(ins.one_over, turn[0])],
        2: [step(ins.one_over, turn[1])],
        3: [step(ins.one_over, turn[2])],
        4: [step(ins.one_over, turn[3])],
        7: [step(ins.one_own, turn[0])],
        9: [step(ins.one_own, turn[1])],
        10: [step(ins.one_own, turn[2])],
        11: [step(ins.one_own, turn[3])],
    }
    acc[...] = jnp.zeros_like(acc)
    gvec[2:4, :] = jnp.zeros((2, C), f32)
    gl1[...] = jnp.zeros_like(gl1)

    def backward(n, _):
        j, i = n // images, n % images
        g = ins.turn(j)
        poll(zero_at, one_at, None, n)

        @pl.when(i == 0)
        def _():
            qkv[...] = jnp.zeros_like(qkv)

        attend_back(i, g, length, sel, gmix, wq, probs, qkv, acc, gvec)

        @pl.when((i == images - 1) & (j < NG - 1))
        def _():
            group_grads(g, gb, qkv, ln1)

            @pl.when(one)
            def _():
                for r in range(2):
                    ins.by_core(2 * g + r, 0, whole).start()

            group_norm_grad(g, wb, qkv, gl1)

        return 0

    lax.fori_loop(0, NG * images, backward, 0)
    own = ins.a
    group_grads(own, gb, qkv, ln1)

    @pl.when(one)
    def _():
        for same in (0, 1):
            for part in PARTS:
                ins.by_core(2 * own + (1 - ins.b if same == 0 else ins.b), 0, part).start()

    pl.when(zero)(lambda: ins.zero_own(0, turn[2], whole))
    scatter_smalls(gvec, gb1, acc, gsm, tabs2)

    @pl.when(zero)
    def _():
        for part in PARTS:
            ins.zero_over(0, own, part)

    group_norm_grad(own, wb, qkv, gl1)
    first_norm_sums(x, gl1, gvec)
    scatter_first(gvec, gsm)
    mid_sm, end_sm, drain_in = smalls_in(gsm, got, part_sm, got2, stotal, rsm_s, rsm_r, rsm_r2)
    pl.when(one)(lambda: ins.one_end(whole))
    lay_rest()
    first_norm_back(x, vecs, gl1, gres, gin)

    @pl.when(zero)
    def _():
        ins.line_here(0)
        for part in PARTS:
            ins.zero_own(0, own, part)
            ins.zero_end(0, part)

    mid_sm()
    lay_first()
    end_sm()
    lay_end()

    @pl.when(zero)
    def _():
        for row in range(MPS):
            for dd in (1, 3):
                ins.by_core(row, dd, whole).wait_send()
        ins.drain_tree(0, 2, whole)
        for n in range(LINES - 1):
            ins.drain_place(0, turn[n], 0, whole)
        for part in PARTS:
            ins.drain_place(0, own, 0, part)
            ins.drain_end(0, part)

    @pl.when(one)
    def _():
        for row in range(MPS):
            ins.by_core(row, 2, whole).wait_send()
        for n in range(LINES - 1):
            for r in range(2):
                ins.by_core(2 * turn[n] + r, 0, whole).wait_send()
        for r in range(2):
            for part in PARTS:
                ins.by_core(2 * own + r, 0, part).wait_send()
        ins.drain_tree(1, ins.d, whole)

    drain_lay()
    drain_in()
    outs.drain()
    drain_sm()


def step_call(x, cot, nlive, pf):
    rows = x.shape[0]
    images = rows // PIX
    length = image_frames(images)[2]
    sel = jnp.asarray(placement(images), bf16)
    mask = jnp.asarray(score_masks(), f32)
    vmem = pl.BlockSpec(memory_space=pltpu.VMEM)
    smem = pl.BlockSpec(memory_space=pltpu.SMEM)
    s = jax.ShapeDtypeStruct
    dma = pltpu.SemaphoreType.DMA
    nb = MPS * DPS
    return pl.pallas_call(
        functools.partial(step_kernel, images, rows, length),
        out_shape=(s((rows, C), bf16), s((rows, C), bf16), s((FLAT, 128), f32)),
        in_specs=[smem] + [vmem] * 5,
        out_specs=(vmem,) * 3,
        scratch_shapes=[
            pltpu.VMEM((792, 128), f32),
            pltpu.VMEM((792, 128), f32),
            pltpu.VMEM((2, 16, 128), f32),
            pltpu.VMEM((2 * C, 128), f32),
            pltpu.VMEM((256, C), f32),
            pltpu.VMEM((nb, QROWS, 256), bf16),
            pltpu.VMEM((MPS, 16, 128), bf16),
            pltpu.VMEM((8, C), f32),
            pltpu.VMEM((1, FF), f32),
            pltpu.VMEM((MPS, 384), f32),
            pltpu.VMEM((MPS, 512), f32),
            pltpu.VMEM((NW * NG, SEG, GH * SEG), f32),
            pltpu.VMEM((8, C), f32),
            pltpu.VMEM((1, FF), f32),
            pltpu.VMEM((NG, SEG, GH * SEG), f32),
            pltpu.VMEM((nb, QROWS, 256), bf16),
            pltpu.VMEM((MPS, 16, 128), f32),
            pltpu.VMEM((MPS, 16, 128), f32),
            pltpu.VMEM((16, 128), f32),
            pltpu.VMEM((DPS, 16, 128), f32),
            pltpu.VMEM((16, 128), f32),
            pltpu.VMEM((2 * MPS, QROWS, 256), bf16),
            pltpu.VMEM((MPS, QROWS, 256), bf16),
            pltpu.VMEM((2 * LINES, QROWS, 256), bf16),
            pltpu.VMEM((2 * LINES, QROWS, 256), bf16),
            pltpu.VMEM((QROWS, 256), f32),
            pltpu.VMEM((QROWS, 256), f32),
            dma((4,)),
            dma((3 + MPS,)),
            dma((MPS,)),
            dma((nb, 6)),
            dma((nb,)),
            dma((MPS,)),
            dma((MPS,)),
            dma((DPS,)),
            dma((2 * MPS, 2)),
            dma((2 * MPS, 2)),
            dma((MPS, 2)),
            dma((MPS, 2)),
            dma((2 * LINES, 2)),
            dma((2 * LINES, 2)),
            dma((2 * LINES, 2)),
            dma((2 * LINES, 2)),
        ]
        + mega_scratch(images, rows),
        compiler_params=pltpu.CompilerParams(
            vmem_limit_bytes=62 * 1024 * 1024, collective_id=0, has_side_effects=True
        ),
    )(nlive, x, cot, pf, sel, mask)


VEC_LABELS = [
    "norm1_gain",
    "norm1_bias",
    "query_bias",
    "value_bias",
    "proj_bias",
    "norm2_gain",
    "norm2_bias",
    "fc2_bias",
]


def segment_shapes(width_rank, hidden_rank):
    return [
        ("qkv_weight", (C, 3 * width_rank)),
        ("proj_weight", (width_rank, C)),
        ("fc1_weight", (C, hidden_rank)),
        ("fc2_weight", (hidden_rank, C)),
        ("norm1_gain", (width_rank,)),
        ("norm1_bias", (width_rank,)),
        ("query_bias", (width_rank,)),
        ("value_bias", (width_rank,)),
        ("proj_bias", (width_rank,)),
        ("norm2_gain", (width_rank,)),
        ("norm2_bias", (width_rank,)),
        ("fc1_bias", (hidden_rank,)),
        ("fc2_bias", (width_rank,)),
        ("table", (SPAN * SPAN, width_rank // HD)),
    ]


def unpack(flat, width_rank, hidden_rank):
    pieces = {}
    offset = 0
    for label, shape in segment_shapes(width_rank, hidden_rank):
        amount = math.prod(shape)
        pieces[label] = flat[:, offset : offset + amount].reshape((flat.shape[0],) + shape)
        offset = offset + amount
    return pieces


def finish(output, grad_input, grad_shard, params, moment_one, moment_two):
    group = lax.axis_index("dp")
    shard_length = params.shape[1]
    weights_rank = (4 * C * C + 2 * C * FF) // lax.axis_size("mp")
    position = group * shard_length + jnp.arange(shard_length, dtype=jnp.int32)[None, :]
    decays = (position < weights_rank).astype(jnp.float32)
    new_one = beta_one * moment_one + (1.0 - beta_one) * grad_shard
    new_two = second_decay_rate * moment_two + (1.0 - second_decay_rate) * grad_shard * grad_shard
    corrected_one = new_one / (1.0 - beta_one**adam_step)
    corrected_two = new_two / (1.0 - second_decay_rate**adam_step)
    new_params = params - learn_rate * (
        corrected_one / (jnp.sqrt(corrected_two) + adam_eps) + weight_decay * decays * params
    )
    return (output, grad_input, grad_shard, new_params, new_one, new_two)


def local_xla(tokens, cotangent, image_counts, params, moment_one, moment_two):
    ranks = lax.axis_size("mp")
    rank = lax.axis_index("mp")
    group = lax.axis_index("dp")
    width = C // ranks
    hidden = FF // ranks
    heads = width // HD
    rows = tokens.shape[0]
    shard_length = params.shape[1]
    length = shard_length * lax.axis_size("dp")
    owned = lax.all_gather(params.astype(bf16), "mp", axis=0, tiled=True)
    owned = lax.all_gather(owned, "dp", axis=1, tiled=True)
    op = unpack(owned, width, hidden)
    wqkv = op["qkv_weight"].reshape(ranks, C, heads, 3, HD).transpose(3, 0, 2, 4, 1).reshape(3 * C, C)
    wproj = op["proj_weight"].reshape(C, C)
    w1 = op["fc1_weight"].transpose(1, 0, 2).reshape(C, FF)
    w2 = op["fc2_weight"].reshape(FF, C)
    vecs = jnp.stack([op[n].reshape(C) for n in VEC_LABELS]).astype(f32)
    b1 = op["fc1_bias"].reshape(1, FF).astype(f32)
    bias = score_bias(op["table"].transpose(1, 0, 2).reshape(-1, HEADS))
    limit = jnp.sum(
        jnp.where(jnp.arange(image_counts.shape[0], dtype=jnp.int32) == group, image_counts, 0)
    )
    nlive = jnp.clip(limit * PIX - rank * rows, 0, rows).reshape(1)
    output, grad_input, gqkv, gproj, g1, g2, gvec, gb1, acc = block_compute(
        tokens, cotangent, nlive, wqkv, wproj, w1, w2, vecs, b1, bias
    )
    gtable = table_back(acc)
    gvec = gvec.reshape(8, ranks, width)
    pieces = [
        gqkv.reshape(3, ranks, heads, HD, C).transpose(1, 4, 2, 0, 3).reshape(ranks, -1),
        gproj.reshape(ranks, -1),
        g1.reshape(C, ranks, hidden).transpose(1, 0, 2).reshape(ranks, -1),
        g2.T.reshape(ranks, -1),
    ]
    pieces += [gvec[i].astype(bf16) for i in range(7)]
    pieces += [gb1.reshape(ranks, hidden).astype(bf16), gvec[7].astype(bf16)]
    pieces += [gtable.reshape(-1, ranks, heads).transpose(1, 0, 2).reshape(ranks, -1).astype(bf16)]
    used = sum(p.shape[1] for p in pieces)
    pieces.append(jnp.zeros((ranks, length - used), bf16))
    flat = jnp.concatenate(pieces, axis=1)
    flat = lax.psum_scatter(flat, "mp", scatter_dimension=0, tiled=True)
    grad_shard = lax.psum_scatter(flat, "dp", scatter_dimension=1, tiled=True).astype(f32)
    return finish(output, grad_input, grad_shard, params, moment_one, moment_two)


def local(tokens, cotangent, image_counts, params, moment_one, moment_two):
    ranks = lax.axis_size("mp")
    rows = tokens.shape[0]
    shard = params.shape[1]
    fits = (
        ranks == MPS
        and lax.axis_size("dp") == DPS
        and rows % 16 == 0
        and image_frames(rows // PIX)[0][-1] + image_frames(rows // PIX)[2] <= rows
        and shard == QUART + OFFSET
    )
    if not fits:
        return local_xla(tokens, cotangent, image_counts, params, moment_one, moment_two)
    rank = lax.axis_index("mp")
    group = lax.axis_index("dp")
    limit = jnp.sum(
        jnp.where(jnp.arange(image_counts.shape[0], dtype=jnp.int32) == group, image_counts, 0)
    )
    nlive = jnp.clip(limit * PIX - rank * rows, 0, rows).reshape(1)
    pf = jnp.pad(params, ((0, 0), (0, FLAT * 128 - shard))).reshape(FLAT, 128)
    output, grad_input, gflat = step_call(tokens, cotangent, nlive, pf)
    grad_shard = gflat.reshape(1, -1)[:, :shard]
    return finish(output, grad_input, grad_shard, params, moment_one, moment_two)


def solution(mesh):
    return jax.shard_map(
        local,
        mesh=mesh,
        in_specs=(
            P(("dp", "mp"), None),
            P(("dp", "mp"), None),
            P(),
            P("mp", "dp"),
            P("mp", "dp"),
            P("mp", "dp"),
        ),
        out_specs=(
            P(("dp", "mp"), None),
            P(("dp", "mp"), None),
            P("mp", "dp"),
            P("mp", "dp"),
            P("mp", "dp"),
            P("mp", "dp"),
        ),
        check_vma=False,
    )
```

```python
import functools
import math

import jax
import jax.numpy as jnp
import numpy as np
from jax import lax
from jax.experimental import pallas as pl
from jax.experimental.pallas import tpu as pltpu
from jax.sharding import PartitionSpec as P

C = 512
FF = 2048
HD = 32
WIN = 7
MAP = 14
SHIFT = 3
PIX = MAP * MAP
HEADS = C // HD
SEG = 64
GH = 4
NG = HEADS // GH
SIDE = MAP // WIN
NW = SIDE * SIDE
SPAN = 2 * WIN - 1

norm_eps = 1e-05
mask_fill = -100.0
learn_rate = 0.05
beta_one = 0.9
second_decay_rate = 0.999
adam_eps = 1e-08
weight_decay = 0.05
adam_step = 2.0
f32 = jnp.float32
bf16 = jnp.bfloat16


def mm(a, b):
    return lax.dot_general(a, b, (((1,), (0,)), ((), ())), preferred_element_type=f32)


def mm_t(a, b):
    return lax.dot_general(a, b, (((1,), (1,)), ((), ())), preferred_element_type=f32)


def mm_r(a, b):
    return lax.dot_general(a, b, (((0,), (0,)), ((), ())), preferred_element_type=f32)


def norm_stats(values):
    center = jnp.mean(values, axis=1, keepdims=True)
    spread = jnp.mean(jnp.square(values - center), axis=1, keepdims=True)
    return center, lax.rsqrt(spread + norm_eps)


def norm_back(scaled, unit, scale):
    return scale * (
        scaled
        - jnp.mean(scaled, axis=1, keepdims=True)
        - unit * jnp.mean(scaled * unit, axis=1, keepdims=True)
    )


def phi_parts(v):
    return 0.5 * (1.0 + lax.erf(v * (1.0 / math.sqrt(2.0)))), jnp.exp(-0.5 * v * v)


def window_sites():
    w = np.arange(NW)[:, None]
    p = np.arange(WIN * WIN)[None, :]
    row = (w // SIDE) * WIN + p // WIN
    col = (w % SIDE) * WIN + p % WIN
    token = ((row + SHIFT) % MAP) * MAP + (col + SHIFT) % MAP

    def region(c):
        return (c >= MAP - WIN).astype(np.int32) + (c >= MAP - SHIFT).astype(np.int32)

    ids = region(row) * 3 + region(col)
    return token, ids


def image_frames(images):
    starts = [PIX * i // 16 * 16 for i in range(images)]
    offsets = [PIX * i - s for i, s in enumerate(starts)]
    length = -(-(PIX + max(offsets)) // 16) * 16
    return starts, offsets, length


def placement(images):
    token, _ = window_sites()
    starts, offsets, length = image_frames(images)
    sel = np.zeros((images, NW * SEG, length), np.float32)
    for i in range(images):
        for w in range(NW):
            sel[i, w * SEG + np.arange(WIN * WIN), token[w] + offsets[i]] = 1.0
    return sel


def score_bias(table):
    size = WIN * WIN
    p = np.arange(size)
    a, b = p // WIN, p % WIN
    off = (a[None, :] - a[:, None] + WIN - 1) * SPAN + b[None, :] - b[:, None] + WIN - 1
    one_hot = np.zeros((size, size, SPAN * SPAN), np.float32)
    one_hot[np.arange(size)[:, None], np.arange(size)[None, :], off] = 1.0
    _, ids = window_sites()
    full_mask = np.full((NW, SEG, SEG), 0.0, np.float32)
    full_mask[:, size:, :] = -1e30
    full_mask[:, :size, :size] = np.where(ids[:, :, None] == ids[:, None, :], 0.0, mask_fill)
    onehot = jnp.asarray(one_hot.reshape(size * size, -1), bf16)
    bias = jnp.dot(table.T.astype(bf16), onehot.T, preferred_element_type=f32)
    bias = bias.reshape(NG, GH, size, size)
    bias = jnp.pad(bias, ((0, 0), (0, 0), (0, SEG - size), (0, SEG - size)))
    bias = bias.transpose(0, 2, 1, 3)
    out = bias[None] + jnp.asarray(full_mask)[:, None, :, None, :]
    return out.reshape(NW * NG, SEG, GH * SEG)


def table_back(acc):
    size = WIN * WIN
    p = np.arange(size)
    a, b = p // WIN, p % WIN
    off = (a[None, :] - a[:, None] + WIN - 1) * SPAN + b[None, :] - b[:, None] + WIN - 1
    one_hot = np.zeros((size * size, SPAN * SPAN), np.float32)
    one_hot[np.arange(size * size), off.reshape(-1)] = 1.0
    acc = acc.reshape(NG, SEG, GH, SEG)[:, :size, :, :size].transpose(0, 2, 1, 3).reshape(HEADS, size * size)
    hi = acc.astype(bf16)
    lo = (acc - hi.astype(f32)).astype(bf16)
    oh = jnp.asarray(one_hot, bf16)
    return (
        jnp.dot(hi, oh, preferred_element_type=f32) + jnp.dot(lo, oh, preferred_element_type=f32)
    ).T


def lane_head_mask():
    return lax.broadcasted_iota(jnp.int32, (SEG, GH * HD), 1) // HD


def block_diag(part, head_of_lane):
    zero = jnp.zeros_like(part)
    return jnp.concatenate([jnp.where(head_of_lane == h, part, zero) for h in range(GH)], axis=0)


def diag_pick(full, head_of_lane):
    out = full[:SEG]
    for h in range(1, GH):
        out = jnp.where(head_of_lane == h, full[h * SEG : (h + 1) * SEG], out)
    return out


def compute_kernel(
    images, rows, block, length,
    nlive, x, cot, wqkv, wproj, w1, w2, vecs, b1, bias, sel,
    out, gin, gqkv_w, gproj_w, g1_w, g2_w, gvec, gb1, acc,
    ln1, qkv, wq, probs, mixw, mixed, ln2, act, gpre, gresb, gres, gmix, gwin,
):
    blocks = rows // block
    frame = image_frames(images)[0]
    head_of_lane = lane_head_mask()

    def vec(i):
        return vecs[i : i + 1, :]

    gvec[...] = jnp.zeros_like(gvec)
    gb1[...] = jnp.zeros_like(gb1)
    acc[...] = jnp.zeros_like(acc)
    mixed[...] = jnp.zeros_like(mixed)

    def norm_rows(t, _):
        sl = pl.ds(pl.multiple_of(t * block, 16), block)
        xin = x[sl, :].astype(f32)
        center, scale = norm_stats(xin)
        normed = ((xin - center) * scale * vec(0) + vec(1)).astype(bf16)
        ln1[sl, :] = normed
        qkv[sl, 0:C] = ((mm_t(normed, wqkv[0:C, :]) + vec(2)) * HD ** (-0.5)).astype(bf16)
        qkv[sl, C : 2 * C] = mm_t(normed, wqkv[C : 2 * C, :]).astype(bf16)
        qkv[sl, 2 * C : 3 * C] = (mm_t(normed, wqkv[2 * C : 3 * C, :]) + vec(3)).astype(bf16)
        return 0

    lax.fori_loop(0, blocks, norm_rows, 0)

    for i in range(images):
        fr = pl.ds(frame[i], length)
        wq[i] = mm(sel[i], qkv[fr, :]).astype(bf16)

        def window(w, _):
            ws = pl.ds(pl.multiple_of(w * SEG, SEG), SEG)
            for g in range(NG):
                q = wq[i, ws, g * 128 : (g + 1) * 128]
                k = wq[i, ws, C + g * 128 : C + (g + 1) * 128]
                v = wq[i, ws, 2 * C + g * 128 : 2 * C + (g + 1) * 128]
                st = mm_t(k, block_diag(q, head_of_lane)) + bias[w * NG + g]
                e = jnp.exp(st - jnp.max(st, axis=0, keepdims=True))
                pt = (e * (1.0 / jnp.sum(e, axis=0, keepdims=True))).astype(bf16)
                probs[i, w * NG + g] = pt
                mixw[ws, g * 128 : (g + 1) * 128] = diag_pick(mm_r(pt, v), head_of_lane).astype(bf16)
            return 0

        lax.fori_loop(0, NW, window, 0)
        mixed[fr, :] = (mixed[fr, :].astype(f32) + mm_r(sel[i], mixw[...])).astype(bf16)

    def middle(t, _):
        sl = pl.ds(pl.multiple_of(t * block, 16), block)
        xin = x[sl, :].astype(f32)
        res = xin + (mm(mixed[sl, :], wproj[...]) + vec(4))
        center, scale = norm_stats(res)
        unit = (res - center) * scale
        normed = (unit * vec(5) + vec(6)).astype(bf16)
        ln2[sl, :] = normed
        live = (
            lax.broadcasted_iota(jnp.int32, (block, 1), 0) + t * block < nlive[0]
        ).astype(f32)
        gout = live * cot[sl, :].astype(f32)
        goutb = gout.astype(bf16)
        feed = jnp.zeros((block, C), f32)
        gln = jnp.zeros((block, C), f32)
        for j in range(4):
            js = slice(j * 512, (j + 1) * 512)
            pre = mm(normed, w1[:, js]) + b1[:, js]
            phi, e = phi_parts(pre)
            av = (pre * phi).astype(bf16)
            act[sl, js] = av
            feed = feed + mm(av, w2[js, :])
            gp = mm_t(goutb, w2[js, :]) * (phi + pre * (e * (1.0 / math.sqrt(2.0 * math.pi))))
            gb1[:, js] += jnp.sum(gp, axis=0, keepdims=True)
            gpb = gp.astype(bf16)
            gpre[sl, js] = gpb
            gln = gln + mm_t(gpb, w1[:, js])
        out[sl, :] = (live * (res + feed + vec(7))).astype(bf16)
        gr = gout + norm_back(gln * vec(5), unit, scale)
        gres[sl, :] = gr
        grb = gr.astype(bf16)
        gresb[sl, :] = grb
        gmix[sl, :] = mm_t(grb, wproj[...]).astype(bf16)
        gvec[4:5, :] += jnp.sum(gr, axis=0, keepdims=True)
        gvec[5:6, :] += jnp.sum(gln * unit, axis=0, keepdims=True)
        gvec[6:7, :] += jnp.sum(gln, axis=0, keepdims=True)
        gvec[7:8, :] += jnp.sum(gout, axis=0, keepdims=True)
        return 0

    lax.fori_loop(0, blocks, middle, 0)

    def masked_cot():
        live = (lax.broadcasted_iota(jnp.int32, (rows, 1), 0) < nlive[0]).astype(bf16)
        return cot[...] * live

    gout_all = masked_cot()

    def ff_grads(j, _):
        js = pl.ds(pl.multiple_of(j * 256, 256), 256)
        g2_w[:, js] = mm_r(gout_all, act[:, js]).astype(g2_w.dtype)
        g1_w[:, js] = mm_r(ln2[...], gpre[:, js]).astype(g1_w.dtype)
        return 0

    lax.fori_loop(0, FF // 256, ff_grads, 0)
    gproj_w[...] = mm_r(mixed[...], gresb[...]).astype(gproj_w.dtype)

    qkv[...] = jnp.zeros_like(qkv)
    for i in range(images):
        fr = pl.ds(frame[i], length)
        mixw[...] = mm(sel[i], gmix[fr, :]).astype(bf16)

        def window(w, _):
            ws = pl.ds(pl.multiple_of(w * SEG, SEG), SEG)
            for g in range(NG):
                q = wq[i, ws, g * 128 : (g + 1) * 128]
                k = wq[i, ws, C + g * 128 : C + (g + 1) * 128]
                v = wq[i, ws, 2 * C + g * 128 : 2 * C + (g + 1) * 128]
                pt = probs[i, w * NG + g]
                dod = block_diag(mixw[ws, g * 128 : (g + 1) * 128], head_of_lane)
                gv = mm(pt, dod)
                dpt = mm_t(v, dod)
                ptf = pt.astype(f32)
                prod = ptf * dpt
                dst = prod - ptf * jnp.sum(prod, axis=0, keepdims=True)
                acc[g] += dst
                dsb = dst.astype(bf16)
                gk = mm(dsb, block_diag(q, head_of_lane))
                gq = diag_pick(mm_r(dsb, k), head_of_lane) * HD ** (-0.5)
                gl = slice(g * 128, (g + 1) * 128)
                gvec[2:3, gl] += jnp.sum(gq, axis=0, keepdims=True)
                gvec[3:4, gl] += jnp.sum(gv, axis=0, keepdims=True)
                gwin[ws, g * 128 : (g + 1) * 128] = gq.astype(bf16)
                gwin[ws, C + g * 128 : C + (g + 1) * 128] = gk.astype(bf16)
                gwin[ws, 2 * C + g * 128 : 2 * C + (g + 1) * 128] = gv.astype(bf16)
            return 0

        lax.fori_loop(0, NW, window, 0)
        qkv[fr, :] = (qkv[fr, :].astype(f32) + mm_r(sel[i], gwin[...])).astype(bf16)

    def last(t, _):
        sl = pl.ds(pl.multiple_of(t * block, 16), block)
        gln = mm(qkv[sl, :], wqkv[...])
        xin = x[sl, :].astype(f32)
        center, scale = norm_stats(xin)
        unit = (xin - center) * scale
        gvec[0:1, :] += jnp.sum(gln * unit, axis=0, keepdims=True)
        gvec[1:2, :] += jnp.sum(gln, axis=0, keepdims=True)
        gin[sl, :] = (gres[sl, :] + norm_back(gln * vec(0), unit, scale)).astype(bf16)
        return 0

    lax.fori_loop(0, blocks, last, 0)

    def qkv_grads(j, _):
        js = pl.ds(pl.multiple_of(j * 256, 256), 256)
        gqkv_w[js, :] = mm_r(qkv[:, js], ln1[...]).astype(gqkv_w.dtype)
        return 0

    lax.fori_loop(0, 3 * C // 256, qkv_grads, 0)


def block_size(rows):
    for cand in (112, 80, 64, 48, 32, 16):
        if rows % cand == 0:
            return cand
    return rows


def block_compute(x, cot, nlive, wqkv, wproj, w1, w2, vecs, b1, bias, interpret=False):
    tokens = x.shape[0]
    images = tokens // PIX
    rows = -(-tokens // 16) * 16
    if rows != tokens:
        x = jnp.pad(x, ((0, rows - tokens), (0, 0)))
        cot = jnp.pad(cot, ((0, rows - tokens), (0, 0)))
    block = block_size(rows)
    starts, _, length = image_frames(images)
    assert starts[-1] + length <= rows
    sel = jnp.asarray(placement(images), bf16)
    vmem = pl.BlockSpec(memory_space=pltpu.VMEM)
    smem = pl.BlockSpec(memory_space=pltpu.SMEM)
    s = jax.ShapeDtypeStruct
    outs = pl.pallas_call(
        functools.partial(compute_kernel, images, rows, block, length),
        out_shape=(
            s((rows, C), bf16),
            s((rows, C), bf16),
            s((3 * C, C), bf16),
            s((C, C), bf16),
            s((C, FF), bf16),
            s((C, FF), bf16),
            s((8, C), f32),
            s((1, FF), f32),
            s((NG, SEG, GH * SEG), f32),
        ),
        in_specs=[smem] + [vmem] * 10,
        out_specs=(vmem,) * 9,
        scratch_shapes=[
            pltpu.VMEM((rows, C), bf16),
            pltpu.VMEM((rows, 3 * C), bf16),
            pltpu.VMEM((images, NW * SEG, 3 * C), bf16),
            pltpu.VMEM((images, NW * NG, SEG, GH * SEG), bf16),
            pltpu.VMEM((NW * SEG, C), bf16),
            pltpu.VMEM((rows, C), bf16),
            pltpu.VMEM((rows, C), bf16),
            pltpu.VMEM((rows, FF), bf16),
            pltpu.VMEM((rows, FF), bf16),
            pltpu.VMEM((rows, C), bf16),
            pltpu.VMEM((rows, C), f32),
            pltpu.VMEM((rows, C), bf16),
            pltpu.VMEM((NW * SEG, 3 * C), bf16),
        ],
        compiler_params=pltpu.CompilerParams(vmem_limit_bytes=60 * 1024 * 1024),
        interpret=interpret,
    )(nlive, x, cot, wqkv, wproj, w1, w2, vecs, b1, bias, sel)
    return (outs[0][:tokens], outs[1][:tokens]) + outs[2:]

LINES = 4
MPS = 8
DPS = 4
QROWS = 384
QUART = QROWS * 256
FLAT = 776
MESH = pl.DeviceIdType.MESH


def base_of(p):
    return (p // WIN) * SPAN + p % WIN


def iota(shape, dim):
    return lax.broadcasted_iota(jnp.int32, shape, dim)


def as_bf(mask):
    return jnp.where(mask, 1.0, 0.0).astype(bf16)


def spread_queries():
    row = iota((GH * 256, GH * SEG), 0)
    lane = iota((GH * 256, GH * SEG), 1)
    q = lane % SEG
    return as_bf((row // 256 == lane // SEG) & (row % 256 == base_of(q)) & (q < WIN * WIN))


def key_rows(reverse):
    k = iota((SEG, 8 * WIN), 0)
    row = iota((SEG, 8 * WIN), 1)
    b = WIN - 1 - k % WIN if reverse else k % WIN
    return as_bf((row == (k // WIN) * 8 + b) & (k < WIN * WIN))


def table_lanes():
    row = iota((384, 512), 0)
    lane = iota((384, 512), 1)
    return as_bf((row == 2 * (lane % 256) + lane // 256) & (lane % 256 < SPAN * SPAN))


def split_mm(op, exact, value):
    hi = value.astype(bf16)
    lo = (value - hi.astype(f32)).astype(bf16)
    return op(exact, hi) + op(exact, lo)


def split_mm_left(op, value, exact):
    hi = value.astype(bf16)
    lo = (value - hi.astype(f32)).astype(bf16)
    return op(hi, exact) + op(lo, exact)


def turn_rows(part):
    return pltpu.roll(part, 0, 1, stride=1, stride_axis=0)


def gather_smalls(sm, vecs, b1, tabs, bias, mask):
    lane = iota((16, 128), 1)
    low = lane < 64
    for g in range(4):
        first, second = sm[2 * g].astype(f32), sm[2 * g + 1].astype(f32)
        turned = [pltpu.roll(first, 64, 1), pltpu.roll(second, 64, 1)]
        los = jnp.where(low, first, turned[1])
        his = jnp.where(low, turned[0], second)
        gl = slice(g * 128, (g + 1) * 128)
        for i, src, row in (
            (0, los, 0), (1, his, 0), (2, los, 1), (3, his, 1), (4, los, 2), (5, his, 2), (6, los, 3), (7, his, 5),
        ):
            vecs[i : i + 1, gl] = src[row : row + 1]
        for k in range(2):
            r = 2 * g + k
            full = (first, second)[k]
            rot = turned[k]
            b1[:, r * 256 : r * 256 + 128] = jnp.where(low[:1], rot[3:4], rot[4:5])
            b1[:, r * 256 + 128 : r * 256 + 256] = jnp.where(low[:1], rot[4:5], rot[5:6])
            for j in range(3):
                tabs[r : r + 1, j * 128 : (j + 1) * 128] = full[6 + j : 7 + j]
    tab = mm(tabs[...].astype(bf16), table_lanes())
    spread = spread_queries()
    keys = key_rows(False)
    for g in range(NG):
        parts = []
        for h in range(GH):
            r, i = divmod(g * GH + h, 2)
            t = jnp.broadcast_to(tab[r : r + 1, i * 256 : (i + 1) * 256], (8, 256))
            rows = [
                turn_rows(pltpu.roll(t, (SPAN * a - 84) % 256, 1)) for a in range(WIN)
            ]
            parts.append(jnp.concatenate(rows, axis=0))
        line = jnp.concatenate(parts, axis=1).astype(bf16)
        placed = mm(line, spread).astype(bf16)
        bt = mm(keys, placed)
        for w in range(NW):
            bias[w * NG + g] = bt + mask[w]


def row_half(gvec, i, r):
    g, k = divmod(r, 2)
    v = gvec[i : i + 1, g * 128 : (g + 1) * 128]
    turned = pltpu.roll(v, 64, 1)
    return (v, turned) if k == 0 else (turned, v)


def scatter_first(gvec, gsm):
    low = iota((1, 128), 1) < 64
    for r in range(MPS):
        gsm[r, 0:1, :] = jnp.where(low, row_half(gvec, 0, r)[0], row_half(gvec, 1, r)[1])


def scatter_smalls(gvec, gb1, acc, gsm, tabs):
    lane = iota((1, 128), 1)
    low = lane < 64
    spread = spread_queries()
    keys = key_rows(True)
    tabs[...] = jnp.zeros_like(tabs)
    for g in range(NG):
        z = split_mm(mm_r, keys, acc[g])
        y = split_mm_left(mm_t, z, spread)
        for h in range(GH):
            r, i = divmod(g * GH + h, 2)
            total = jnp.zeros((8, 256), f32)
            for a in range(WIN):
                part = y[8 * a : 8 * a + 8, h * 256 : (h + 1) * 256]
                total = total + turn_rows(pltpu.roll(part, (78 - SPAN * a) % 256, 1))
            tabs[r : r + 1, i * 256 : (i + 1) * 256] = jnp.sum(total, axis=0, keepdims=True)
    flat = split_mm_left(mm_t, tabs[...], table_lanes())

    half = functools.partial(row_half, gvec)
    zero = jnp.zeros((1, 128), f32)
    for r in range(MPS):
        fb0 = gb1[:, r * 256 : r * 256 + 128]
        fb1 = gb1[:, r * 256 + 128 : r * 256 + 256]
        t0, t1 = pltpu.roll(fb0, 64, 1), pltpu.roll(fb1, 64, 1)
        rows = [
            jnp.where(low, half(2, r)[0], half(3, r)[1]),
            jnp.where(low, half(4, r)[0], half(5, r)[1]),
            jnp.where(low, half(6, r)[0], t0),
            jnp.where(low, t0, t1),
            jnp.where(low, t1, half(7, r)[1]),
        ]
        for j, row in enumerate(rows):
            gsm[r, 1 + j : 2 + j, :] = row
        for j in range(3):
            gsm[r, 6 + j : 7 + j, :] = flat[r : r + 1, j * 128 : (j + 1) * 128]
        for j in range(9, 16):
            gsm[r, j : j + 1, :] = zero


def slot(m, d):
    return m * DPS + d


def w_qkv(wb, kind, quad, half):
    return jnp.concatenate(
        [wb[slot(4 * quad + r, 0), half * 192 + kind * 64 : half * 192 + kind * 64 + 64, :] for r in range(4)], axis=0
    )


def w_proj(wb, quad, half):
    return jnp.concatenate([wb[slot(4 * quad + r, 1), half * 64 : half * 64 + 64, :] for r in range(4)], axis=0)


def w_one(wb, r, half):
    return wb[slot(r, 1), 128:384, :] if half == 0 else wb[slot(r, 2), 0:256, :]


def w_two(wb, r, half):
    return jnp.concatenate(
        [
            wb[slot(r, 2), 256 + half * 64 : 256 + half * 64 + 64, :],
            wb[slot(r, 3), half * 192 : half * 192 + 192, :],
        ],
        axis=0,
    )


HALVES = (slice(0, 256), slice(256, 512))


def first_norm(x, vecs, ln1):
    xin = x[...].astype(f32)
    center, scale = norm_stats(xin)
    ln1[...] = ((xin - center) * scale * vecs[0:1, :] + vecs[1:2, :]).astype(bf16)


def group_lanes(g):
    return pl.ds(pl.multiple_of(g * 128, 128), 128)


def group_qkv(wb, g, half):
    return jnp.concatenate(
        [
            wb[slot(2 * g + r, 0), half * 192 + kind * 64 : half * 192 + kind * 64 + 64, :]
            for kind in range(3)
            for r in range(2)
        ],
        axis=0,
    )


def project_group(g, wb, vecs, ln1, qkv):
    val = mm_t(ln1[:, HALVES[0]], group_qkv(wb, g, 0)) + mm_t(ln1[:, HALVES[1]], group_qkv(wb, g, 1))
    gl = group_lanes(g)
    qkv[:, 0:128] = ((val[:, 0:128] + vecs[2:3, gl]) * HD ** (-0.5)).astype(bf16)
    qkv[:, 128:256] = val[:, 128:256].astype(bf16)
    qkv[:, 256:384] = (val[:, 256:384] + vecs[3:4, gl]).astype(bf16)


def frame_rows(i, length):
    return pl.ds(pl.multiple_of(PIX * i // 16 * 16, 16), length)


def attend(i, g, length, sel, bias, qkv, wq, probs, mixed):
    head_of_lane = lane_head_mask()
    fr = frame_rows(i, length)
    wq[g, i] = mm(sel[i], qkv[fr, :]).astype(bf16)
    outs = []
    for w in range(NW):
        ws = slice(w * SEG, (w + 1) * SEG)
        q, k, v = (wq[g, i, ws, n * 128 : (n + 1) * 128] for n in range(3))
        st = mm_t(k, block_diag(q, head_of_lane)) + bias[w * NG + g]
        e = jnp.exp(st - jnp.max(st, axis=0, keepdims=True))
        pt = (e * (1.0 / jnp.sum(e, axis=0, keepdims=True))).astype(bf16)
        probs[g, i, w] = pt
        outs.append(diag_pick(mm_r(pt, v), head_of_lane).astype(bf16))
    gl = group_lanes(g)
    back = mm_r(sel[i], jnp.concatenate(outs, axis=0))
    mixed[fr, gl] = (mixed[fr, gl].astype(f32) + back).astype(bf16)


def attend_back(i, g, length, sel, gmix, wq, probs, gqkv, acc, gvec):
    head_of_lane = lane_head_mask()
    fr = frame_rows(i, length)
    gl = group_lanes(g)
    gwin = mm(sel[i], gmix[fr, gl]).astype(bf16)
    outs = []
    for w in range(NW):
        ws = slice(w * SEG, (w + 1) * SEG)
        q, k, v = (wq[g, i, ws, n * 128 : (n + 1) * 128] for n in range(3))
        pt = probs[g, i, w]
        dod = block_diag(gwin[ws, :], head_of_lane)
        gv = mm(pt, dod)
        dpt = mm_t(v, dod)
        ptf = pt.astype(f32)
        prod = ptf * dpt
        dst = prod - ptf * jnp.sum(prod, axis=0, keepdims=True)
        acc[g] += dst
        dsb = dst.astype(bf16)
        gk = mm(dsb, block_diag(q, head_of_lane))
        gq = diag_pick(mm_r(dsb, k), head_of_lane) * HD ** (-0.5)
        gvec[2:3, gl] += jnp.sum(gq, axis=0, keepdims=True)
        gvec[3:4, gl] += jnp.sum(gv, axis=0, keepdims=True)
        outs.append(jnp.concatenate([gq.astype(bf16), gk.astype(bf16), gv.astype(bf16)], axis=1))
    back = mm_r(sel[i], jnp.concatenate(outs, axis=0))
    gqkv[fr, :] = (gqkv[fr, :].astype(f32) + back).astype(bf16)


def group_grads(g, gb, gqkv, ln1):
    part = mm_r(gqkv[...], ln1[...]).astype(bf16)
    for kind in range(3):
        for r in range(2):
            at = kind * 128 + r * 64
            for h in range(2):
                to = h * 192 + kind * 64
                gb[slot(2 * g + r, 0), to : to + 64, :] = part[at : at + 64, HALVES[h]]


def group_norm_grad(g, wb, gqkv, gl1):
    for h in range(2):
        gl1[:, HALVES[h]] += mm(gqkv[...], group_qkv(wb, g, h))


def feed_forward(rows, live_rows, x, cot, wb, vecs, b1, out, gvec, gb1, mixed, ln2, act, gpre, gresb, gres, gmix, goutb):
    def vec(i):
        return vecs[i : i + 1, :]

    att = [mm(mixed[:, HALVES[0]], w_proj(wb, 0, h)) + mm(mixed[:, HALVES[1]], w_proj(wb, 1, h)) for h in range(2)]
    res = x[...].astype(f32) + (jnp.concatenate(att, axis=1) + vec(4))
    center, scale = norm_stats(res)
    unit = (res - center) * scale
    ln2[...] = (unit * vec(5) + vec(6)).astype(bf16)
    live = (iota((rows, 1), 0) < live_rows).astype(f32)
    gout = live * cot[...].astype(f32)
    goutb[...] = gout.astype(bf16)
    feed = [jnp.zeros((rows, 256), f32)] * 2
    gln = [jnp.zeros((rows, 256), f32)] * 2
    for r in range(MPS):
        js = slice(r * 256, (r + 1) * 256)
        pre = mm(ln2[:, HALVES[0]], w_one(wb, r, 0)) + mm(ln2[:, HALVES[1]], w_one(wb, r, 1)) + b1[:, js]
        phi, e = phi_parts(pre)
        av = (pre * phi).astype(bf16)
        act[:, js] = av
        feed = [feed[h] + mm(av, w_two(wb, r, h)) for h in range(2)]
        ga = mm_t(goutb[:, HALVES[0]], w_two(wb, r, 0)) + mm_t(goutb[:, HALVES[1]], w_two(wb, r, 1))
        gp = ga * (phi + pre * (e * (1.0 / math.sqrt(2.0 * math.pi))))
        gb1[:, js] = jnp.sum(gp, axis=0, keepdims=True)
        gpb = gp.astype(bf16)
        gpre[:, js] = gpb
        gln = [gln[h] + mm_t(gpb, w_one(wb, r, h)) for h in range(2)]
    feed = jnp.concatenate(feed, axis=1)
    gln = jnp.concatenate(gln, axis=1)
    out[...] = (live * (res + feed + vec(7))).astype(bf16)
    gr = gout + norm_back(gln * vec(5), unit, scale)
    gres[...] = gr
    grb = gr.astype(bf16)
    gresb[...] = grb
    for quad in range(2):
        gmix[:, HALVES[quad]] = (
            mm_t(grb[:, HALVES[0]], w_proj(wb, quad, 0)) + mm_t(grb[:, HALVES[1]], w_proj(wb, quad, 1))
        ).astype(bf16)
    gvec[4:5, :] = jnp.sum(gr, axis=0, keepdims=True)
    gvec[5:6, :] = jnp.sum(gln * unit, axis=0, keepdims=True)
    gvec[6:7, :] = jnp.sum(gln, axis=0, keepdims=True)
    gvec[7:8, :] = jnp.sum(gout, axis=0, keepdims=True)


def proj_grads(gb, mixed, gresb):
    gproj = mm_r(mixed[...], gresb[...]).astype(bf16)
    for r in range(MPS):
        for h in range(2):
            gb[slot(r, 1), h * 64 : h * 64 + 64, :] = gproj[r * 64 : r * 64 + 64, HALVES[h]]


def feed_forward_grads(r, gb, act, goutb, ln2, gpre):
    js = pl.ds(pl.multiple_of(r * 256, 256), 256)
    two = mm_r(act[:, js], goutb[...]).astype(bf16)
    for h in range(2):
        gb[slot(r, 2), 256 + h * 64 : 256 + h * 64 + 64, :] = two[0:64, HALVES[h]]
        gb[slot(r, 3), h * 192 : h * 192 + 192, :] = two[64:256, HALVES[h]]
    one = mm_r(ln2[...], gpre[:, js]).astype(bf16)
    gb[slot(r, 1), 128:384, :] = one[0:256]
    gb[slot(r, 2), 0:256, :] = one[256:512]


def first_norm_sums(x, gl1, gvec):
    xin = x[...].astype(f32)
    center, scale = norm_stats(xin)
    unit = (xin - center) * scale
    gln = gl1[...]
    gvec[0:1, :] = jnp.sum(gln * unit, axis=0, keepdims=True)
    gvec[1:2, :] = jnp.sum(gln, axis=0, keepdims=True)


def first_norm_back(x, vecs, gl1, gres, gin):
    xin = x[...].astype(f32)
    center, scale = norm_stats(xin)
    unit = (xin - center) * scale
    gin[...] = (gres[...] + norm_back(gl1[...] * vecs[0:1, :], unit, scale)).astype(bf16)


def mega_scratch(images, rows):
    return [
        pltpu.VMEM((rows, C), bf16),
        pltpu.VMEM((rows, 384), bf16),
        pltpu.VMEM((NG, images, NW * SEG, 384), bf16),
        pltpu.VMEM((NG, images, NW, SEG, GH * SEG), bf16),
        pltpu.VMEM((rows, C), bf16),
        pltpu.VMEM((rows, C), bf16),
        pltpu.VMEM((rows, FF), bf16),
        pltpu.VMEM((rows, FF), bf16),
        pltpu.VMEM((rows, C), bf16),
        pltpu.VMEM((rows, C), f32),
        pltpu.VMEM((rows, C), bf16),
        pltpu.VMEM((rows, C), f32),
        pltpu.VMEM((rows, C), bf16),
    ]


def score_masks():
    _, ids = window_sites()
    size = WIN * WIN
    full = np.zeros((NW, SEG, SEG), np.float32)
    full[:, size:, :] = -1e30
    full[:, :size, :size] = np.where(ids[:, :, None] == ids[:, None, :], 0.0, mask_fill)
    return np.tile(full, (1, 1, GH))


def place():
    d, m = lax.axis_index("dp"), lax.axis_index("mp")
    return d, m, d // 2, d % 2, m // 2, m % 2


def twin(a, j):
    return 2 * ((a // 2 + j // 2) % 2) + (a + j) % 2


def remote(src, dst, send, recv, dev):
    return pltpu.make_async_remote_copy(
        src_ref=src, dst_ref=dst, send_sem=send, recv_sem=recv, device_id=dev, device_id_type=MESH
    )


def peers():
    d, m, *_ = place()
    return [{"dp": (d + k) % DPS, "mp": m} for k in range(1, DPS)] + [
        {"dp": d, "mp": (m + k) % MPS} for k in range(1, MPS)
    ]


def greet():
    barrier = pltpu.get_barrier_semaphore()
    for dev in peers():
        pl.semaphore_signal(barrier, inc=1, device_id=dev, device_id_type=MESH)


def greeted():
    pl.semaphore_wait(pltpu.get_barrier_semaphore(), DPS - 1 + MPS - 1)


OFFSET = 277


def flatten_params(pf, fl, roll, head, head_sem, wide, wb, sm):
    d, m, *_ = place()
    lane = iota((FLAT, 128), 1)
    roll[0:8, :] = jnp.zeros((8, 128), f32)
    fl[FLAT : FLAT + 16, :] = jnp.zeros((16, 128), f32)
    for k in range(DPS):

        @pl.when(d == k)
        def _(k=k):
            lanes, down = OFFSET * k % 128, OFFSET * k // 128
            if k == 0:
                fl[0:FLAT, :] = pf[...]
            else:
                roll[8 : 8 + FLAT, :] = pltpu.roll(pf[...], lanes, 1)
                fl[down : down + FLAT, :] = jnp.where(
                    lane >= lanes, roll[8 : 8 + FLAT, :], roll[7 : 7 + FLAT, :]
                )

    def cut(start, size, step):
        return fl[pl.ds(start, size, stride=step), :]

    @pl.when(d == 0)
    def _():
        low = iota((256, 128), 1) < 64
        one, two = pltpu.roll(cut(1, 256, 3), 64, 1), pltpu.roll(cut(2, 256, 3), 64, 1)
        wide[pl.ds(0, 256, stride=2), :] = cut(0, 256, 3)
        wide[pl.ds(C, 256, stride=2), :] = cut(1, 256, 3)
        wide[pl.ds(1, 256, stride=2), :] = jnp.where(low, one, two)
        wide[pl.ds(C + 1, 256, stride=2), :] = two
        turned = jnp.concatenate([wide[0:C, :].T, wide[C : 2 * C, :].T], axis=0).astype(bf16)
        s = slot(m, 0)
        for half in range(2):
            for kind in range(3):
                for i in range(2):
                    to = half * 192 + kind * 64 + i * 32
                    frm = i * 96 + kind * 32
                    wb[s, to : to + 32, :] = turned[frm : frm + 32, HALVES[half]]

    @pl.when(d == DPS - 1)
    def _():
        sm[m] = fl[768:784, :].astype(bf16)

    over = remote(fl.at[768:784], head.at[0], head_sem.at[0], head_sem.at[1], {"dp": (d + 1) % DPS, "mp": m})

    def rest():
        @pl.when(d > 0)
        def _():
            over.wait_recv()
            pos = iota((8, 128), 0) * 128 + iota((8, 128), 1)
            fl[0:8, :] = jnp.where(pos < OFFSET * d, head[0, 0:8, :], fl[0:8, :])

        @pl.when(d == 1)
        def _():
            s = slot(m, 1)
            for j in range(2):
                js = slice(j * 128, (j + 1) * 128)
                for half in range(2):
                    wb[s, half * 64 : half * 64 + 64, js] = cut(2 * half + j, 64, 4).astype(bf16)
                wb[s, 128:384, js] = cut(256 + j, 256, 2).astype(bf16)

        @pl.when(d == 2)
        def _():
            s = slot(m, 2)
            for j in range(2):
                js = slice(j * 128, (j + 1) * 128)
                wb[s, 0:256, js] = cut(j, 256, 2).astype(bf16)
                for half in range(2):
                    at = 256 + half * 64
                    wb[s, at : at + 64, js] = cut(512 + 2 * half + j, 64, 4).astype(bf16)

        @pl.when(d == 3)
        def _():
            s = slot(m, 3)
            for j in range(2):
                js = slice(j * 128, (j + 1) * 128)
                for half in range(2):
                    wb[s, half * 192 : half * 192 + 192, js] = cut(2 * half + j, 192, 4).astype(bf16)

        pl.when(d < DPS - 1)(lambda: over.wait_send())

    return lambda: pl.when(d < DPS - 1)(lambda: over.start()), rest


def smalls_out(sm, ssem, rsem):
    d, m, *_ = place()
    last = d == DPS - 1

    def over_mp(k):
        return remote(sm.at[m], sm.at[m], ssem.at[k], rsem.at[m], {"dp": d, "mp": (m + k) % MPS})

    def over_dp(k):
        return remote(sm, sm, ssem.at[MPS + k], rsem.at[MPS], {"dp": k, "mp": m})

    def begin():
        @pl.when(last)
        def _():
            for k in range(1, MPS):
                over_mp(k).start()

    def finish():
        @pl.when(last)
        def _():
            for k in range(1, MPS):
                src = (m + k) % MPS
                remote(sm.at[src], sm.at[src], ssem.at[0], rsem.at[src], {"dp": d, "mp": src}).wait_recv()
            for k in range(DPS - 1):
                over_dp(k).start()

        pl.when(d < DPS - 1)(lambda: over_dp(0).wait_recv())

    def drain():
        @pl.when(last)
        def _():
            for k in range(1, MPS):
                over_mp(k).wait_send()
            for k in range(DPS - 1):
                over_dp(k).wait_send()

    return begin, finish, drain


SIDE_Z, SIDE_Y, SIDE_X, CORE = 0, 3, 4, 5


class BlocksOut:
    def __init__(self, wb, ssem, rsem):
        self.wb, self.ssem, self.rsem = wb, ssem, rsem
        self.d, self.m, self.x, self.c, self.a, self.b = place()
        d, m, b, c = self.d, self.m, self.b, self.c
        self.far = (d + 2) % DPS
        self.dev = {
            SIDE_Y: {"dp": d, "mp": m + 1 - 2 * b},
            SIDE_X: {"dp": self.far, "mp": m},
            CORE: {"dp": d + 1 - 2 * c, "mp": m},
        }
        for j in range(1, LINES):
            self.dev[SIDE_Z + j - 1] = {"dp": d, "mp": 2 * twin(self.a, j) + b}

    def copy(self, s, way):
        return remote(self.wb.at[s], self.wb.at[s], self.ssem.at[0], self.rsem.at[s], self.dev[way])

    def arrive(self, s):
        self.copy(s, CORE).wait_recv()

    def row(self, j, same):
        return 2 * twin(self.a, j) + (self.b if same else 1 - self.b)

    def own_ways(self, core):
        return [SIDE_Z, SIDE_Z + 1, SIDE_Z + 2, SIDE_Y] + ([SIDE_X] if core else []) + [CORE]

    def start(self, s, ways):
        for way in ways:
            self.copy(s, way).start()

    def origin_x(self, dd):
        pl.when(self.d == dd)(lambda: self.start(slot(self.m, dd), [SIDE_X]))

    def origin_out(self, dd):
        pl.when(self.d == dd)(lambda: self.start(slot(self.m, dd), self.own_ways(0)))

    def origin_in(self, dd):
        @pl.when(self.d != dd)
        def _():
            s = slot(self.m, dd)
            self.arrive(s)
            self.start(s, self.own_ways(0))

    def own(self):
        self.start(slot(self.m, self.d), self.own_ways(1))

    def line_ways(self, core):
        return [SIDE_Y] + ([SIDE_X] if core else []) + [CORE]

    def side_ways(self, core):
        return ([SIDE_X] if core else []) + [CORE]

    def line(self, core, dd, j):
        s = slot(self.row(j, True), dd)
        self.arrive(s)
        self.start(s, self.line_ways(core))

    def side(self, core, dd, j):
        s = slot(self.row(j, False), dd)
        self.arrive(s)
        self.start(s, self.side_ways(core))

    def cross(self, j, same):
        s = slot(self.row(j, same), self.far)
        self.arrive(s)
        self.start(s, [CORE])

    def from_core(self, dd):
        for row in range(MPS):
            self.arrive(slot(row, dd))

    def group_from_core(self, dd, j):
        self.arrive(slot(self.row(j, True), dd))
        self.arrive(slot(self.row(j, False), dd))

    def drain(self):
        sent_all(self.wb, self.ssem, self.dev[CORE])


def sent_all(blocks, sem, dev):
    span = blocks.at[pl.ds(0, MPS * DPS - 1)]
    remote(span, span, sem.at[0], sem.at[0], dev).wait_send()


class BlocksIn:
    def __init__(self, gb, rc, rx, ry, rz, total, spare, sent, sems):
        self.gb, self.rc, self.rx, self.ry, self.rz = gb, rc, rx, ry, rz
        self.total, self.spare = total, spare
        self.sent, self.sems = sent, sems
        self.d, self.m, self.x, self.c, self.a, self.b = place()
        d, m, b, c = self.d, self.m, self.b, self.c
        self.far = (d + 2) % DPS
        self.twin = d + 1 - 2 * c
        self.to_core = {"dp": self.twin, "mp": m}
        self.to_x = {"dp": self.far, "mp": m}
        self.to_y = {"dp": d, "mp": m + 1 - 2 * b}

    def move(self, s, dst, name, k, part, dev):
        rows = pl.ds(*part[1:])
        return remote(self.gb.at[s, rows], dst.at[rows], self.sent.at[0], self.sems[name].at[k, part[0]], dev)

    def by_core(self, row, dd, part):
        k = dd // 2 * MPS + row
        return self.move(slot(row, dd), self.rc.at[k], "core", k, part, self.to_core)

    def by_x(self, k, s, part):
        return self.move(s, self.rx.at[k], "x", k, part, self.to_x)

    def by_y(self, k, t, dd, part):
        return self.move(slot(2 * t + 1 - self.b, dd), self.ry.at[k * LINES + t], "y", k * LINES + t, part, self.to_y)

    def by_z(self, k, t, dd, part):
        rows = pl.ds(*part[1:])
        n = k * LINES + self.a
        return remote(
            self.gb.at[slot(2 * t + self.b, dd), rows],
            self.rz.at[n].at[rows],
            self.sent.at[0],
            self.sems["z"].at[n, part[0]],
            {"dp": self.d, "mp": 2 * t + self.b},
        )

    def from_z(self, k, t, part):
        rs = self.sems["z"]
        ref = self.rz.at[k * LINES + t].at[pl.ds(*part[1:])]
        remote(ref, ref, rs.at[k * LINES + t, part[0]], rs.at[k * LINES + t, part[0]], self.to_y).wait_recv()

    def add(self, s, part, *got):
        rows = pl.ds(*part[1:])
        value = self.gb[s, rows].astype(f32)
        for ref in got:
            value = value + ref[rows].astype(f32)
        self.gb[s, rows] = value.astype(bf16)

    def along_z(self, k, t, dd, part):
        pl.when(t != self.a)(lambda: self.by_z(k, t, dd, part).start())

    def line_here(self, k):
        for j in range(1, LINES):
            self.from_z(k, twin(self.a, j), WHOLE[0])

    def end_z(self, k, dd, part, to):
        rows = pl.ds(*part[1:])
        value = self.gb[slot(self.m, dd), rows].astype(f32)
        for j in range(1, LINES):
            value = value + self.rz[k * LINES + twin(self.a, j), rows].astype(f32)
        to[rows, :] = value

    def zero_over(self, dd, t, part):
        row = 2 * t + 1 - self.b
        self.by_core(row, dd, part).wait_recv()
        self.add(slot(row, dd), part, self.rc.at[dd // 2 * MPS + row])
        self.by_y(dd // 2, t, dd, part).start()

    def zero_own(self, dd, t, part):
        row = 2 * t + self.b
        k = dd // 2
        self.by_core(row, dd, part).wait_recv()
        self.by_y(k, t, dd, part).wait_recv()
        self.add(slot(row, dd), part, self.rc.at[k * MPS + row], self.ry.at[k * LINES + t])
        self.along_z(k, t, dd, part)

    def zero_end(self, dd, part):
        k = dd // 2
        s = slot(self.m, dd)
        rows = pl.ds(*part[1:])
        self.end_z(k, dd, part, self.spare)

        @pl.when(self.d != dd)
        def _():
            self.gb[s, rows] = self.spare[rows, :].astype(bf16)
            self.by_x(k, s, part).start()

        @pl.when(self.d == dd)
        def _():
            self.total[rows, :] = self.spare[rows, :]

    def zero_take(self, dd, part):
        rows = pl.ds(*part[1:])

        @pl.when(self.d == dd)
        def _():
            self.by_x(dd // 2, slot(self.m, dd), part).wait_recv()
            self.total[rows, :] += self.rx[dd // 2, rows].astype(f32)

    def one_end(self, part):
        self.line_here(0)
        self.end_z(0, self.d, part, self.total)

    def turn(self, n):
        return twin(self.a, LINES - 1 - n % LINES)

    def row_turn(self, n):
        return 2 * self.turn(n) + self.b + (1 - 2 * self.b) * (1 - n // LINES)

    def one_far(self, n, part):
        row = self.row_turn(n)
        dd = self.far
        self.by_core(row, dd, part).wait_recv()
        self.add(slot(row, dd), part, self.rc.at[dd // 2 * MPS + row])
        self.by_x(row, slot(row, dd), part).start()

    def one_over(self, t, part):
        row = 2 * t + 1 - self.b
        dd = self.d
        self.by_core(row, dd, part).wait_recv()
        self.by_x(row, slot(row, dd), part).wait_recv()
        self.add(slot(row, dd), part, self.rc.at[dd // 2 * MPS + row], self.rx.at[row])
        self.by_y(0, t, dd, part).start()

    def one_own(self, t, part):
        row = 2 * t + self.b
        dd = self.d
        self.by_core(row, dd, part).wait_recv()
        self.by_x(row, slot(row, dd), part).wait_recv()
        self.by_y(0, t, dd, part).wait_recv()
        self.add(slot(row, dd), part, self.rc.at[dd // 2 * MPS + row], self.rx.at[row], self.ry.at[t])
        self.along_z(0, t, dd, part)

    def drain(self):
        sent_all(self.gb, self.sent, self.to_core)


WHOLE = ((0, 0, QROWS),)
PARTS = ((0, 0, QROWS // 2), (1, QROWS // 2, QROWS // 2))


def smalls_in(gsm, got, part, got2, total, ssem, rsem, rsem2):
    d, m, *_ = place()

    def over_mp(k):
        dst = (m + k) % MPS
        return remote(gsm.at[dst], got.at[k], ssem.at[k], rsem.at[k], {"dp": d, "mp": dst})

    def over_dp(k):
        return remote(part, got2.at[k], ssem.at[0], rsem2.at[k], {"dp": DPS - 1, "mp": m})

    for k in range(1, MPS):
        over_mp(k).start()

    def middle():
        value = gsm[m]
        for k in range(1, MPS):
            over_mp(k).wait_recv()
            value = value + got[k]
        part[...] = value
        for k in range(DPS - 1):
            pl.when(d == k)(lambda k=k: over_dp(k).start())

    def end():
        @pl.when(d == DPS - 1)
        def _():
            total[...] = part[...]
            for k in range(DPS - 1):
                over_dp(k).wait_recv()
                total[...] += got2[k]

    def drain():
        for k in range(DPS - 1):
            pl.when(d == k)(lambda k=k: over_dp(k).wait_send())
        for k in range(1, MPS):
            over_mp(k).wait_send()

    return middle, end, drain


def flat_grads(total, smalls, fl, roll, head, head_sem, wide, tall, gflat):
    d, m, *_ = place()
    back = remote(fl.at[0:8], head.at[1, 0:8], head_sem.at[2], head_sem.at[3], {"dp": (d + DPS - 1) % DPS, "mp": m})

    def put(start, size, step, val):
        fl[pl.ds(start, size, stride=step), :] = val

    def rest():
        fl[768:792, :] = jnp.zeros((24, 128), f32)

        @pl.when(d == 1)
        def _():
            for j in range(2):
                js = slice(j * 128, (j + 1) * 128)
                for half in range(2):
                    put(2 * half + j, 64, 4, total[half * 64 : half * 64 + 64, js])
                put(256 + j, 256, 2, total[128:384, js])

        @pl.when(d == 2)
        def _():
            for j in range(2):
                js = slice(j * 128, (j + 1) * 128)
                put(j, 256, 2, total[0:256, js])
                for half in range(2):
                    at = 256 + half * 64
                    put(512 + 2 * half + j, 64, 4, total[at : at + 64, js])

        @pl.when(d == 3)
        def _():
            for j in range(2):
                js = slice(j * 128, (j + 1) * 128)
                for half in range(2):
                    put(2 * half + j, 192, 4, total[half * 192 : half * 192 + 192, js])

        pl.when(d > 0)(lambda: back.start())

    def first():
        @pl.when(d == 0)
        def _():
            tall[192:256, :] = jnp.zeros((64, C), f32)
            for half in range(2):
                for kind in range(3):
                    for i in range(2):
                        frm = half * 192 + kind * 64 + i * 32
                        to = i * 96 + kind * 32
                        tall[to : to + 32, HALVES[half]] = total[frm : frm + 32, :]
            wide[0:C, :] = tall[0:128, :].T
            wide[C : 2 * C, :] = tall[128:256, :].T
            low = iota((256, 128), 1) < 64

            def every(start):
                return wide[pl.ds(start, 256, stride=2), :]

            one, two = pltpu.roll(every(1), 64, 1), pltpu.roll(every(C + 1), 64, 1)
            put(0, 256, 3, every(0))
            put(1, 256, 3, jnp.where(low, every(C), one))
            put(2, 256, 3, jnp.where(low, one, two))

    def end():
        @pl.when(d == DPS - 1)
        def _():
            fl[768:784, :] = smalls[...]

        @pl.when(d < DPS - 1)
        def _():
            back.wait_recv()
            fl[768:776, :] = head[1, 0:8, :]

        lane = iota((FLAT, 128), 1)
        for k in range(DPS):

            @pl.when(d == k)
            def _(k=k):
                lanes, down = OFFSET * k % 128, OFFSET * k // 128
                if k == 0:
                    gflat[...] = fl[0:FLAT, :]
                else:
                    roll[0:784, :] = pltpu.roll(fl[0:784, :], 128 - lanes, 1)
                    roll[784:792, :] = jnp.zeros((8, 128), f32)
                    gflat[...] = jnp.where(lane < 128 - lanes, roll[down : down + FLAT, :], roll[down + 1 : down + 1 + FLAT, :])

    def drain():
        pl.when(d > 0)(lambda: back.wait_send())

    return rest, first, end, drain


def step_kernel(images, rows, length, *refs):
    (counts, *far_in) = refs[:6]
    (*far_out, gflat) = refs[6:9]
    (
        fl, roll, head, wide, tall, wb, sm, vecs, b1, tabs, tabs2, bias, gvec, gb1, acc, gb, gsm, got, part_sm, got2,
        stotal, rc, rx, ry, rz, total, spare,
        head_sem, sm_s, sm_r, ag_s, ag_r, rsm_s, rsm_r, rsm_r2, sent, r_core, r_x, r_y, r_z,
    ) = refs[9:49]
    (x, cot, pf, sel, mask, out, gin, near_sem) = refs[49:57]
    ln1, qkv, wq, probs, mixed, ln2, act, gpre, gresb, gres, gmix, gl1, goutb = refs[57:]
    x_in, cot_in, pf_in, sel_in, mask_in = (
        pltpu.make_async_copy(src, dst, near_sem.at[n]) for n, (src, dst) in enumerate(zip(far_in, (x, cot, pf, sel, mask)))
    )
    out_back = pltpu.make_async_copy(out, far_out[0], near_sem.at[5])
    gin_back = pltpu.make_async_copy(gin, far_out[1], near_sem.at[6])
    greet()
    for copy in (pf_in, mask_in, x_in, sel_in, cot_in):
        copy.start()
    pf_in.wait()
    hand_tail, flatten_rest = flatten_params(pf, fl, roll, head, head_sem, wide, wb, sm)
    outs = BlocksOut(wb, ag_s, ag_r)
    zero, one = outs.c == 0, outs.c == 1
    begin_sm, finish_sm, drain_sm = smalls_out(sm, sm_s, sm_r)
    greeted()
    hand_tail()
    begin_sm()

    @pl.when(zero)
    def _():
        outs.origin_x(0)
        outs.origin_out(0)

    flatten_rest()
    pl.when(one)(lambda: outs.own())

    @pl.when(zero)
    def _():
        outs.origin_x(2)
        outs.origin_in(0)

    finish_sm()
    mask_in.wait()
    gather_smalls(sm, vecs, b1, tabs, bias, mask)
    x_in.wait()
    first_norm(x, vecs, ln1)
    sel_in.wait()

    def two(fn, *args):
        return functools.partial(fn, 0, 2, *args)

    def qk(fn, j):
        return functools.partial(fn, 0, 0, j)

    def mine(fn, *args):
        return functools.partial(fn, 1, outs.d, *args)

    def cross(j, same):
        return functools.partial(outs.cross, j, same)

    def run(fns):
        for fn in fns:
            fn()

    def at_point(zeros, ones, point):
        if point in zeros:
            pl.when(zero)(lambda: run(zeros[point]))
        if point in ones:
            pl.when(one)(lambda: run(ones[point]))

    def poll(zeros, ones, j, i):
        points = set(zeros) | set(ones)

        def group(jj):
            for ii in range(images):
                if images * jj + ii in points:
                    pl.when(i == ii)(functools.partial(at_point, zeros, ones, images * jj + ii))

        for jj in range(NG):
            if points & set(range(images * jj, images * jj + images)):
                pl.when(j == jj)(functools.partial(group, jj))

    zero_at = {
        0: [functools.partial(outs.origin_out, 2), qk(outs.line, 1), qk(outs.side, 0)],
        1: [qk(outs.line, 2), functools.partial(outs.origin_in, 2)],
        2: [qk(outs.line, 3)],
        4: [qk(outs.side, 1)],
        5: [two(outs.line, 1)],
        6: [two(outs.side, 0)],
        7: [two(outs.line, 2)],
        8: [qk(outs.side, 2)],
        9: [two(outs.line, 3)],
        10: [two(outs.side, 1)],
        12: [qk(outs.side, 3), two(outs.side, 2)],
        14: [two(outs.side, 3)],
    }
    one_at = {
        0: [mine(outs.line, 1), mine(outs.side, 0), functools.partial(outs.group_from_core, 0, 0)],
        1: [cross(0, True)],
        2: [mine(outs.line, 2)],
        4: [functools.partial(outs.group_from_core, 0, 1), mine(outs.side, 1)],
        5: [mine(outs.line, 3)],
        6: [cross(1, True), cross(0, False)],
        7: [mine(outs.side, 2)],
        8: [functools.partial(outs.group_from_core, 0, 2), cross(2, True), cross(1, False)],
        10: [mine(outs.side, 3), cross(3, True)],
        12: [functools.partial(outs.group_from_core, 0, 3), cross(2, False)],
        14: [cross(3, False)],
    }
    mixed[...] = jnp.zeros_like(mixed)

    def forward(n, _):
        j, i = n // images, n % images
        g = twin(outs.a, j)
        poll(zero_at, one_at, j, i)
        pl.when(i == 0)(lambda: project_group(g, wb, vecs, ln1, qkv))
        attend(i, g, length, sel, bias, qkv, wq, probs, mixed)
        return 0

    lax.fori_loop(0, NG * images, forward, 0)
    at_point(zero_at, one_at, 16)

    @pl.when(zero)
    def _():
        outs.from_core(1)
        outs.from_core(3)

    pl.when(one)(lambda: outs.from_core(2))

    cot_in.wait()
    feed_forward(
        rows, counts[outs.d] * PIX - outs.m * rows, x, cot, wb, vecs, b1, out, gvec, gb1, mixed, ln2, act, gpre, gresb, gres, gmix, goutb
    )
    out_back.start()
    proj_grads(gb, mixed, gresb)
    ins = BlocksIn(
        gb, rc, rx, ry, rz, total, spare, sent, {"core": r_core, "x": r_x, "y": r_y, "z": r_z}
    )
    whole = WHOLE[0]

    def grads(n, _):
        row = ins.row_turn(n)
        feed_forward_grads(row, gb, act, goutb, ln2, gpre)

        @pl.when(zero)
        def _():
            for dd in (1, 3):
                ins.by_core(row, dd, whole).start()

        pl.when(one)(lambda: ins.by_core(row, 2, whole).start())
        pl.when((n >= 1) & one)(lambda: ins.one_far(n - 1, whole))
        pl.when((n >= 1) & (n <= LINES) & zero)(lambda: ins.zero_over(2, ins.turn(n - 1), whole))
        return 0

    lax.fori_loop(0, MPS, grads, 0)
    turn = [ins.turn(n) for n in range(LINES)]

    def step(fn, *args):
        return functools.partial(fn, *args, whole)

    lay_rest, lay_first, lay_end, drain_lay = flat_grads(
        total, stotal, fl, roll, head, head_sem, wide, tall, gflat
    )
    zero_at = {
        1: [step(ins.zero_own, 2, turn[0])],
        2: [step(ins.zero_own, 2, turn[1])],
        3: [step(ins.zero_own, 2, turn[2])],
        4: [step(ins.zero_own, 2, turn[3])],
        5: [step(ins.zero_over, 0, turn[0])],
        8: [step(ins.zero_own, 0, turn[0])],
        9: [step(ins.zero_over, 0, turn[1])],
        14: [functools.partial(ins.line_here, 1), step(ins.zero_end, 2)],
        12: [step(ins.zero_own, 0, turn[1])],
        13: [step(ins.zero_over, 0, turn[2])],
        15: [step(ins.zero_own, 0, turn[2])],
    }
    one_at = {
        0: [step(ins.one_far, MPS - 1)],
        1: [step(ins.one_over, turn[0])],
        2: [step(ins.one_over, turn[1])],
        3: [step(ins.one_over, turn[2])],
        4: [step(ins.one_over, turn[3])],
        7: [step(ins.one_own, turn[0])],
        9: [step(ins.one_own, turn[1])],
        10: [step(ins.one_own, turn[2])],
        11: [step(ins.one_own, turn[3])],
    }
    acc[...] = jnp.zeros_like(acc)
    gvec[2:4, :] = jnp.zeros((2, C), f32)
    gl1[...] = jnp.zeros_like(gl1)

    def backward(n, _):
        j, i = n // images, n % images
        g = ins.turn(j)
        poll(zero_at, one_at, j, i)

        @pl.when(i == 0)
        def _():
            qkv[...] = jnp.zeros_like(qkv)

        attend_back(i, g, length, sel, gmix, wq, probs, qkv, acc, gvec)

        @pl.when((i == images - 1) & (j < NG - 1))
        def _():
            group_grads(g, gb, qkv, ln1)

            @pl.when(one)
            def _():
                for r in range(2):
                    ins.by_core(2 * g + r, 0, whole).start()

            group_norm_grad(g, wb, qkv, gl1)

        return 0

    lax.fori_loop(0, NG * images, backward, 0)
    own = ins.a
    group_grads(own, gb, qkv, ln1)

    @pl.when(one)
    def _():
        for same in (0, 1):
            for part in PARTS:
                ins.by_core(2 * own + (1 - ins.b if same == 0 else ins.b), 0, part).start()

    scatter_smalls(gvec, gb1, acc, gsm, tabs2)

    @pl.when(zero)
    def _():
        for part in PARTS:
            ins.zero_over(0, own, part)

    group_norm_grad(own, wb, qkv, gl1)
    first_norm_sums(x, gl1, gvec)
    scatter_first(gvec, gsm)
    mid_sm, end_sm, drain_in = smalls_in(gsm, got, part_sm, got2, stotal, rsm_s, rsm_r, rsm_r2)
    pl.when(one)(lambda: ins.one_end(whole))
    pl.when(zero)(lambda: ins.zero_take(2, whole))
    lay_rest()
    first_norm_back(x, vecs, gl1, gres, gin)
    gin_back.start()

    @pl.when(zero)
    def _():
        ins.line_here(0)
        for part in PARTS:
            ins.zero_own(0, own, part)
            ins.zero_end(0, part)

    mid_sm()

    @pl.when(zero)
    def _():
        for part in PARTS:
            ins.zero_take(0, part)

    lay_first()
    end_sm()
    lay_end()

    ins.drain()
    out_back.wait()
    gin_back.wait()
    drain_lay()
    drain_in()
    outs.drain()
    drain_sm()


def step_call(x, cot, counts, pf):
    rows = x.shape[0]
    images = rows // PIX
    length = image_frames(images)[2]
    sel = jnp.asarray(placement(images), bf16)
    mask = jnp.asarray(score_masks(), f32)
    vmem = pl.BlockSpec(memory_space=pltpu.VMEM)
    smem = pl.BlockSpec(memory_space=pltpu.SMEM)
    far = pl.BlockSpec(memory_space=pl.ANY)
    s = jax.ShapeDtypeStruct
    dma = pltpu.SemaphoreType.DMA
    nb = MPS * DPS
    return pl.pallas_call(
        functools.partial(step_kernel, images, rows, length),
        out_shape=(s((rows, C), bf16), s((rows, C), bf16), s((FLAT, 128), f32)),
        in_specs=[smem] + [far] * 5,
        out_specs=(far, far, vmem),
        scratch_shapes=[
            pltpu.VMEM((792, 128), f32),
            pltpu.VMEM((792, 128), f32),
            pltpu.VMEM((2, 16, 128), f32),
            pltpu.VMEM((2 * C, 128), f32),
            pltpu.VMEM((256, C), f32),
            pltpu.VMEM((nb, QROWS, 256), bf16),
            pltpu.VMEM((MPS, 16, 128), bf16),
            pltpu.VMEM((8, C), f32),
            pltpu.VMEM((1, FF), f32),
            pltpu.VMEM((MPS, 384), f32),
            pltpu.VMEM((MPS, 512), f32),
            pltpu.VMEM((NW * NG, SEG, GH * SEG), f32),
            pltpu.VMEM((8, C), f32),
            pltpu.VMEM((1, FF), f32),
            pltpu.VMEM((NG, SEG, GH * SEG), f32),
            pltpu.VMEM((nb, QROWS, 256), bf16),
            pltpu.VMEM((MPS, 16, 128), f32),
            pltpu.VMEM((MPS, 16, 128), f32),
            pltpu.VMEM((16, 128), f32),
            pltpu.VMEM((DPS, 16, 128), f32),
            pltpu.VMEM((16, 128), f32),
            pltpu.VMEM((2 * MPS, QROWS, 256), bf16),
            pltpu.VMEM((MPS, QROWS, 256), bf16),
            pltpu.VMEM((2 * LINES, QROWS, 256), bf16),
            pltpu.VMEM((2 * LINES, QROWS, 256), bf16),
            pltpu.VMEM((QROWS, 256), f32),
            pltpu.VMEM((QROWS, 256), f32),
            dma((4,)),
            dma((MPS + DPS - 1,)),
            dma((MPS + 1,)),
            dma((1,)),
            dma((nb,)),
            dma((MPS,)),
            dma((MPS,)),
            dma((DPS,)),
            dma((1,)),
            dma((2 * MPS, 2)),
            dma((MPS, 2)),
            dma((2 * LINES, 2)),
            dma((2 * LINES, 2)),
            pltpu.VMEM((rows, C), bf16),
            pltpu.VMEM((rows, C), bf16),
            pltpu.VMEM((FLAT, 128), f32),
            pltpu.VMEM((images, NW * SEG, length), bf16),
            pltpu.VMEM((NW, SEG, GH * SEG), f32),
            pltpu.VMEM((rows, C), bf16),
            pltpu.VMEM((rows, C), bf16),
            dma((7,)),
        ]
        + mega_scratch(images, rows),
        compiler_params=pltpu.CompilerParams(
            vmem_limit_bytes=62 * 1024 * 1024, collective_id=0, has_side_effects=True
        ),
    )(counts, x, cot, pf, sel, mask)


VEC_LABELS = [
    "norm1_gain",
    "norm1_bias",
    "query_bias",
    "value_bias",
    "proj_bias",
    "norm2_gain",
    "norm2_bias",
    "fc2_bias",
]


def segment_shapes(width_rank, hidden_rank):
    return [
        ("qkv_weight", (C, 3 * width_rank)),
        ("proj_weight", (width_rank, C)),
        ("fc1_weight", (C, hidden_rank)),
        ("fc2_weight", (hidden_rank, C)),
        ("norm1_gain", (width_rank,)),
        ("norm1_bias", (width_rank,)),
        ("query_bias", (width_rank,)),
        ("value_bias", (width_rank,)),
        ("proj_bias", (width_rank,)),
        ("norm2_gain", (width_rank,)),
        ("norm2_bias", (width_rank,)),
        ("fc1_bias", (hidden_rank,)),
        ("fc2_bias", (width_rank,)),
        ("table", (SPAN * SPAN, width_rank // HD)),
    ]


def unpack(flat, width_rank, hidden_rank):
    pieces = {}
    offset = 0
    for label, shape in segment_shapes(width_rank, hidden_rank):
        amount = math.prod(shape)
        pieces[label] = flat[:, offset : offset + amount].reshape((flat.shape[0],) + shape)
        offset = offset + amount
    return pieces


def finish(output, grad_input, grad_shard, params, moment_one, moment_two):
    group = lax.axis_index("dp")
    shard_length = params.shape[1]
    weights_rank = (4 * C * C + 2 * C * FF) // lax.axis_size("mp")
    position = group * shard_length + jnp.arange(shard_length, dtype=jnp.int32)[None, :]
    decays = (position < weights_rank).astype(jnp.float32)
    new_one = beta_one * moment_one + (1.0 - beta_one) * grad_shard
    new_two = second_decay_rate * moment_two + (1.0 - second_decay_rate) * grad_shard * grad_shard
    corrected_one = new_one / (1.0 - beta_one**adam_step)
    corrected_two = new_two / (1.0 - second_decay_rate**adam_step)
    new_params = params - learn_rate * (
        corrected_one / (jnp.sqrt(corrected_two) + adam_eps) + weight_decay * decays * params
    )
    return (output, grad_input, grad_shard, new_params, new_one, new_two)


def local_xla(tokens, cotangent, image_counts, params, moment_one, moment_two):
    ranks = lax.axis_size("mp")
    rank = lax.axis_index("mp")
    group = lax.axis_index("dp")
    width = C // ranks
    hidden = FF // ranks
    heads = width // HD
    rows = tokens.shape[0]
    shard_length = params.shape[1]
    length = shard_length * lax.axis_size("dp")
    owned = lax.all_gather(params.astype(bf16), "mp", axis=0, tiled=True)
    owned = lax.all_gather(owned, "dp", axis=1, tiled=True)
    op = unpack(owned, width, hidden)
    wqkv = op["qkv_weight"].reshape(ranks, C, heads, 3, HD).transpose(3, 0, 2, 4, 1).reshape(3 * C, C)
    wproj = op["proj_weight"].reshape(C, C)
    w1 = op["fc1_weight"].transpose(1, 0, 2).reshape(C, FF)
    w2 = op["fc2_weight"].reshape(FF, C)
    vecs = jnp.stack([op[n].reshape(C) for n in VEC_LABELS]).astype(f32)
    b1 = op["fc1_bias"].reshape(1, FF).astype(f32)
    bias = score_bias(op["table"].transpose(1, 0, 2).reshape(-1, HEADS))
    limit = jnp.sum(
        jnp.where(jnp.arange(image_counts.shape[0], dtype=jnp.int32) == group, image_counts, 0)
    )
    nlive = jnp.clip(limit * PIX - rank * rows, 0, rows).reshape(1)
    output, grad_input, gqkv, gproj, g1, g2, gvec, gb1, acc = block_compute(
        tokens, cotangent, nlive, wqkv, wproj, w1, w2, vecs, b1, bias
    )
    gtable = table_back(acc)
    gvec = gvec.reshape(8, ranks, width)
    pieces = [
        gqkv.reshape(3, ranks, heads, HD, C).transpose(1, 4, 2, 0, 3).reshape(ranks, -1),
        gproj.reshape(ranks, -1),
        g1.reshape(C, ranks, hidden).transpose(1, 0, 2).reshape(ranks, -1),
        g2.T.reshape(ranks, -1),
    ]
    pieces += [gvec[i].astype(bf16) for i in range(7)]
    pieces += [gb1.reshape(ranks, hidden).astype(bf16), gvec[7].astype(bf16)]
    pieces += [gtable.reshape(-1, ranks, heads).transpose(1, 0, 2).reshape(ranks, -1).astype(bf16)]
    used = sum(p.shape[1] for p in pieces)
    pieces.append(jnp.zeros((ranks, length - used), bf16))
    flat = jnp.concatenate(pieces, axis=1)
    flat = lax.psum_scatter(flat, "mp", scatter_dimension=0, tiled=True)
    grad_shard = lax.psum_scatter(flat, "dp", scatter_dimension=1, tiled=True).astype(f32)
    return finish(output, grad_input, grad_shard, params, moment_one, moment_two)


def local(tokens, cotangent, image_counts, params, moment_one, moment_two):
    ranks = lax.axis_size("mp")
    rows = tokens.shape[0]
    shard = params.shape[1]
    fits = (
        ranks == MPS
        and lax.axis_size("dp") == DPS
        and rows % 16 == 0
        and image_frames(rows // PIX)[0][-1] + image_frames(rows // PIX)[2] <= rows
        and shard == QUART + OFFSET
    )
    if not fits:
        return local_xla(tokens, cotangent, image_counts, params, moment_one, moment_two)
    pf = jnp.pad(params, ((0, 0), (0, FLAT * 128 - shard))).reshape(FLAT, 128)
    output, grad_input, gflat = step_call(tokens, cotangent, image_counts, pf)
    grad_shard = gflat.reshape(1, -1)[:, :shard]
    return finish(output, grad_input, grad_shard, params, moment_one, moment_two)


def solution(mesh):
    return jax.shard_map(
        local,
        mesh=mesh,
        in_specs=(
            P(("dp", "mp"), None),
            P(("dp", "mp"), None),
            P(),
            P("mp", "dp"),
            P("mp", "dp"),
            P("mp", "dp"),
        ),
        out_specs=(
            P(("dp", "mp"), None),
            P(("dp", "mp"), None),
            P("mp", "dp"),
            P("mp", "dp"),
            P("mp", "dp"),
            P("mp", "dp"),
        ),
        check_vma=False,
    )
```
